128 devices in a mesh: slab: 128 (over z, x, y, core).
Axes of the slice: x: 4, y: 4, z: 4, core: 2. Of those that a mesh axis runs over, the one named last changes fastest.
Arguments:
- offsets: float32 [2, 128, 16, 128], P(None, 'slab'), may hold values from 0 to 1
- velocity: float32 [2, 128, 16, 128], P(None, 'slab'), may hold values from -4 to 4
- affine: float32 [4, 128, 16, 128], P(None, 'slab'), may hold values from -1.5 to 1.5
- strain: float32 [4, 128, 16, 128], P(None, 'slab'), may hold values from -0.3 to 0.3
- tile_fill: int32 [128, 16], P('slab'), may hold values from 32 to 128
- force_field: float32 [2, 512, 1024], P(None, 'slab'), may hold values from -6 to 6
- cotangent: float32 [12, 128, 16, 128], P(None, 'slab'), may hold values from -6 to 6
Outputs:
- state_grad: float32 [12, 128, 16, 128], P(None, 'slab')
- force_grad: float32 [2, 512, 1024], P(None, 'slab')
The draws below stay inside these ranges and needn't reach their ends.
All inputs are finite; a program needn't handle non-finite values.
Results may differ from the reference program's by a relative error of at most 0.0003.
Values sent between devices are 32-bit elements; how exact they have to be, the bound alone decides.
A program may use at most 64 MiB of HBM per device.

```python
from functools import partial
import jax
import jax.numpy as jnp
from jax import lax

BR = 4
BC = 64
P_SIZE = 128
STEPS = 4
NCB = 16
BANDS = 128
ROWS = 512
W = 1024


def place_ends(values, stream_key, smallest, high):
    index_at = [jax.random.randint(jax.random.fold_in(stream_key, axis), (), 0, length) for axis, length in enumerate(values.shape)]
    longest = values.shape.index(max(values.shape))
    beside = index_at[:longest] + [(index_at[longest] + 1) % values.shape[longest]] + index_at[longest + 1:]
    return values.at[tuple(index_at)].set(smallest).at[tuple(beside)].set(high)


def shard_levels(stream_key, dims, split, least, high):
    gain = 1.0
    for axis_at, shards_of in split:
        draws = jax.random.uniform(jax.random.fold_in(jax.random.fold_in(stream_key, 6), axis_at), (shards_of,), jnp.float32, least / len(split), high / len(split))
        gain = gain * jnp.repeat(jnp.exp(draws), dims[axis_at] // shards_of).reshape((-1,) + (1,) * (len(dims) - 1 - axis_at))
    return gain


def bell_draw(own_key, shape, width, limit, split=(), held_as=jnp.bfloat16):
    values = width * jax.random.normal(own_key, shape, jnp.float32)
    if split:
        values = values * shard_levels(own_key, shape, split, -0.22, 0.18)
    return jnp.clip(values, -limit, limit).astype(held_as)


def setup_inputs(seed: int = 0) -> dict:
    splits = jax.random.split(jax.random.key(seed), 8)
    offsets = jnp.clip(1.0 * jax.random.uniform(splits[0], (2, BANDS, NCB, P_SIZE), jnp.float32) ** shard_levels(splits[0], (2, BANDS, NCB, P_SIZE), ((1, 128),), -0.2, 0.2), 0.0, 1.0)
    velocity = bell_draw(splits[1], (2, BANDS, NCB, P_SIZE), 1.0, 4.0, ((1, 128),), jnp.float32)
    affine = bell_draw(splits[2], (4, BANDS, NCB, P_SIZE), 0.3, 1.5, ((1, 128),), jnp.float32)
    strain = bell_draw(splits[3], (4, BANDS, NCB, P_SIZE), 0.08, 0.3, ((1, 128),), jnp.float32)
    tile_fill = place_ends(jax.random.randint(splits[4], (BANDS, NCB), P_SIZE // 4, P_SIZE + 1), jax.random.fold_in(splits[4], 1), P_SIZE // 4, P_SIZE).astype(jnp.int32)
    force_field = bell_draw(splits[5], (2, ROWS, W), 1.0, 6.0, ((1, 128),), jnp.float32)
    cotangent = bell_draw(splits[6], (12, BANDS, NCB, P_SIZE), 1.0, 6.0, ((1, 128),), jnp.float32)
    return {"offsets": offsets, "velocity": velocity, "affine": affine, "strain": strain, "tile_fill": tile_fill, "force_field": force_field, "cotangent": cotangent}


time_step = 0.1
shear_modulus = 2.0
bulk_modulus = 2.0
particle_mass = 1.0
mass_floor = 0.25
stress_factor = -0.4
highest = lax.Precision.HIGHEST

def spline(distance):
    magnitude = jnp.abs(distance)
    inside = 0.75 - magnitude * magnitude
    outside = 0.5 * jnp.square(jnp.maximum(1.5 - magnitude, 0.0))
    return jnp.where(magnitude < 0.5, inside, outside)

def band_weights(position):
    row_nodes = jnp.arange(2 * BR, dtype=jnp.float32)
    col_nodes = jnp.arange(2 * BC, dtype=jnp.float32)
    row_dist = row_nodes[None, None, :] - position[0][:, :, None]
    col_dist = col_nodes[None, None, :] - position[1][:, :, None]
    return (spline(row_dist), spline(col_dist), row_dist, col_dist)

def scatter_band(particles, alive_mask):
    row_weight, col_weight, row_dist, col_dist = band_weights(particles[0:2])
    upper_left, upper_right = (particles[8], particles[9])
    lower_left, lower_right = (particles[10], particles[11])
    jacobian = upper_left * lower_right - upper_right * lower_left
    pressure = bulk_modulus * (jacobian - 1.0) * jacobian
    stress_xx = shear_modulus * (upper_left * upper_left + upper_right * upper_right - 1.0) + pressure
    stress_xy = shear_modulus * (upper_left * lower_left + upper_right * lower_right)
    stress_yy = shear_modulus * (lower_left * lower_left + lower_right * lower_right - 1.0) + pressure
    masses = particle_mass * alive_mask
    moment_xx = alive_mask * stress_factor * stress_xx + masses * particles[4]
    moment_xy = alive_mask * stress_factor * stress_xy + masses * particles[5]
    moment_yx = alive_mask * stress_factor * stress_xy + masses * particles[6]
    moment_yy = alive_mask * stress_factor * stress_yy + masses * particles[7]
    plain_part = jnp.stack([row_weight * masses[:, :, None], row_weight * (masses * particles[2])[:, :, None] + row_weight * row_dist * moment_xx[:, :, None], row_weight * (masses * particles[3])[:, :, None] + row_weight * row_dist * moment_yx[:, :, None]], axis=2)
    slope_part = jnp.stack([jnp.zeros_like(row_weight), row_weight * moment_xy[:, :, None], row_weight * moment_yy[:, :, None]], axis=2)
    window_sum = jnp.einsum('cpkr,cpj->krcj', plain_part, col_weight, precision=highest)
    window_sum = window_sum + jnp.einsum('cpkr,cpj->krcj', slope_part, col_weight * col_dist, precision=highest)
    col_slots = window_sum[..., :BC] + jnp.roll(window_sum[..., BC:], 1, axis=2)
    blocks = col_slots.shape[2]
    return jnp.roll(col_slots.reshape(3, 2 * BR, blocks * BC), -(BC // 2), axis=-1)

def gather_band(particles, band_velocity):
    position = particles[0:2]
    row_weight, col_weight, row_dist, col_dist = band_weights(position)
    blocks = particles.shape[1]
    shifted = jnp.roll(band_velocity, BC // 2, axis=-1).reshape(2, 2 * BR, blocks, BC)
    windows = jnp.concatenate([shifted, jnp.roll(shifted, -1, axis=2)], axis=-1)
    plain_part = jnp.einsum('cpj,arcj->acpr', col_weight, windows, precision=highest)
    slope_part = jnp.einsum('cpj,arcj->acpr', col_weight * col_dist, windows, precision=highest)
    new_velocity = lax.optimization_barrier(jnp.sum(row_weight[None] * plain_part, axis=-1))
    along_rows = 4.0 * lax.optimization_barrier(jnp.sum((row_weight * row_dist)[None] * plain_part, axis=-1))
    along_cols = 4.0 * lax.optimization_barrier(jnp.sum(row_weight[None] * slope_part, axis=-1))
    grow_xx = 1.0 + time_step * along_rows[0]
    grow_xy = time_step * along_cols[0]
    grow_yx = time_step * along_rows[1]
    grow_yy = 1.0 + time_step * along_cols[1]
    upper_left, upper_right = (particles[8], particles[9])
    lower_left, lower_right = (particles[10], particles[11])
    return jnp.stack([position[0] + time_step * new_velocity[0], position[1] + time_step * new_velocity[1], new_velocity[0], new_velocity[1], along_rows[0], along_cols[0], along_rows[1], along_cols[1], grow_xx * upper_left + grow_xy * lower_left, grow_xx * upper_right + grow_xy * lower_right, grow_yx * upper_left + grow_yy * lower_left, grow_yx * upper_right + grow_yy * lower_right])

def place_rows(windows):
    padded_top = jnp.pad(windows[:, :, :BR], ((0, 1), (0, 0), (0, 0), (0, 0)))
    padded_low = jnp.pad(windows[:, :, BR:], ((1, 0), (0, 0), (0, 0), (0, 0)))
    slots_sum = padded_top + padded_low
    return jnp.moveaxis(slots_sum, 0, 1).reshape(slots_sum.shape[1], -1, slots_sum.shape[3])

def band_rows(extended):
    stacked = extended.reshape(extended.shape[0], -1, BR, extended.shape[2])
    paired = jnp.concatenate([stacked[:, :-1], stacked[:, 1:]], axis=2)
    return jnp.moveaxis(paired, 1, 0)

def scatter_pair(inputs):
    return scatter_band(inputs[0], inputs[1])

def gather_pair(inputs):
    return gather_band(inputs[0], inputs[1])

def gather_back(inputs):
    outputs, pullback = jax.vjp(gather_band, inputs[0], inputs[1])
    return pullback(inputs[2])

def scatter_back(inputs):
    outputs, pullback = jax.vjp(partial(scatter_band, alive_mask=inputs[1]), inputs[0])
    return pullback(inputs[2])[0]

def initial_particles(offsets, velocity, affine, strain):
    position = jnp.stack([BR // 2 + BR * offsets[0], BC // 2 + BC * offsets[1]])
    identity = jnp.array([1.0, 0.0, 0.0, 1.0], dtype=jnp.float32).reshape(4, 1, 1, 1)
    return jnp.concatenate([position, velocity, affine, strain + identity])

def fold_rows(extended):
    margin = BR // 2
    height = extended.shape[1] - BR
    interior = extended[:, margin:height + margin]
    low_rows = interior[:, :margin] + extended[:, height + margin:]
    high_rows = interior[:, height - margin:] + extended[:, :margin]
    return jnp.concatenate([low_rows, interior[:, margin:height - margin], high_rows], axis=1)

def wrap_rows(grid_field):
    margin = BR // 2
    return jnp.concatenate([grid_field[:, -margin:], grid_field, grid_field[:, :margin]], axis=1)

def reference(offsets, velocity, affine, strain, tile_fill, force_field, cotangent):
    alive_mask = (jnp.arange(P_SIZE, dtype=jnp.int32)[None, None, :] < tile_fill[:, :, None]).astype(jnp.float32)
    particles = initial_particles(offsets, velocity, affine, strain)
    history = []
    for step_index in range(STEPS):
        by_band = jnp.moveaxis(particles, 1, 0)
        summed = fold_rows(place_rows(lax.map(scatter_pair, (by_band, alive_mask))))
        inverse = 1.0 / (summed[0] + mass_floor)
        velocity_grid = (summed[1:3] + time_step * force_field) * inverse[None]
        history.append((particles, velocity_grid, inverse))
        particles = jnp.moveaxis(lax.map(gather_pair, (by_band, band_rows(wrap_rows(velocity_grid)))), 0, 1)
    adjoint = cotangent * alive_mask[None]
    force_grad = jnp.zeros_like(force_field)
    for step_index in reversed(range(STEPS)):
        particles, velocity_grid, inverse = history[step_index]
        by_band = jnp.moveaxis(particles, 1, 0)
        back_state, back_rows = lax.map(gather_back, (by_band, band_rows(wrap_rows(velocity_grid)), jnp.moveaxis(adjoint, 1, 0)))
        velocity_adjoint = fold_rows(place_rows(back_rows))
        momentum_adjoint = velocity_adjoint * inverse[None]
        mass_adjoint = -lax.optimization_barrier(jnp.sum(velocity_adjoint * velocity_grid, axis=0)) * inverse
        force_grad = force_grad + time_step * momentum_adjoint
        grid_adjoint = wrap_rows(jnp.concatenate([mass_adjoint[None], momentum_adjoint]))
        back_scatter = lax.map(scatter_back, (by_band, alive_mask, band_rows(grid_adjoint)))
        adjoint = jnp.moveaxis(back_state + back_scatter, 0, 1)
    scales = jnp.array([BR, BC], dtype=jnp.float32).reshape(2, 1, 1, 1)
    state_grad = jnp.concatenate([adjoint[0:2] * scales, adjoint[2:]])
    return (state_grad, force_grad)
```

```python
import functools

import jax
import jax.numpy as jnp
from jax import lax
from jax.experimental import pallas as pl
from jax.experimental.pallas import tpu as pltpu
from jax.sharding import PartitionSpec as P

BR = 4
BC = 64
NB = 16
NP = 128
STEPS = 4
COLS = 8
DT = 0.1
F32 = jnp.float32
BF16 = jnp.bfloat16
MESH = pl.DeviceIdType.MESH
SHIFTS = (-1, 0, 1)

EXCHANGES = 7
MAX_CH = 5


def row_spline(d):
    m = jnp.abs(d)
    t = jnp.maximum(1.5 - m, 0.0)
    near = m < 0.5
    value = jnp.where(near, 0.75 - m * m, 0.5 * t * t)
    return value, t, near


def row_slope(d, t, near):
    return jnp.where(near, -2.0 * d, jnp.where(d > 0.0, -t, t))


def col_center(p1):
    return jnp.floor(p1 + 0.5)


def col_parts(p1):
    c = col_center(p1)
    d0 = c - p1
    lo, hi = 0.5 + d0, 0.5 - d0
    values = (0.5 * lo * lo, 0.75 - d0 * d0, 0.5 * hi * hi)
    slopes = (lo, -2.0 * d0, -hi)
    w, wp, dc = [], [], []
    for s, value, slope in zip(SHIFTS, values, slopes):
        inside = jnp.logical_and(c >= float(-s), c <= float(2 * BC - 1 - s))
        w.append(jnp.where(inside, value, 0.0))
        wp.append(jnp.where(inside, slope, 0.0))
        dc.append(jnp.where(inside, d0 + float(s), 0.0))
    return c, w, wp, dc


def split_rows(x):
    top = x.astype(BF16).astype(F32)
    return jnp.concatenate([top, x - top], axis=0)


def roll(x, by):
    return pltpu.roll(x, by % x.shape[-1], axis=x.ndim - 1)


def kernel(
    n,
    off,
    vel,
    aff,
    strn,
    fill,
    force,
    cot,
    sg,
    fg,
    st,
    amat,
    alive_ref,
    hot,
    qm,
    ev,
    od,
    part,
    vg,
    inv,
    frc,
    gat,
    tsave,
    adj,
    fgacc,
    send,
    recv,
    send_sem,
    recv_sem,
):
    me = lax.axis_index("slab")
    right, left = lax.rem(me + 1, n), lax.rem(me + n - 1, n)
    barrier = pltpu.get_barrier_semaphore()
    for other in (left, right):
        pl.semaphore_signal(barrier, inc=1, device_id=(other,), device_id_type=MESH)

    lane16 = lax.broadcasted_iota(jnp.int32, (16, 128), 1)
    sub8 = lax.broadcasted_iota(jnp.int32, (8, 128), 0)
    lane8 = lax.broadcasted_iota(jnp.int32, (8, 128), 1)
    rows8 = sub8.astype(F32)
    top_half = sub8 < 4
    left_half = lane8 < 64

    eye = lax.broadcasted_iota(jnp.int32, (16, 16), 0) == lax.broadcasted_iota(jnp.int32, (16, 16), 1)
    fills = jnp.where(eye, jnp.broadcast_to(fill[...].astype(F32), (16, 16)), 0.0)
    count = jnp.sum(fills, axis=1, keepdims=True)
    alive_ref[...] = jnp.where(lane16.astype(F32) < count, 1.0, 0.0)
    st[0, 0] = BR // 2 + BR * off[0]
    st[0, 1] = BC // 2 + BC * off[1]
    for i in range(2):
        st[0, 2 + i] = vel[i]
    for i in range(4):
        st[0, 4 + i] = aff[i]
        st[0, 8 + i] = strn[i] + (1.0 if i in (0, 3) else 0.0)
    for a in range(2):
        rows = DT * force[a]
        zero = jnp.zeros((2, COLS * 128), F32)
        frc[a] = roll(jnp.concatenate([zero, rows, zero], axis=0), BC // 2)

    def prepare_forward(k):
        alive = alive_ref[...]
        p1 = st[k, 1]
        f00, f01, f10, f11 = (st[k, 8 + i] for i in range(4))
        jac = f00 * f11 - f01 * f10
        pressure = 2.0 * (jac - 1.0) * jac
        sxx = 2.0 * (f00 * f00 + f01 * f01 - 1.0) + pressure
        sxy = 2.0 * (f00 * f10 + f01 * f11)
        syy = 2.0 * (f10 * f10 + f11 * f11 - 1.0) + pressure
        tau = (sxx, sxy, sxy, syy)
        a_mat = []
        for i in range(4):
            value = alive * (-0.4 * tau[i] + st[k, 4 + i])
            amat[k, i] = value
            a_mat.append(value)
        c, w, _, dc = col_parts(p1)
        moved = (alive * st[k, 2], alive * st[k, 3])
        for j in range(3):
            wd = w[j] * dc[j]
            qm[j] = w[j] * alive
            for a in range(2):
                qm[3 + 3 * a + j] = w[j] * moved[a] + wd * a_mat[2 * a + 1]
                qm[9 + 3 * a + j] = w[j] * a_mat[2 * a]
        qm[30] = st[k, 0]
        qm[31] = jnp.where(c < 0.0, c + 128.0, jnp.where(c > 127.0, c - 128.0, c))

    def build_hot(k):
        nodes = lax.broadcasted_iota(jnp.int32, (128, 128), 0).astype(F32)
        for b in range(NB):
            row = qm[31, pl.ds(b, 1), :]
            hot[k, b] = jnp.where(nodes == jnp.broadcast_to(row, (128, 128)), 1.0, 0.0).astype(BF16)

    def adjoint_rows(k, base):
        f00, f01, f10, f11 = (st[k, 8 + i] for i in range(4))
        gf = [adj[8 + i] for i in range(4)]
        v = [adj[2 + a] + DT * adj[a] for a in range(2)]
        x = []
        for a in range(2):
            g0, g1 = gf[2 * a], gf[2 * a + 1]
            x.append(4.0 * (adj[4 + 2 * a] + DT * (g0 * f00 + g1 * f01)))
            x.append(4.0 * (adj[5 + 2 * a] + DT * (g0 * f10 + g1 * f11)))
        _, w, _, dc = col_parts(st[k, 1])
        for j in range(3):
            wd = w[j] * dc[j]
            for a in range(2):
                qm[base + 3 * a + j] = w[j] * v[a] + wd * x[2 * a + 1]
                qm[base + 6 + 3 * a + j] = w[j] * x[2 * a]
        qm[30] = st[k, 0]
        return v, x

    def scatter(k, rows):
        for b in range(NB):
            d = rows8 - jnp.broadcast_to(qm[30, pl.ds(b, 1), :], (8, 128))
            nr, _, _ = row_spline(d)
            nd = nr * d
            pieces = []
            for channel in rows:
                for q, m in channel:
                    x = nr * jnp.broadcast_to(qm[q, pl.ds(b, 1), :], (8, 128))
                    if m is not None:
                        x = x + nd * jnp.broadcast_to(qm[m, pl.ds(b, 1), :], (8, 128))
                    pieces.append(split_rows(x))
            lhs = jnp.concatenate(pieces, axis=0).astype(BF16)
            out = lax.dot_general(
                lhs, hot[k, b], (((1,), (1,)), ((), ())), preferred_element_type=F32
            )
            target = ev if b % 2 == 0 else od
            for ch in range(len(rows)):
                total = None
                for j, s in enumerate(SHIFTS):
                    at = (3 * ch + j) * 16
                    value = out[at : at + 8] + out[at + 8 : at + 16]
                    if s:
                        value = roll(value, s)
                    total = value if total is None else total + value
                if b % 2:
                    total = roll(total, 64)
                target[ch, b // 2] = total

    def forward_channels():
        return [[(j, None) for j in range(3)]] + [
            [(3 + 3 * a + j, 9 + 3 * a + j) for j in range(3)] for a in range(2)
        ]

    def adjoint_channels(base):
        return [[(base + 3 * a + j, base + 6 + 3 * a + j) for j in range(3)] for a in range(2)]

    def pack_and_send(e, count, with_force):
        for ch in range(count):
            sums = []
            for i in range(COLS):
                value = ev[ch, i] + jnp.where(left_half, od[ch, (i - 1) % COLS], od[ch, i])
                if with_force and ch in (1, 2):
                    value = value + frc[ch - 1, :, pl.ds(i * 128, 128)]
                part[ch, :, pl.ds(i * 128, 128)] = value
                sums.append(value)
            for i in range(COLS // 2):
                a, b = sums[2 * i], sums[2 * i + 1]
                down = jnp.where(top_half, pltpu.roll(a, 4, axis=0), b)
                up = jnp.where(top_half, a, pltpu.roll(b, 4, axis=0))
                send[e, 0, ch, :, pl.ds(i * 128, 128)] = down
                send[e, 1, ch, :, pl.ds(i * 128, 128)] = up
        for copy in copies(e, count):
            copy.start()

    def copies(e, count):
        return [
            pltpu.make_async_remote_copy(
                src_ref=send.at[e, side, pl.ds(0, count)],
                dst_ref=recv.at[e, side, pl.ds(0, count)],
                send_sem=send_sem.at[e, side],
                recv_sem=recv_sem.at[e, side],
                device_id=(other,),
                device_id_type=MESH,
            )
            for side, other in ((0, right), (1, left))
        ]

    def summed(e, ch, i):
        above = recv[e, 0, ch, :, pl.ds(i * 128, 128)]
        below = recv[e, 1, ch, :, pl.ds(i * 128, 128)]
        first = jnp.where(top_half, above, pltpu.roll(below, 4, axis=0))
        second = jnp.where(top_half, pltpu.roll(above, 4, axis=0), below)
        return (
            part[ch, :, pl.ds(2 * i * 128, 128)] + first,
            part[ch, :, pl.ds((2 * i + 1) * 128, 128)] + second,
        )

    def wait_halo(e, count):
        for copy in copies(e, count):
            copy.wait_recv()

    def grid_velocity(k, e):
        for i in range(COLS // 2):
            mass = summed(e, 0, i)
            mom = [summed(e, 1 + a, i) for a in range(2)]
            for h in range(2):
                at = pl.ds((2 * i + h) * 128, 128)
                inverse = 1.0 / (mass[h] + 0.25)
                inv[k, :, at] = inverse
                for a in range(2):
                    vg[k, a, :, at] = mom[a][h] * inverse

    def grid_adjoint(k, e, base):
        for i in range(COLS // 2):
            u = [summed(e, base + a, i) for a in range(2)]
            for h in range(2):
                at = pl.ds((2 * i + h) * 128, 128)
                inverse = inv[k, :, at]
                total = u[0][h] * vg[k, 0, :, at] + u[1][h] * vg[k, 1, :, at]
                part[0, :, at] = -total * inverse
                for a in range(2):
                    value = u[a][h] * inverse
                    part[1 + a, :, at] = value
                    fgacc[a, :, at] = fgacc[a, :, at] + DT * value

    def gather(k, column, channels):
        stride = 3 * channels * 64
        for b in range(NB):
            i = b // 2
            pieces = []
            for ch in range(channels):
                window = column(ch, i)
                if b % 2:
                    window = roll(jnp.where(left_half, column(ch, (i + 1) % COLS), window), 64)
                for s in SHIFTS:
                    pieces.append(split_rows(roll(window, -s) if s else window))
            lhs = jnp.concatenate(pieces, axis=0).astype(BF16)
            out = jnp.dot(lhs, hot[k, b], preferred_element_type=F32)
            for q in range(3 * channels):
                value = out[16 * q : 16 * q + 8] + out[16 * q + 8 : 16 * q + 16]
                gat[pl.ds((b // 8) * stride + q * 64 + b % 8, 8, stride=8), :] = value

    def gathered(half, channels, q, r):
        return gat[pl.ds(half * 3 * channels * 64 + q * 64 + r * 8, 8), :]

    def row_sums(half, channels, q, weights):
        totals = [None] * len(weights)
        for r in range(2 * BR):
            g = gathered(half, channels, q, r)
            for t, weight in enumerate(weights):
                value = weight[r] * g
                totals[t] = value if totals[t] is None else totals[t] + value
        return totals

    def dot3(a, b):
        return a[0] * b[0] + a[1] * b[1] + a[2] * b[2]

    def row_weights(p0, slopes):
        plain, slant, slope, slope_d = [], [], [], []
        for r in range(2 * BR):
            d = float(r) - p0
            value, t, near = row_spline(d)
            plain.append(value)
            slant.append(value * d)
            if slopes:
                der = row_slope(d, t, near)
                slope.append(der)
                slope_d.append(der * d)
        return (plain, slant, slope, slope_d) if slopes else (plain, slant)

    def advance(k, store_state):
        for half in range(2):
            at = pl.ds(8 * half, 8)
            p0, p1 = st[k, 0, at], st[k, 1, at]
            weights = row_weights(p0, False)
            _, w, _, dc = col_parts(p1)
            wd = [w[j] * dc[j] for j in range(3)]
            new_v, new_c = [], []
            for a in range(2):
                sums = [row_sums(half, 2, 3 * a + j, weights) for j in range(3)]
                r0 = [x[0] for x in sums]
                r1 = [x[1] for x in sums]
                new_v.append(dot3(w, r0))
                new_c.append(4.0 * dot3(w, r1))
                new_c.append(4.0 * dot3(wd, r0))
            for a in range(2):
                tsave[k, a, at] = new_v[a]
            for i in range(4):
                tsave[k, 2 + i, at] = new_c[i]
            if store_state:
                f = [st[k, 8 + i, at] for i in range(4)]
                st[k + 1, 0, at] = p0 + DT * new_v[0]
                st[k + 1, 1, at] = p1 + DT * new_v[1]
                for a in range(2):
                    st[k + 1, 2 + a, at] = new_v[a]
                for i in range(4):
                    st[k + 1, 4 + i, at] = new_c[i]
                for a in range(2):
                    c0, c1 = DT * new_c[2 * a], DT * new_c[2 * a + 1]
                    for j in range(2):
                        st[k + 1, 8 + 2 * a + j, at] = f[2 * a + j] + (c0 * f[j] + c1 * f[2 + j])

    def slopes_of(half, channels, first, p0, p1, count, plain_only):
        weights = row_weights(p0, True)
        _, w, wp, dc = col_parts(p1)
        wd = [w[j] * dc[j] for j in range(3)]
        wpd = [wp[j] * dc[j] for j in range(3)]
        results = []
        for ch in range(first, first + count):
            if ch < plain_only:
                sums = [row_sums(half, channels, 3 * ch + j, (weights[0], weights[2])) for j in range(3)]
                r0, r2 = ([x[t] for x in sums] for t in range(2))
                results.append((dot3(w, r2), dot3(wp, r0)))
                continue
            sums = [row_sums(half, channels, 3 * ch + j, weights) for j in range(3)]
            r0, r1, r2, r3 = ([x[t] for x in sums] for t in range(4))
            results.append(
                dict(
                    nw=dot3(w, r0),
                    dw=dot3(w, r1),
                    nwd=dot3(wd, r0),
                    pw=dot3(w, r2),
                    pdw=dot3(w, r3),
                    pwd=dot3(wd, r2),
                    nwp=dot3(wp, r0),
                    dwp=dot3(wp, r1),
                    nwpd=dot3(wpd, r0),
                )
            )
        return results

    def save_slopes(k):
        for half in range(2):
            at = pl.ds(8 * half, 8)
            found = slopes_of(half, 2, 0, st[k, 0, at], st[k, 1, at], 2, 0)
            for a, t in enumerate(found):
                for i, name in enumerate(("pw", "pdw", "pwd", "nwp", "dwp", "nwpd")):
                    value = t[name]
                    if name in ("pdw", "nwpd"):
                        value = value + t["nw"]
                    tsave[k, 6 + 6 * a + i, at] = value

    def pull_gather(k, v, x):
        gf = [adj[8 + i] for i in range(4)]
        p0, p1 = adj[0], adj[1]
        for a in range(2):
            pw, pdw, pwd, nwp, dwp, nwpd = (tsave[k, 6 + 6 * a + i] for i in range(6))
            p0 = p0 - (v[a] * pw + x[2 * a] * pdw + x[2 * a + 1] * pwd)
            p1 = p1 - (v[a] * nwp + x[2 * a] * dwp + x[2 * a + 1] * nwpd)
        adj[0] = p0
        adj[1] = p1
        c = [tsave[k, 2 + i] for i in range(4)]
        for b in range(2):
            for j in range(2):
                adj[8 + 2 * b + j] = gf[2 * b + j] + DT * (c[b] * gf[j] + c[2 + b] * gf[2 + j])

    def pull_scatter(k):
        for half in range(2):
            at = pl.ds(8 * half, 8)
            alive = alive_ref[at]
            p0, p1 = st[k, 0, at], st[k, 1, at]
            mass, px, py = slopes_of(half, 3, 0, p0, p1, 3, 1)
            a_mat = [amat[k, i, at] for i in range(4)]
            g0 = adj[0, at] - alive * mass[0]
            g1 = adj[1, at] - alive * mass[1]
            back = []
            for a, t in enumerate((px, py)):
                moved = alive * st[k, 2 + a, at]
                a0, a1 = a_mat[2 * a], a_mat[2 * a + 1]
                g0 = g0 - (moved * t["pw"] + a0 * (t["pdw"] + t["nw"]) + a1 * t["pwd"])
                g1 = g1 - (moved * t["nwp"] + a0 * t["dwp"] + a1 * (t["nwpd"] + t["nw"]))
                adj[2 + a, at] = alive * t["nw"]
                back += [alive * t["dw"], alive * t["nwd"]]
            adj[0, at] = g0
            adj[1, at] = g1
            for i in range(4):
                adj[4 + i, at] = back[i]
            f00, f01, f10, f11 = (st[k, 8 + i, at] for i in range(4))
            sxx, syy = -0.4 * back[0], -0.4 * back[3]
            sxy = -0.4 * (back[1] + back[2])
            jac = f00 * f11 - f01 * f10
            gj = (sxx + syy) * (2.0 * (2.0 * jac - 1.0))
            adj[8, at] = adj[8, at] + (4.0 * f00 * sxx + 2.0 * f10 * sxy + gj * f11)
            adj[9, at] = adj[9, at] + (4.0 * f01 * sxx + 2.0 * f11 * sxy - gj * f10)
            adj[10, at] = adj[10, at] + (4.0 * f10 * syy + 2.0 * f00 * sxy - gj * f01)
            adj[11, at] = adj[11, at] + (4.0 * f11 * syy + 2.0 * f01 * sxy + gj * f00)

    def grid_column(k):
        return lambda ch, i: vg[k, ch, :, pl.ds(i * 128, 128)]

    def part_column(ch, i):
        return part[ch, :, pl.ds(i * 128, 128)]

    def forward_step(k, first):
        prepare_forward(k)
        build_hot(k)
        scatter(k, forward_channels())
        if first:
            pl.semaphore_wait(barrier, 2)
        pack_and_send(k, 3, True)
        if not first:
            save_slopes(k - 1)
        wait_halo(k, 3)
        grid_velocity(k, k)
        gather(k, grid_column(k), 2)
        advance(k, True)

    forward_step(0, True)

    def forward_body(k, carry):
        forward_step(k, False)
        return carry

    lax.fori_loop(1, STEPS - 1, forward_body, 0)

    last = STEPS - 1
    for i in range(12):
        adj[i] = cot[i] * alive_ref[...]
    for a in range(2):
        fgacc[a] = jnp.zeros((8, COLS * 128), F32)
    prepare_forward(last)
    build_hot(last)
    adjoint_rows(last, 15)
    scatter(last, forward_channels() + adjoint_channels(15))
    pack_and_send(last, 5, True)
    save_slopes(last - 1)
    wait_halo(last, 5)
    grid_velocity(last, last)
    gather(last, grid_column(last), 2)
    advance(last, False)
    save_slopes(last)
    v, x = adjoint_rows(last, 15)
    pull_gather(last, v, x)
    grid_adjoint(last, last, 3)
    gather(last, part_column, 3)
    pull_scatter(last)

    def backward_body(t, carry):
        k = last - 1 - t
        e = last + 1 + t
        v, x = adjoint_rows(k, 15)
        scatter(k, adjoint_channels(15))
        pack_and_send(e, 2, False)
        pull_gather(k, v, x)
        wait_halo(e, 2)
        grid_adjoint(k, e, 0)
        gather(k, part_column, 3)
        pull_scatter(k)
        return carry

    lax.fori_loop(0, STEPS - 1, backward_body, 0)

    sg[0] = adj[0] * float(BR)
    sg[1] = adj[1] * float(BC)
    for i in range(2, 12):
        sg[i] = adj[i]
    for a in range(2):
        fg[a] = roll(fgacc[a], -(BC // 2))[2:6]
    for e in range(EXCHANGES):
        for copy in copies(e, 3 if e < last else (5 if e == last else 2)):
            copy.wait_send()


def per_device(n, offsets, velocity, affine, strain, tile_fill, force_field, cotangent):
    def flat(x):
        return x.reshape(x.shape[0], NB, NP)

    vmem = pl.BlockSpec(memory_space=pltpu.VMEM)
    width = COLS * 128
    state_grad, force_grad = pl.pallas_call(
        functools.partial(kernel, n),
        out_shape=(
            jax.ShapeDtypeStruct((12, NB, NP), F32),
            jax.ShapeDtypeStruct((2, BR, width), F32),
        ),
        in_specs=[vmem] * 7,
        out_specs=(vmem, vmem),
        scratch_shapes=[
            pltpu.VMEM((STEPS, 12, NB, NP), F32),
            pltpu.VMEM((STEPS, 4, NB, NP), F32),
            pltpu.VMEM((NB, NP), F32),
            pltpu.VMEM((STEPS, NB, 128, NP), BF16),
            pltpu.VMEM((32, NB, NP), F32),
            pltpu.VMEM((MAX_CH, COLS, 8, 128), F32),
            pltpu.VMEM((MAX_CH, COLS, 8, 128), F32),
            pltpu.VMEM((MAX_CH, 8, width), F32),
            pltpu.VMEM((STEPS, 2, 8, width), F32),
            pltpu.VMEM((STEPS, 8, width), F32),
            pltpu.VMEM((2, 8, width), F32),
            pltpu.VMEM((2 * 72 * 8, 128), F32),
            pltpu.VMEM((STEPS, 18, NB, NP), F32),
            pltpu.VMEM((12, NB, NP), F32),
            pltpu.VMEM((2, 8, width), F32),
            pltpu.VMEM((EXCHANGES, 2, MAX_CH, 8, width // 2), F32),
            pltpu.VMEM((EXCHANGES, 2, MAX_CH, 8, width // 2), F32),
            pltpu.SemaphoreType.DMA((EXCHANGES, 2)),
            pltpu.SemaphoreType.DMA((EXCHANGES, 2)),
        ],
        compiler_params=pltpu.CompilerParams(collective_id=0, has_side_effects=True),
    )(
        flat(offsets),
        flat(velocity),
        flat(affine),
        flat(strain),
        tile_fill,
        force_field,
        flat(cotangent),
    )
    return state_grad.reshape(12, 1, NB, NP), force_grad


def solution(mesh):
    n = mesh.shape["slab"]
    tiles = P(None, "slab", None, None)
    return jax.shard_map(
        functools.partial(per_device, n),
        mesh=mesh,
        in_specs=(tiles, tiles, tiles, tiles, P("slab", None), P(None, "slab", None), tiles),
        out_specs=(tiles, P(None, "slab", None)),
        check_vma=False,
    )
```

```python
import functools

import jax
import jax.numpy as jnp
from jax import lax
from jax.experimental import pallas as pl
from jax.experimental.pallas import tpu as pltpu
from jax.sharding import PartitionSpec as P

BR = 4
BC = 64
NB = 16
NP = 128
STEPS = 4
COLS = 8
DT = 0.1
F32 = jnp.float32
BF16 = jnp.bfloat16
MESH = pl.DeviceIdType.MESH
SHIFTS = (-1, 0, 1)

EXCHANGES = 8
MAX_CH = 5
OWN = STEPS
RAW, COT, FORCE, ADJ, FGRAD = range(5)
CHIPS = {64: (4, 4, 4), 8: (2, 2, 2), 4: (1, 2, 2)}


def host_of(band, n):
    _, nx, ny = CHIPS[n // 2]
    core, chip = lax.rem(band, 2), lax.div(band, 2)
    y, x, z = lax.rem(chip, ny), lax.rem(lax.div(chip, ny), nx), lax.div(chip, nx * ny)
    y = y + lax.rem(x, 2) * (ny - 1 - 2 * y)
    x = x + lax.rem(z, 2) * (nx - 1 - 2 * x)
    return ((z * nx + x) * ny + y) * 2 + core


def band_of(device, n):
    _, nx, ny = CHIPS[n // 2]
    core, chip = lax.rem(device, 2), lax.div(device, 2)
    y, x, z = lax.rem(chip, ny), lax.rem(lax.div(chip, ny), nx), lax.div(chip, nx * ny)
    x = x + lax.rem(z, 2) * (nx - 1 - 2 * x)
    y = y + lax.rem(x, 2) * (ny - 1 - 2 * y)
    return ((z * nx + x) * ny + y) * 2 + core


def row_spline(d):
    m = jnp.abs(d)
    t = jnp.maximum(1.5 - m, 0.0)
    near = m < 0.5
    value = jnp.where(near, 0.75 - m * m, 0.5 * t * t)
    return value, t, near


def row_slope(d, t, near):
    return jnp.where(near, -2.0 * d, jnp.where(d > 0.0, -t, t))


def col_center(p1):
    return jnp.floor(p1 + 0.5)


def col_parts(p1):
    c = col_center(p1)
    d0 = c - p1
    lo, hi = 0.5 + d0, 0.5 - d0
    values = (0.5 * lo * lo, 0.75 - d0 * d0, 0.5 * hi * hi)
    slopes = (lo, -2.0 * d0, -hi)
    w, wp, dc = [], [], []
    for s, value, slope in zip(SHIFTS, values, slopes):
        inside = jnp.logical_and(c >= float(-s), c <= float(2 * BC - 1 - s))
        w.append(jnp.where(inside, value, 0.0))
        wp.append(jnp.where(inside, slope, 0.0))
        dc.append(jnp.where(inside, d0 + float(s), 0.0))
    return c, w, wp, dc


def split_rows(x):
    top = x.astype(BF16).astype(F32)
    return jnp.concatenate([top, x - top], axis=0)


def roll(x, by):
    return pltpu.roll(x, by % x.shape[-1], axis=x.ndim - 1)


def kernel(
    n,
    off_hbm,
    vel_hbm,
    aff_hbm,
    strn_hbm,
    fill_hbm,
    force_hbm,
    cot_hbm,
    sg,
    fg,
    fill,
    raw,
    force,
    cot,
    st,
    amat,
    hot,
    qm,
    ev,
    od,
    parts,
    vg,
    inv,
    frc,
    gat,
    tsave,
    adjs,
    fgacc,
    fgmove,
    send,
    recv,
    load_sem,
    send_sem,
    recv_sem,
    move_send,
    move_recv,
):
    me = lax.axis_index("slab")
    band = band_of(me, n)
    home = host_of(me, n)
    moved = home != me
    stays = home == me

    def after(i):
        return lax.rem(i + 1, n)

    def before(i):
        return lax.rem(i + n - 1, n)

    ring = (host_of(after(band), n), host_of(before(band), n))
    to_hosts = (host_of(after(me), n), host_of(before(me), n))
    to_owners = (after(band), before(band))
    owners = (after(me), before(me))

    loads = [
        pltpu.make_async_copy(src, dst, load_sem.at[i])
        for i, (src, dst) in enumerate(
            (
                (off_hbm, raw.at[1, pl.ds(0, 2)]),
                (vel_hbm, raw.at[1, pl.ds(2, 2)]),
                (aff_hbm, raw.at[1, pl.ds(4, 4)]),
                (strn_hbm, raw.at[1, pl.ds(8, 4)]),
                (fill_hbm, fill),
                (force_hbm, force.at[1]),
                (cot_hbm, cot.at[1]),
            )
        )
    ]
    for load in loads:
        load.start()

    barrier = pltpu.get_barrier_semaphore()
    for other in ring + to_hosts + to_owners + owners:
        pl.semaphore_signal(barrier, inc=1, device_id=(other,), device_id_type=MESH)

    @pl.when(moved)
    def _():
        pl.semaphore_signal(barrier, inc=1, device_id=(home,), device_id_type=MESH)
        pl.semaphore_signal(barrier, inc=1, device_id=(band,), device_id_type=MESH)

    def barrier_wait():
        @pl.when(moved)
        def _():
            pl.semaphore_wait(barrier, 10)

        @pl.when(stays)
        def _():
            pl.semaphore_wait(barrier, 8)

    def move(which, src, dst, device):
        return pltpu.make_async_remote_copy(
            src_ref=src,
            dst_ref=dst,
            send_sem=move_send.at[which],
            recv_sem=move_recv.at[which],
            device_id=(device,),
            device_id_type=MESH,
        )

    moves = [
        move(RAW, raw.at[1], raw.at[0], home),
        move(COT, cot.at[1], cot.at[0], home),
        move(FORCE, force.at[1], force.at[0], home),
        move(ADJ, adjs.at[0], adjs.at[1], band),
        move(FGRAD, fgmove.at[0], fgmove.at[1], band),
    ]

    def start_move(which):
        @pl.when(moved)
        def _():
            moves[which].start()

    def end_move(which, ref, src, dst):
        @pl.when(moved)
        def _():
            moves[which].wait_recv()

        @pl.when(stays)
        def _():
            ref[dst] = ref[src]

    lane16 = lax.broadcasted_iota(jnp.int32, (16, 128), 1)
    sub8 = lax.broadcasted_iota(jnp.int32, (8, 128), 0)
    lane8 = lax.broadcasted_iota(jnp.int32, (8, 128), 1)
    rows8 = sub8.astype(F32)
    top_half = sub8 < 4
    left_half = lane8 < 64

    def initial_state(role, k):
        st[k, 0] = BR // 2 + BR * raw[role, 0]
        st[k, 1] = BC // 2 + BC * raw[role, 1]
        for i in range(2, 12):
            st[k, i] = raw[role, i] + (1.0 if i in (8, 11) else 0.0)

    def place_force(role):
        for a in range(2):
            rows = DT * force[role, a]
            zero = jnp.zeros((2, COLS * 128), F32)
            frc[role, a] = roll(jnp.concatenate([zero, rows, zero], axis=0), BC // 2)

    for i in (4, 0, 1, 2, 3):
        loads[i].wait()
    eye = lax.broadcasted_iota(jnp.int32, (16, 16), 0) == lax.broadcasted_iota(jnp.int32, (16, 16), 1)
    fills = jnp.where(eye, jnp.broadcast_to(fill[...].astype(F32), (16, 16)), 0.0)
    count = jnp.sum(fills, axis=1, keepdims=True)
    raw[1, 12] = jnp.where(lane16.astype(F32) < count, 1.0, 0.0)

    def prepare_forward(k, role):
        alive = raw[role, 12]
        p1 = st[k, 1]
        f00, f01, f10, f11 = (st[k, 8 + i] for i in range(4))
        jac = f00 * f11 - f01 * f10
        pressure = 2.0 * (jac - 1.0) * jac
        sxx = 2.0 * (f00 * f00 + f01 * f01 - 1.0) + pressure
        sxy = 2.0 * (f00 * f10 + f01 * f11)
        syy = 2.0 * (f10 * f10 + f11 * f11 - 1.0) + pressure
        tau = (sxx, sxy, sxy, syy)
        a_mat = []
        for i in range(4):
            value = alive * (-0.4 * tau[i] + st[k, 4 + i])
            amat[k, i] = value
            a_mat.append(value)
        c, w, _, dc = col_parts(p1)
        moved = (alive * st[k, 2], alive * st[k, 3])
        for j in range(3):
            wd = w[j] * dc[j]
            qm[j] = w[j] * alive
            for a in range(2):
                qm[3 + 3 * a + j] = w[j] * moved[a] + wd * a_mat[2 * a + 1]
                qm[9 + 3 * a + j] = w[j] * a_mat[2 * a]
        qm[30] = st[k, 0]
        qm[31] = jnp.where(c < 0.0, c + 128.0, jnp.where(c > 127.0, c - 128.0, c))

    def build_hot(k):
        nodes = lax.broadcasted_iota(jnp.int32, (128, 128), 0).astype(F32)
        for b in range(NB):
            row = qm[31, pl.ds(b, 1), :]
            hot[k, b] = jnp.where(nodes == jnp.broadcast_to(row, (128, 128)), 1.0, 0.0).astype(BF16)

    def adjoint_rows(k, base, adj):
        f00, f01, f10, f11 = (st[k, 8 + i] for i in range(4))
        gf = [adj[8 + i] for i in range(4)]
        v = [adj[2 + a] + DT * adj[a] for a in range(2)]
        x = []
        for a in range(2):
            g0, g1 = gf[2 * a], gf[2 * a + 1]
            x.append(4.0 * (adj[4 + 2 * a] + DT * (g0 * f00 + g1 * f01)))
            x.append(4.0 * (adj[5 + 2 * a] + DT * (g0 * f10 + g1 * f11)))
        _, w, _, dc = col_parts(st[k, 1])
        for j in range(3):
            wd = w[j] * dc[j]
            for a in range(2):
                qm[base + 3 * a + j] = w[j] * v[a] + wd * x[2 * a + 1]
                qm[base + 6 + 3 * a + j] = w[j] * x[2 * a]
        qm[30] = st[k, 0]
        return v, x

    def scatter(k, rows):
        for b in range(NB):
            d = rows8 - jnp.broadcast_to(qm[30, pl.ds(b, 1), :], (8, 128))
            nr, _, _ = row_spline(d)
            nd = nr * d
            pieces = []
            for channel in rows:
                for q, m in channel:
                    x = nr * jnp.broadcast_to(qm[q, pl.ds(b, 1), :], (8, 128))
                    if m is not None:
                        x = x + nd * jnp.broadcast_to(qm[m, pl.ds(b, 1), :], (8, 128))
                    pieces.append(split_rows(x))
            lhs = jnp.concatenate(pieces, axis=0).astype(BF16)
            out = lax.dot_general(
                lhs, hot[k, b], (((1,), (1,)), ((), ())), preferred_element_type=F32
            )
            target = ev if b % 2 == 0 else od
            for ch in range(len(rows)):
                total = None
                for j, s in enumerate(SHIFTS):
                    at = (3 * ch + j) * 16
                    value = out[at : at + 8] + out[at + 8 : at + 16]
                    if s:
                        value = roll(value, s)
                    total = value if total is None else total + value
                if b % 2:
                    total = roll(total, 64)
                target[ch, b // 2] = total

    def forward_channels():
        return [[(j, None) for j in range(3)]] + [
            [(3 + 3 * a + j, 9 + 3 * a + j) for j in range(3)] for a in range(2)
        ]

    def adjoint_channels(base):
        return [[(base + 3 * a + j, base + 6 + 3 * a + j) for j in range(3)] for a in range(2)]

    def combine(count, part, force_role):
        for ch in range(count):
            for i in range(COLS):
                value = ev[ch, i] + jnp.where(left_half, od[ch, (i - 1) % COLS], od[ch, i])
                if force_role is not None and ch in (1, 2):
                    value = value + frc[force_role, ch - 1, :, pl.ds(i * 128, 128)]
                part[ch, :, pl.ds(i * 128, 128)] = value

    def pack(e, count, part):
        for ch in range(count):
            for i in range(COLS // 2):
                a = part[ch, :, pl.ds(2 * i * 128, 128)]
                b = part[ch, :, pl.ds((2 * i + 1) * 128, 128)]
                down = jnp.where(top_half, pltpu.roll(a, 4, axis=0), b)
                up = jnp.where(top_half, a, pltpu.roll(b, 4, axis=0))
                send[e, 0, ch, :, pl.ds(i * 128, 128)] = down
                send[e, 1, ch, :, pl.ds(i * 128, 128)] = up

    def copies(e, count, targets, source=None):
        return [
            pltpu.make_async_remote_copy(
                src_ref=send.at[e if source is None else source, side, pl.ds(0, count)],
                dst_ref=recv.at[e, side, pl.ds(0, count)],
                send_sem=send_sem.at[e, side],
                recv_sem=recv_sem.at[e, side],
                device_id=(other,),
                device_id_type=MESH,
            )
            for side, other in enumerate(targets)
        ]

    def start_halo(e, count, targets, source=None):
        for copy in copies(e, count, targets, source):
            copy.start()

    def summed(e, part, ch, i):
        above = recv[e, 0, ch, :, pl.ds(i * 128, 128)]
        below = recv[e, 1, ch, :, pl.ds(i * 128, 128)]
        first = jnp.where(top_half, above, pltpu.roll(below, 4, axis=0))
        second = jnp.where(top_half, pltpu.roll(above, 4, axis=0), below)
        return (
            part[ch, :, pl.ds(2 * i * 128, 128)] + first,
            part[ch, :, pl.ds((2 * i + 1) * 128, 128)] + second,
        )

    def wait_halo(e, count, targets, source=None):
        for copy in copies(e, count, targets, source):
            copy.wait_recv()

    def grid_velocity(k, e, part):
        for i in range(COLS // 2):
            mass = summed(e, part, 0, i)
            mom = [summed(e, part, 1 + a, i) for a in range(2)]
            for h in range(2):
                at = pl.ds((2 * i + h) * 128, 128)
                inverse = 1.0 / (mass[h] + 0.25)
                inv[k, :, at] = inverse
                for a in range(2):
                    vg[k, a, :, at] = mom[a][h] * inverse

    def grid_adjoint(k, e, base, part, first):
        for i in range(COLS // 2):
            u = [summed(e, part, base + a, i) for a in range(2)]
            for h in range(2):
                at = pl.ds((2 * i + h) * 128, 128)
                inverse = inv[k, :, at]
                total = u[0][h] * vg[k, 0, :, at] + u[1][h] * vg[k, 1, :, at]
                part[0, :, at] = -total * inverse
                for a in range(2):
                    value = u[a][h] * inverse
                    part[1 + a, :, at] = value
                    fgacc[a, :, at] = DT * value if first else fgacc[a, :, at] + DT * value

    def gather(k, column, channels):
        stride = 3 * channels * 64
        for b in range(NB):
            i = b // 2
            pieces = []
            for ch in range(channels):
                window = column(ch, i)
                if b % 2:
                    window = roll(jnp.where(left_half, column(ch, (i + 1) % COLS), window), 64)
                for s in SHIFTS:
                    pieces.append(split_rows(roll(window, -s) if s else window))
            lhs = jnp.concatenate(pieces, axis=0).astype(BF16)
            out = jnp.dot(lhs, hot[k, b], preferred_element_type=F32)
            for q in range(3 * channels):
                value = out[16 * q : 16 * q + 8] + out[16 * q + 8 : 16 * q + 16]
                gat[pl.ds((b // 8) * stride + q * 64 + b % 8, 8, stride=8), :] = value

    def gathered(half, channels, q, r):
        return gat[pl.ds(half * 3 * channels * 64 + q * 64 + r * 8, 8), :]

    def row_sums(half, channels, q, weights):
        totals = [None] * len(weights)
        for r in range(2 * BR):
            g = gathered(half, channels, q, r)
            for t, weight in enumerate(weights):
                value = weight[r] * g
                totals[t] = value if totals[t] is None else totals[t] + value
        return totals

    def dot3(a, b):
        return a[0] * b[0] + a[1] * b[1] + a[2] * b[2]

    def row_weights(p0, slopes):
        plain, slant, slope, slope_d = [], [], [], []
        for r in range(2 * BR):
            d = float(r) - p0
            value, t, near = row_spline(d)
            plain.append(value)
            slant.append(value * d)
            if slopes:
                der = row_slope(d, t, near)
                slope.append(der)
                slope_d.append(der * d)
        return (plain, slant, slope, slope_d) if slopes else (plain, slant)

    def advance(k, store_state):
        for half in range(2):
            at = pl.ds(8 * half, 8)
            p0, p1 = st[k, 0, at], st[k, 1, at]
            weights = row_weights(p0, False)
            _, w, _, dc = col_parts(p1)
            wd = [w[j] * dc[j] for j in range(3)]
            new_v, new_c = [], []
            for a in range(2):
                sums = [row_sums(half, 2, 3 * a + j, weights) for j in range(3)]
                r0 = [x[0] for x in sums]
                r1 = [x[1] for x in sums]
                new_v.append(dot3(w, r0))
                new_c.append(4.0 * dot3(w, r1))
                new_c.append(4.0 * dot3(wd, r0))
            for a in range(2):
                tsave[k, a, at] = new_v[a]
            for i in range(4):
                tsave[k, 2 + i, at] = new_c[i]
            if store_state:
                f = [st[k, 8 + i, at] for i in range(4)]
                st[k + 1, 0, at] = p0 + DT * new_v[0]
                st[k + 1, 1, at] = p1 + DT * new_v[1]
                for a in range(2):
                    st[k + 1, 2 + a, at] = new_v[a]
                for i in range(4):
                    st[k + 1, 4 + i, at] = new_c[i]
                for a in range(2):
                    c0, c1 = DT * new_c[2 * a], DT * new_c[2 * a + 1]
                    for j in range(2):
                        st[k + 1, 8 + 2 * a + j, at] = f[2 * a + j] + (c0 * f[j] + c1 * f[2 + j])

    def slopes_of(half, channels, first, p0, p1, count, plain_only):
        weights = row_weights(p0, True)
        _, w, wp, dc = col_parts(p1)
        wd = [w[j] * dc[j] for j in range(3)]
        wpd = [wp[j] * dc[j] for j in range(3)]
        results = []
        for ch in range(first, first + count):
            if ch < plain_only:
                sums = [row_sums(half, channels, 3 * ch + j, (weights[0], weights[2])) for j in range(3)]
                r0, r2 = ([x[t] for x in sums] for t in range(2))
                results.append((dot3(w, r2), dot3(wp, r0)))
                continue
            sums = [row_sums(half, channels, 3 * ch + j, weights) for j in range(3)]
            r0, r1, r2, r3 = ([x[t] for x in sums] for t in range(4))
            results.append(
                dict(
                    nw=dot3(w, r0),
                    dw=dot3(w, r1),
                    nwd=dot3(wd, r0),
                    pw=dot3(w, r2),
                    pdw=dot3(w, r3),
                    pwd=dot3(wd, r2),
                    nwp=dot3(wp, r0),
                    dwp=dot3(wp, r1),
                    nwpd=dot3(wpd, r0),
                )
            )
        return results

    def save_slopes(k):
        for half in range(2):
            at = pl.ds(8 * half, 8)
            found = slopes_of(half, 2, 0, st[k, 0, at], st[k, 1, at], 2, 0)
            for a, t in enumerate(found):
                for i, name in enumerate(("pw", "pdw", "pwd", "nwp", "dwp", "nwpd")):
                    value = t[name]
                    if name in ("pdw", "nwpd"):
                        value = value + t["nw"]
                    tsave[k, 6 + 6 * a + i, at] = value

    def pull_gather(k, v, x, adj):
        gf = [adj[8 + i] for i in range(4)]
        p0, p1 = adj[0], adj[1]
        for a in range(2):
            pw, pdw, pwd, nwp, dwp, nwpd = (tsave[k, 6 + 6 * a + i] for i in range(6))
            p0 = p0 - (v[a] * pw + x[2 * a] * pdw + x[2 * a + 1] * pwd)
            p1 = p1 - (v[a] * nwp + x[2 * a] * dwp + x[2 * a + 1] * nwpd)
        adj[0] = p0
        adj[1] = p1
        c = [tsave[k, 2 + i] for i in range(4)]
        for b in range(2):
            for j in range(2):
                adj[8 + 2 * b + j] = gf[2 * b + j] + DT * (c[b] * gf[j] + c[2 + b] * gf[2 + j])

    def pull_scatter(k, role, adj):
        for half in range(2):
            at = pl.ds(8 * half, 8)
            alive = raw[role, 12, at]
            p0, p1 = st[k, 0, at], st[k, 1, at]
            mass, px, py = slopes_of(half, 3, 0, p0, p1, 3, 1)
            a_mat = [amat[k, i, at] for i in range(4)]
            g0 = adj[0, at] - alive * mass[0]
            g1 = adj[1, at] - alive * mass[1]
            back = []
            for a, t in enumerate((px, py)):
                moved = alive * st[k, 2 + a, at]
                a0, a1 = a_mat[2 * a], a_mat[2 * a + 1]
                g0 = g0 - (moved * t["pw"] + a0 * (t["pdw"] + t["nw"]) + a1 * t["pwd"])
                g1 = g1 - (moved * t["nwp"] + a0 * t["dwp"] + a1 * (t["nwpd"] + t["nw"]))
                adj[2 + a, at] = alive * t["nw"]
                back += [alive * t["dw"], alive * t["nwd"]]
            adj[0, at] = g0
            adj[1, at] = g1
            for i in range(4):
                adj[4 + i, at] = back[i]
            f00, f01, f10, f11 = (st[k, 8 + i, at] for i in range(4))
            sxx, syy = -0.4 * back[0], -0.4 * back[3]
            sxy = -0.4 * (back[1] + back[2])
            jac = f00 * f11 - f01 * f10
            gj = (sxx + syy) * (2.0 * (2.0 * jac - 1.0))
            adj[8, at] = adj[8, at] + (4.0 * f00 * sxx + 2.0 * f10 * sxy + gj * f11)
            adj[9, at] = adj[9, at] + (4.0 * f01 * sxx + 2.0 * f11 * sxy - gj * f10)
            adj[10, at] = adj[10, at] + (4.0 * f10 * syy + 2.0 * f00 * sxy - gj * f01)
            adj[11, at] = adj[11, at] + (4.0 * f11 * syy + 2.0 * f01 * sxy + gj * f00)

    def grid_column(k):
        return lambda ch, i: vg[k, ch, :, pl.ds(i * 128, 128)]

    def part_column(part):
        return lambda ch, i: part[ch, :, pl.ds(i * 128, 128)]

    def forward_front(k, role):
        prepare_forward(k, role)
        build_hot(k)
        scatter(k, forward_channels())

    def forward_back(k, e, part, store_state):
        grid_velocity(k, e, part)
        gather(k, grid_column(k), 2)
        advance(k, store_state)

    part, part_own = parts.at[0], parts.at[1]
    adj, adj_own = adjs.at[0], adjs.at[1]
    last = STEPS - 1

    initial_state(1, OWN)
    forward_front(OWN, 1)
    loads[5].wait()
    loads[6].wait()
    place_force(1)
    combine(3, part_own, 1)
    barrier_wait()
    start_move(RAW)
    pack(0, 3, part_own)
    start_halo(0, 3, to_hosts)
    start_move(FORCE)
    start_move(COT)
    start_halo(7, 3, owners, 0)

    end_move(RAW, raw, 1, 0)
    initial_state(0, 0)
    forward_front(0, 0)
    end_move(FORCE, force, 1, 0)
    place_force(0)
    combine(3, part, 0)
    wait_halo(0, 3, to_hosts)
    forward_back(0, 0, part, True)

    for k in range(1, last):
        forward_front(k, 0)
        combine(3, part, 0)
        pack(k, 3, part)
        start_halo(k, 3, ring)
        save_slopes(k - 1)
        if k == 1:
            wait_halo(7, 3, owners, 0)
            forward_back(OWN, 7, part_own, False)
            save_slopes(OWN)
        wait_halo(k, 3, ring)
        forward_back(k, k, part, True)

    end_move(COT, cot, 1, 0)
    for i in range(12):
        adj[i] = cot[0, i] * raw[0, 12]
    adjoint_rows(last, 15, adj)
    prepare_forward(last, 0)
    build_hot(last)
    scatter(last, forward_channels() + adjoint_channels(15))
    combine(5, part, 0)
    pack(last, 5, part)
    start_halo(last, 5, ring)
    save_slopes(last - 1)
    wait_halo(last, 5, ring)
    forward_back(last, last, part, False)
    save_slopes(last)
    v, x = adjoint_rows(last, 15, adj)
    pull_gather(last, v, x, adj)
    grid_adjoint(last, last, 3, part, True)
    gather(last, part_column(part), 3)
    pull_scatter(last, 0, adj)

    def backward_body(t, carry):
        k = last - 1 - t
        e = last + 1 + t
        v, x = adjoint_rows(k, 15, adj)
        scatter(k, adjoint_channels(15))
        combine(2, part, None)
        pack(e, 2, part)
        start_halo(e, 2, ring)
        pull_gather(k, v, x, adj)
        wait_halo(e, 2, ring)
        grid_adjoint(k, e, 0, part, False)
        gather(k, part_column(part), 3)
        pull_scatter(k, 0, adj)
        return carry

    lax.fori_loop(0, STEPS - 2, backward_body, 0)

    adjoint_rows(0, 15, adj)
    start_move(ADJ)
    scatter(0, adjoint_channels(15))
    combine(2, part, None)
    pack(6, 2, part)
    start_halo(6, 2, to_owners)
    for a in range(2):
        fgmove[0, a] = roll(fgacc[a], -(BC // 2))[2:6]
    start_move(FGRAD)

    end_move(ADJ, adjs, 0, 1)
    v, x = adjoint_rows(OWN, 15, adj_own)
    scatter(OWN, adjoint_channels(15))
    combine(2, part_own, None)
    pull_gather(OWN, v, x, adj_own)
    wait_halo(6, 2, to_owners)
    grid_adjoint(OWN, 6, 0, part_own, True)
    gather(OWN, part_column(part_own), 3)
    pull_scatter(OWN, 1, adj_own)

    sg[0] = adj_own[0] * float(BR)
    sg[1] = adj_own[1] * float(BC)
    for i in range(2, 12):
        sg[i] = adj_own[i]
    end_move(FGRAD, fgmove, 0, 1)
    for a in range(2):
        fg[a] = fgmove[1, a] + roll(fgacc[a], -(BC // 2))[2:6]

    for e in range(EXCHANGES):
        targets = {0: to_hosts, 6: to_owners, 7: owners}.get(e, ring)
        count = 5 if e == last else (2 if e in (4, 5, 6) else 3)
        for copy in copies(e, count, targets, 0 if e == 7 else None):
            copy.wait_send()

    @pl.when(moved)
    def _():
        for copy in moves:
            copy.wait_send()


def per_device(n, offsets, velocity, affine, strain, tile_fill, force_field, cotangent):
    def flat(x):
        return x.reshape(x.shape[0], NB, NP)

    vmem = pl.BlockSpec(memory_space=pltpu.VMEM)
    width = COLS * 128
    state_grad, force_grad = pl.pallas_call(
        functools.partial(kernel, n),
        out_shape=(
            jax.ShapeDtypeStruct((12, NB, NP), F32),
            jax.ShapeDtypeStruct((2, BR, width), F32),
        ),
        in_specs=[pl.BlockSpec(memory_space=pl.ANY)] * 7,
        out_specs=(vmem, vmem),
        scratch_shapes=[
            pltpu.VMEM((1, NB), jnp.int32),
            pltpu.VMEM((2, 13, NB, NP), F32),
            pltpu.VMEM((2, 2, BR, width), F32),
            pltpu.VMEM((2, 12, NB, NP), F32),
            pltpu.VMEM((STEPS + 1, 12, NB, NP), F32),
            pltpu.VMEM((STEPS + 1, 4, NB, NP), F32),
            pltpu.VMEM((STEPS + 1, NB, 128, NP), BF16),
            pltpu.VMEM((32, NB, NP), F32),
            pltpu.VMEM((MAX_CH, COLS, 8, 128), F32),
            pltpu.VMEM((MAX_CH, COLS, 8, 128), F32),
            pltpu.VMEM((2, MAX_CH, 8, width), F32),
            pltpu.VMEM((STEPS + 1, 2, 8, width), F32),
            pltpu.VMEM((STEPS + 1, 8, width), F32),
            pltpu.VMEM((2, 2, 8, width), F32),
            pltpu.VMEM((2 * 72 * 8, 128), F32),
            pltpu.VMEM((STEPS + 1, 18, NB, NP), F32),
            pltpu.VMEM((2, 12, NB, NP), F32),
            pltpu.VMEM((2, 8, width), F32),
            pltpu.VMEM((2, 2, BR, width), F32),
            pltpu.VMEM((EXCHANGES, 2, MAX_CH, 8, width // 2), F32),
            pltpu.VMEM((EXCHANGES, 2, MAX_CH, 8, width // 2), F32),
            pltpu.SemaphoreType.DMA((7,)),
            pltpu.SemaphoreType.DMA((EXCHANGES, 2)),
            pltpu.SemaphoreType.DMA((EXCHANGES, 2)),
            pltpu.SemaphoreType.DMA((5,)),
            pltpu.SemaphoreType.DMA((5,)),
        ],
        compiler_params=pltpu.CompilerParams(collective_id=0, has_side_effects=True),
    )(
        flat(offsets),
        flat(velocity),
        flat(affine),
        flat(strain),
        tile_fill,
        force_field,
        flat(cotangent),
    )
    return state_grad.reshape(12, 1, NB, NP), force_grad


def solution(mesh):
    n = mesh.shape["slab"]
    tiles = P(None, "slab", None, None)
    return jax.shard_map(
        functools.partial(per_device, n),
        mesh=mesh,
        in_specs=(tiles, tiles, tiles, tiles, P("slab", None), P(None, "slab", None), tiles),
        out_specs=(tiles, P(None, "slab", None)),
        check_vma=False,
    )
```

```python
import functools

import jax
import jax.numpy as jnp
from jax import lax
from jax.experimental import pallas as pl
from jax.experimental.pallas import tpu as pltpu
from jax.sharding import PartitionSpec as P

BR = 4
BC = 64
NB = 16
NP = 128
STEPS = 4
COLS = 8
DT = 0.1
F32 = jnp.float32
BF16 = jnp.bfloat16
MESH = pl.DeviceIdType.MESH
SHIFTS = (-1, 0, 1)

EXCHANGES = 8
MAX_CH = 5
OWN = STEPS
RAW, STRAIN, COT, FORCE, RATES, ADJ, FGRAD = range(7)
CHIPS = {64: (4, 4, 4), 8: (2, 2, 2), 4: (1, 2, 2)}


def host_of(band, n):
    _, nx, ny = CHIPS[n // 2]
    core, chip = lax.rem(band, 2), lax.div(band, 2)
    y, x, z = lax.rem(chip, ny), lax.rem(lax.div(chip, ny), nx), lax.div(chip, nx * ny)
    y = y + lax.rem(x, 2) * (ny - 1 - 2 * y)
    x = x + lax.rem(z, 2) * (nx - 1 - 2 * x)
    return ((z * nx + x) * ny + y) * 2 + core


def band_of(device, n):
    _, nx, ny = CHIPS[n // 2]
    core, chip = lax.rem(device, 2), lax.div(device, 2)
    y, x, z = lax.rem(chip, ny), lax.rem(lax.div(chip, ny), nx), lax.div(chip, nx * ny)
    x = x + lax.rem(z, 2) * (nx - 1 - 2 * x)
    y = y + lax.rem(x, 2) * (ny - 1 - 2 * y)
    return ((z * nx + x) * ny + y) * 2 + core


def row_spline(d):
    m = jnp.abs(d)
    t = jnp.maximum(1.5 - m, 0.0)
    near = m < 0.5
    value = jnp.where(near, 0.75 - m * m, 0.5 * t * t)
    return value, t, near


def row_slope(d, t, near):
    return jnp.where(near, -2.0 * d, jnp.where(d > 0.0, -t, t))


def col_center(p1):
    return jnp.floor(p1 + 0.5)


def col_parts(p1):
    c = col_center(p1)
    d0 = c - p1
    lo, hi = 0.5 + d0, 0.5 - d0
    values = (0.5 * lo * lo, 0.75 - d0 * d0, 0.5 * hi * hi)
    slopes = (lo, -2.0 * d0, -hi)
    w, wp, dc = [], [], []
    for s, value, slope in zip(SHIFTS, values, slopes):
        inside = jnp.logical_and(c >= float(-s), c <= float(2 * BC - 1 - s))
        w.append(jnp.where(inside, value, 0.0))
        wp.append(jnp.where(inside, slope, 0.0))
        dc.append(jnp.where(inside, d0 + float(s), 0.0))
    return c, w, wp, dc


def split_rows(x):
    top = x.astype(BF16).astype(F32)
    return jnp.concatenate([top, x - top], axis=0)


def roll(x, by):
    return pltpu.roll(x, by % x.shape[-1], axis=x.ndim - 1)


def kernel(
    n,
    off_hbm,
    vel_hbm,
    aff_hbm,
    strn_hbm,
    fill_hbm,
    force_hbm,
    cot_hbm,
    sg,
    fg,
    fill,
    raw,
    aff,
    strn,
    first,
    rates,
    rest,
    force,
    cot,
    st,
    amat,
    hot,
    qm,
    ev,
    od,
    parts,
    vg,
    inv,
    frc,
    gat,
    tsave,
    adjs,
    fgacc,
    fgmove,
    send,
    recv,
    load_sem,
    send_sem,
    recv_sem,
    move_send,
    move_recv,
):
    me = lax.axis_index("slab")
    band = band_of(me, n)
    home = host_of(me, n)
    moved = home != me
    stays = home == me

    def after(i):
        return lax.rem(i + 1, n)

    def before(i):
        return lax.rem(i + n - 1, n)

    ring = (host_of(after(band), n), host_of(before(band), n))
    to_hosts = (host_of(after(me), n), host_of(before(me), n))
    to_owners = (after(band), before(band))
    owners = (after(me), before(me))

    loads = [
        pltpu.make_async_copy(src, dst, load_sem.at[i])
        for i, (src, dst) in enumerate(
            (
                (off_hbm, raw.at[pl.ds(0, 2)]),
                (vel_hbm, raw.at[pl.ds(2, 2)]),
                (aff_hbm, aff),
                (strn_hbm, strn.at[1]),
                (fill_hbm, fill),
                (force_hbm, force.at[1]),
                (cot_hbm, cot.at[1]),
            )
        )
    ]
    for load in loads:
        load.start()

    barrier = pltpu.get_barrier_semaphore()
    for other in ring + to_hosts + to_owners + owners:
        pl.semaphore_signal(barrier, inc=1, device_id=(other,), device_id_type=MESH)

    @pl.when(moved)
    def _():
        pl.semaphore_signal(barrier, inc=1, device_id=(home,), device_id_type=MESH)
        pl.semaphore_signal(barrier, inc=1, device_id=(band,), device_id_type=MESH)

    def barrier_wait():
        @pl.when(moved)
        def _():
            pl.semaphore_wait(barrier, 10)

        @pl.when(stays)
        def _():
            pl.semaphore_wait(barrier, 8)

    def move(which, src, dst, device):
        return pltpu.make_async_remote_copy(
            src_ref=src,
            dst_ref=dst,
            send_sem=move_send.at[which],
            recv_sem=move_recv.at[which],
            device_id=(device,),
            device_id_type=MESH,
        )

    moves = [
        move(RAW, first.at[1], first.at[0], home),
        move(STRAIN, strn.at[1], strn.at[0], home),
        move(COT, cot.at[1], cot.at[0], home),
        move(FORCE, force.at[1], force.at[0], home),
        move(RATES, rates.at[0], rates.at[1], band),
        move(ADJ, rest.at[0], rest.at[1], band),
        move(FGRAD, fgmove.at[0], fgmove.at[1], band),
    ]

    def start_move(which):
        @pl.when(moved)
        def _():
            moves[which].start()

    def end_move(which, ref, src, dst):
        @pl.when(moved)
        def _():
            moves[which].wait_recv()

        @pl.when(stays)
        def _():
            ref[dst] = ref[src]

    lane16 = lax.broadcasted_iota(jnp.int32, (16, 128), 1)
    sub8 = lax.broadcasted_iota(jnp.int32, (8, 128), 0)
    lane8 = lax.broadcasted_iota(jnp.int32, (8, 128), 1)
    rows8 = sub8.astype(F32)
    top_half = sub8 < 4
    left_half = lane8 < 64

    def load_state():
        for i, value in enumerate(
            (BR // 2 + BR * raw[0], BC // 2 + BC * raw[1], raw[2], raw[3])
        ):
            st[OWN, i] = value
            first[1, i] = value
        for i in range(4):
            st[OWN, 4 + i] = aff[i]
            st[OWN, 8 + i] = strn[1, i] + (1.0 if i in (0, 3) else 0.0)

    def host_state():
        for i in range(4):
            st[0, i] = first[0, i]
            amat[0, i] = first[0, 5 + i]

    def place_force(role):
        for a in range(2):
            rows = DT * force[role, a]
            zero = jnp.zeros((2, COLS * 128), F32)
            frc[role, a] = roll(jnp.concatenate([zero, rows, zero], axis=0), BC // 2)

    for i in (4, 0, 1, 2, 3):
        loads[i].wait()
    eye = lax.broadcasted_iota(jnp.int32, (16, 16), 0) == lax.broadcasted_iota(jnp.int32, (16, 16), 1)
    fills = jnp.where(eye, jnp.broadcast_to(fill[...].astype(F32), (16, 16)), 0.0)
    count = jnp.sum(fills, axis=1, keepdims=True)
    first[1, 4] = jnp.where(lane16.astype(F32) < count, 1.0, 0.0)

    def stress_matrix(k, role):
        alive = first[role, 4]
        f00, f01, f10, f11 = (st[k, 8 + i] for i in range(4))
        jac = f00 * f11 - f01 * f10
        pressure = 2.0 * (jac - 1.0) * jac
        sxx = 2.0 * (f00 * f00 + f01 * f01 - 1.0) + pressure
        sxy = 2.0 * (f00 * f10 + f01 * f11)
        syy = 2.0 * (f10 * f10 + f11 * f11 - 1.0) + pressure
        tau = (sxx, sxy, sxy, syy)
        for i in range(4):
            value = alive * (-0.4 * tau[i] + st[k, 4 + i])
            amat[k, i] = value
            if k is OWN:
                first[1, 5 + i] = value

    def prepare_forward(k, role):
        alive = first[role, 4]
        p1 = st[k, 1]
        a_mat = [amat[k, i] for i in range(4)]
        c, w, _, dc = col_parts(p1)
        moved = (alive * st[k, 2], alive * st[k, 3])
        for j in range(3):
            wd = w[j] * dc[j]
            qm[j] = w[j] * alive
            for a in range(2):
                qm[3 + 3 * a + j] = w[j] * moved[a] + wd * a_mat[2 * a + 1]
                qm[9 + 3 * a + j] = w[j] * a_mat[2 * a]
        qm[30] = st[k, 0]
        qm[31] = jnp.where(c < 0.0, c + 128.0, jnp.where(c > 127.0, c - 128.0, c))

    def build_hot(k):
        nodes = lax.broadcasted_iota(jnp.int32, (128, 128), 0).astype(F32)
        for b in range(NB):
            row = qm[31, pl.ds(b, 1), :]
            hot[k, b] = jnp.where(nodes == jnp.broadcast_to(row, (128, 128)), 1.0, 0.0).astype(BF16)

    def adjoint_rows(k, base, adj):
        f00, f01, f10, f11 = (st[k, 8 + i] for i in range(4))
        gf = [adj[8 + i] for i in range(4)]
        v = [adj[2 + a] + DT * adj[a] for a in range(2)]
        x = []
        for a in range(2):
            g0, g1 = gf[2 * a], gf[2 * a + 1]
            x.append(4.0 * (adj[4 + 2 * a] + DT * (g0 * f00 + g1 * f01)))
            x.append(4.0 * (adj[5 + 2 * a] + DT * (g0 * f10 + g1 * f11)))
        _, w, _, dc = col_parts(st[k, 1])
        for j in range(3):
            wd = w[j] * dc[j]
            for a in range(2):
                qm[base + 3 * a + j] = w[j] * v[a] + wd * x[2 * a + 1]
                qm[base + 6 + 3 * a + j] = w[j] * x[2 * a]
        qm[30] = st[k, 0]
        return v, x

    def rate_rows(k):
        v = [rates[1, a] for a in range(2)]
        x = [rates[1, 2 + i] for i in range(4)]
        _, w, _, dc = col_parts(st[k, 1])
        for j in range(3):
            wd = w[j] * dc[j]
            for a in range(2):
                qm[15 + 3 * a + j] = w[j] * v[a] + wd * x[2 * a + 1]
                qm[21 + 3 * a + j] = w[j] * x[2 * a]
        qm[30] = st[k, 0]

    def scatter(k, rows):
        for b in range(NB):
            d = rows8 - jnp.broadcast_to(qm[30, pl.ds(b, 1), :], (8, 128))
            nr, _, _ = row_spline(d)
            nd = nr * d
            pieces = []
            for channel in rows:
                for q, m in channel:
                    x = nr * jnp.broadcast_to(qm[q, pl.ds(b, 1), :], (8, 128))
                    if m is not None:
                        x = x + nd * jnp.broadcast_to(qm[m, pl.ds(b, 1), :], (8, 128))
                    pieces.append(split_rows(x))
            lhs = jnp.concatenate(pieces, axis=0).astype(BF16)
            out = lax.dot_general(
                lhs, hot[k, b], (((1,), (1,)), ((), ())), preferred_element_type=F32
            )
            target = ev if b % 2 == 0 else od
            for ch in range(len(rows)):
                total = None
                for j, s in enumerate(SHIFTS):
                    at = (3 * ch + j) * 16
                    value = out[at : at + 8] + out[at + 8 : at + 16]
                    if s:
                        value = roll(value, s)
                    total = value if total is None else total + value
                if b % 2:
                    total = roll(total, 64)
                target[ch, b // 2] = total

    def forward_channels():
        return [[(j, None) for j in range(3)]] + [
            [(3 + 3 * a + j, 9 + 3 * a + j) for j in range(3)] for a in range(2)
        ]

    def adjoint_channels(base):
        return [[(base + 3 * a + j, base + 6 + 3 * a + j) for j in range(3)] for a in range(2)]

    def combine(count, part, force_role):
        for ch in range(count):
            for i in range(COLS):
                value = ev[ch, i] + jnp.where(left_half, od[ch, (i - 1) % COLS], od[ch, i])
                if force_role is not None and ch in (1, 2):
                    value = value + frc[force_role, ch - 1, :, pl.ds(i * 128, 128)]
                part[ch, :, pl.ds(i * 128, 128)] = value

    def pack(e, count, part):
        for ch in range(count):
            for i in range(COLS // 2):
                a = part[ch, :, pl.ds(2 * i * 128, 128)]
                b = part[ch, :, pl.ds((2 * i + 1) * 128, 128)]
                down = jnp.where(top_half, pltpu.roll(a, 4, axis=0), b)
                up = jnp.where(top_half, a, pltpu.roll(b, 4, axis=0))
                send[e, 0, ch, :, pl.ds(i * 128, 128)] = down
                send[e, 1, ch, :, pl.ds(i * 128, 128)] = up

    def copies(e, count, targets, source=None):
        return [
            pltpu.make_async_remote_copy(
                src_ref=send.at[e if source is None else source, side, pl.ds(0, count)],
                dst_ref=recv.at[e, side, pl.ds(0, count)],
                send_sem=send_sem.at[e, side],
                recv_sem=recv_sem.at[e, side],
                device_id=(other,),
                device_id_type=MESH,
            )
            for side, other in enumerate(targets)
        ]

    def start_halo(e, count, targets, source=None):
        for copy in copies(e, count, targets, source):
            copy.start()

    def summed(e, part, ch, i):
        above = recv[e, 0, ch, :, pl.ds(i * 128, 128)]
        below = recv[e, 1, ch, :, pl.ds(i * 128, 128)]
        first = jnp.where(top_half, above, pltpu.roll(below, 4, axis=0))
        second = jnp.where(top_half, pltpu.roll(above, 4, axis=0), below)
        return (
            part[ch, :, pl.ds(2 * i * 128, 128)] + first,
            part[ch, :, pl.ds((2 * i + 1) * 128, 128)] + second,
        )

    def wait_halo(e, count, targets, source=None):
        for copy in copies(e, count, targets, source):
            copy.wait_recv()

    def grid_velocity(k, e, part):
        for i in range(COLS // 2):
            mass = summed(e, part, 0, i)
            mom = [summed(e, part, 1 + a, i) for a in range(2)]
            for h in range(2):
                at = pl.ds((2 * i + h) * 128, 128)
                inverse = 1.0 / (mass[h] + 0.25)
                inv[k, :, at] = inverse
                for a in range(2):
                    vg[k, a, :, at] = mom[a][h] * inverse

    def grid_adjoint(k, e, base, part, first):
        for i in range(COLS // 2):
            u = [summed(e, part, base + a, i) for a in range(2)]
            for h in range(2):
                at = pl.ds((2 * i + h) * 128, 128)
                inverse = inv[k, :, at]
                total = u[0][h] * vg[k, 0, :, at] + u[1][h] * vg[k, 1, :, at]
                part[0, :, at] = -total * inverse
                for a in range(2):
                    value = u[a][h] * inverse
                    part[1 + a, :, at] = value
                    fgacc[a, :, at] = DT * value if first else fgacc[a, :, at] + DT * value

    def gather(k, column, channels):
        stride = 3 * channels * 64
        for b in range(NB):
            i = b // 2
            pieces = []
            for ch in range(channels):
                window = column(ch, i)
                if b % 2:
                    window = roll(jnp.where(left_half, column(ch, (i + 1) % COLS), window), 64)
                for s in SHIFTS:
                    pieces.append(split_rows(roll(window, -s) if s else window))
            lhs = jnp.concatenate(pieces, axis=0).astype(BF16)
            out = jnp.dot(lhs, hot[k, b], preferred_element_type=F32)
            for q in range(3 * channels):
                value = out[16 * q : 16 * q + 8] + out[16 * q + 8 : 16 * q + 16]
                gat[pl.ds((b // 8) * stride + q * 64 + b % 8, 8, stride=8), :] = value

    def gathered(half, channels, q, r):
        return gat[pl.ds(half * 3 * channels * 64 + q * 64 + r * 8, 8), :]

    def row_sums(half, channels, q, weights):
        totals = [None] * len(weights)
        for r in range(2 * BR):
            g = gathered(half, channels, q, r)
            for t, weight in enumerate(weights):
                value = weight[r] * g
                totals[t] = value if totals[t] is None else totals[t] + value
        return totals

    def dot3(a, b):
        return a[0] * b[0] + a[1] * b[1] + a[2] * b[2]

    def row_weights(p0, slopes):
        plain, slant, slope, slope_d = [], [], [], []
        for r in range(2 * BR):
            d = float(r) - p0
            value, t, near = row_spline(d)
            plain.append(value)
            slant.append(value * d)
            if slopes:
                der = row_slope(d, t, near)
                slope.append(der)
                slope_d.append(der * d)
        return (plain, slant, slope, slope_d) if slopes else (plain, slant)

    def advance(k, store_state):
        for half in range(2):
            at = pl.ds(8 * half, 8)
            p0, p1 = st[k, 0, at], st[k, 1, at]
            weights = row_weights(p0, False)
            _, w, _, dc = col_parts(p1)
            wd = [w[j] * dc[j] for j in range(3)]
            new_v, new_c = [], []
            for a in range(2):
                sums = [row_sums(half, 2, 3 * a + j, weights) for j in range(3)]
                r0 = [x[0] for x in sums]
                r1 = [x[1] for x in sums]
                new_v.append(dot3(w, r0))
                new_c.append(4.0 * dot3(w, r1))
                new_c.append(4.0 * dot3(wd, r0))
            for a in range(2):
                tsave[k, a, at] = new_v[a]
            for i in range(4):
                tsave[k, 2 + i, at] = new_c[i]
            if store_state:
                f = [st[k, 8 + i, at] for i in range(4)]
                st[k + 1, 0, at] = p0 + DT * new_v[0]
                st[k + 1, 1, at] = p1 + DT * new_v[1]
                for a in range(2):
                    st[k + 1, 2 + a, at] = new_v[a]
                for i in range(4):
                    st[k + 1, 4 + i, at] = new_c[i]
                for a in range(2):
                    c0, c1 = DT * new_c[2 * a], DT * new_c[2 * a + 1]
                    for j in range(2):
                        st[k + 1, 8 + 2 * a + j, at] = f[2 * a + j] + (c0 * f[j] + c1 * f[2 + j])

    def slopes_of(half, channels, first, p0, p1, count, plain_only):
        weights = row_weights(p0, True)
        _, w, wp, dc = col_parts(p1)
        wd = [w[j] * dc[j] for j in range(3)]
        wpd = [wp[j] * dc[j] for j in range(3)]
        results = []
        for ch in range(first, first + count):
            if ch < plain_only:
                sums = [row_sums(half, channels, 3 * ch + j, (weights[0], weights[2])) for j in range(3)]
                r0, r2 = ([x[t] for x in sums] for t in range(2))
                results.append((dot3(w, r2), dot3(wp, r0)))
                continue
            sums = [row_sums(half, channels, 3 * ch + j, weights) for j in range(3)]
            r0, r1, r2, r3 = ([x[t] for x in sums] for t in range(4))
            results.append(
                dict(
                    nw=dot3(w, r0),
                    dw=dot3(w, r1),
                    nwd=dot3(wd, r0),
                    pw=dot3(w, r2),
                    pdw=dot3(w, r3),
                    pwd=dot3(wd, r2),
                    nwp=dot3(wp, r0),
                    dwp=dot3(wp, r1),
                    nwpd=dot3(wpd, r0),
                )
            )
        return results

    def save_slopes(k):
        for half in range(2):
            at = pl.ds(8 * half, 8)
            found = slopes_of(half, 2, 0, st[k, 0, at], st[k, 1, at], 2, 0)
            for a, t in enumerate(found):
                for i, name in enumerate(("pw", "pdw", "pwd", "nwp", "dwp", "nwpd")):
                    value = t[name]
                    if name in ("pdw", "nwpd"):
                        value = value + t["nw"]
                    tsave[k, 6 + 6 * a + i, at] = value

    def pull_gather(k, v, x, adj):
        gf = [adj[8 + i] for i in range(4)]
        p0, p1 = adj[0], adj[1]
        for a in range(2):
            pw, pdw, pwd, nwp, dwp, nwpd = (tsave[k, 6 + 6 * a + i] for i in range(6))
            p0 = p0 - (v[a] * pw + x[2 * a] * pdw + x[2 * a + 1] * pwd)
            p1 = p1 - (v[a] * nwp + x[2 * a] * dwp + x[2 * a + 1] * nwpd)
        adj[0] = p0
        adj[1] = p1
        c = [tsave[k, 2 + i] for i in range(4)]
        for b in range(2):
            for j in range(2):
                adj[8 + 2 * b + j] = gf[2 * b + j] + DT * (c[b] * gf[j] + c[2 + b] * gf[2 + j])

    def pull_scatter(k, role, adj):
        for half in range(2):
            at = pl.ds(8 * half, 8)
            alive = first[role, 4, at]
            p0, p1 = st[k, 0, at], st[k, 1, at]
            mass, px, py = slopes_of(half, 3, 0, p0, p1, 3, 1)
            a_mat = [amat[k, i, at] for i in range(4)]
            g0 = adj[0, at] - alive * mass[0]
            g1 = adj[1, at] - alive * mass[1]
            back = []
            for a, t in enumerate((px, py)):
                moved = alive * st[k, 2 + a, at]
                a0, a1 = a_mat[2 * a], a_mat[2 * a + 1]
                g0 = g0 - (moved * t["pw"] + a0 * (t["pdw"] + t["nw"]) + a1 * t["pwd"])
                g1 = g1 - (moved * t["nwp"] + a0 * t["dwp"] + a1 * (t["nwpd"] + t["nw"]))
                adj[2 + a, at] = alive * t["nw"]
                back += [alive * t["dw"], alive * t["nwd"]]
            adj[0, at] = g0
            adj[1, at] = g1
            for i in range(4):
                adj[4 + i, at] = back[i]
            f00, f01, f10, f11 = (st[k, 8 + i, at] for i in range(4))
            sxx, syy = -0.4 * back[0], -0.4 * back[3]
            sxy = -0.4 * (back[1] + back[2])
            jac = f00 * f11 - f01 * f10
            gj = (sxx + syy) * (2.0 * (2.0 * jac - 1.0))
            adj[8, at] = adj[8, at] + (4.0 * f00 * sxx + 2.0 * f10 * sxy + gj * f11)
            adj[9, at] = adj[9, at] + (4.0 * f01 * sxx + 2.0 * f11 * sxy - gj * f10)
            adj[10, at] = adj[10, at] + (4.0 * f10 * syy + 2.0 * f00 * sxy - gj * f01)
            adj[11, at] = adj[11, at] + (4.0 * f11 * syy + 2.0 * f01 * sxy + gj * f00)

    def grid_column(k):
        return lambda ch, i: vg[k, ch, :, pl.ds(i * 128, 128)]

    def part_column(part):
        return lambda ch, i: part[ch, :, pl.ds(i * 128, 128)]

    def forward_front(k, role):
        if k or role:
            stress_matrix(k, role)
        prepare_forward(k, role)
        build_hot(k)
        scatter(k, forward_channels())

    def forward_back(k, e, part, store_state):
        grid_velocity(k, e, part)
        gather(k, grid_column(k), 2)
        advance(k, store_state)

    part, part_own = parts.at[0], parts.at[1]
    adj, adj_own = adjs.at[0], adjs.at[1]
    last = STEPS - 1

    load_state()
    forward_front(OWN, 1)
    loads[5].wait()
    loads[6].wait()
    place_force(1)
    combine(3, part_own, 1)
    barrier_wait()
    start_move(RAW)
    pack(0, 3, part_own)
    start_halo(0, 3, to_hosts)
    start_move(FORCE)
    start_move(STRAIN)
    start_move(COT)
    start_halo(7, 3, owners, 0)

    end_move(RAW, first, 1, 0)
    host_state()
    forward_front(0, 0)
    end_move(FORCE, force, 1, 0)
    place_force(0)
    combine(3, part, 0)
    wait_halo(0, 3, to_hosts)
    end_move(STRAIN, strn, 1, 0)
    for i in range(4):
        st[0, 8 + i] = strn[0, i] + (1.0 if i in (0, 3) else 0.0)
    forward_back(0, 0, part, True)

    for k in range(1, last):
        forward_front(k, 0)
        combine(3, part, 0)
        pack(k, 3, part)
        start_halo(k, 3, ring)
        save_slopes(k - 1)
        if k == 1:
            wait_halo(7, 3, owners, 0)
            grid_velocity(OWN, 7, part_own)
        wait_halo(k, 3, ring)
        forward_back(k, k, part, True)

    end_move(COT, cot, 1, 0)
    for i in range(12):
        adj[i] = cot[0, i] * first[0, 4]
    adjoint_rows(last, 15, adj)
    stress_matrix(last, 0)
    prepare_forward(last, 0)
    build_hot(last)
    scatter(last, forward_channels() + adjoint_channels(15))
    combine(5, part, 0)
    pack(last, 5, part)
    start_halo(last, 5, ring)
    save_slopes(last - 1)
    wait_halo(last, 5, ring)
    forward_back(last, last, part, False)
    save_slopes(last)
    v, x = adjoint_rows(last, 15, adj)
    pull_gather(last, v, x, adj)
    grid_adjoint(last, last, 3, part, True)
    gather(last, part_column(part), 3)
    pull_scatter(last, 0, adj)

    def backward_body(t, carry):
        k = last - 1 - t
        e = last + 1 + t
        v, x = adjoint_rows(k, 15, adj)
        scatter(k, adjoint_channels(15))
        combine(2, part, None)
        pack(e, 2, part)
        start_halo(e, 2, ring)
        pull_gather(k, v, x, adj)
        wait_halo(e, 2, ring)
        grid_adjoint(k, e, 0, part, False)
        gather(k, part_column(part), 3)
        pull_scatter(k, 0, adj)
        return carry

    lax.fori_loop(0, STEPS - 2, backward_body, 0)

    v, x = adjoint_rows(0, 15, adj)
    for i, value in enumerate(v + x):
        rates[0, i] = value
    scatter(0, adjoint_channels(15))
    start_move(RATES)
    combine(2, part, None)
    pack(6, 2, part)
    start_halo(6, 2, to_owners)
    pull_gather(0, v, x, adj)
    for i in range(6):
        rest[0, i] = adj[i if i < 2 else 6 + i]
    for a in range(2):
        fgmove[0, a] = roll(fgacc[a], -(BC // 2))[2:6]
    start_move(ADJ)
    start_move(FGRAD)

    end_move(RATES, rates, 0, 1)
    rate_rows(OWN)
    scatter(OWN, adjoint_channels(15))
    combine(2, part_own, None)
    wait_halo(6, 2, to_owners)
    grid_adjoint(OWN, 6, 0, part_own, True)
    gather(OWN, part_column(part_own), 3)
    end_move(ADJ, rest, 0, 1)
    for i in range(6):
        adj_own[i if i < 2 else 6 + i] = rest[1, i]
    pull_scatter(OWN, 1, adj_own)

    sg[0] = adj_own[0] * float(BR)
    sg[1] = adj_own[1] * float(BC)
    for i in range(2, 12):
        sg[i] = adj_own[i]
    end_move(FGRAD, fgmove, 0, 1)
    for a in range(2):
        fg[a] = fgmove[1, a] + roll(fgacc[a], -(BC // 2))[2:6]

    for e in range(EXCHANGES):
        targets = {0: to_hosts, 6: to_owners, 7: owners}.get(e, ring)
        count = 5 if e == last else (2 if e in (4, 5, 6) else 3)
        for copy in copies(e, count, targets, 0 if e == 7 else None):
            copy.wait_send()

    @pl.when(moved)
    def _():
        for copy in moves:
            copy.wait_send()


def per_device(n, offsets, velocity, affine, strain, tile_fill, force_field, cotangent):
    def flat(x):
        return x.reshape(x.shape[0], NB, NP)

    vmem = pl.BlockSpec(memory_space=pltpu.VMEM)
    width = COLS * 128
    state_grad, force_grad = pl.pallas_call(
        functools.partial(kernel, n),
        out_shape=(
            jax.ShapeDtypeStruct((12, NB, NP), F32),
            jax.ShapeDtypeStruct((2, BR, width), F32),
        ),
        in_specs=[pl.BlockSpec(memory_space=pltpu.HBM)] * 7,
        out_specs=(vmem, vmem),
        scratch_shapes=[
            pltpu.VMEM((1, NB), jnp.int32),
            pltpu.VMEM((4, NB, NP), F32),
            pltpu.VMEM((4, NB, NP), F32),
            pltpu.VMEM((2, 4, NB, NP), F32),
            pltpu.VMEM((2, 9, NB, NP), F32),
            pltpu.VMEM((2, 6, NB, NP), F32),
            pltpu.VMEM((2, 6, NB, NP), F32),
            pltpu.VMEM((2, 2, BR, width), F32),
            pltpu.VMEM((2, 12, NB, NP), F32),
            pltpu.VMEM((STEPS + 1, 12, NB, NP), F32),
            pltpu.VMEM((STEPS + 1, 4, NB, NP), F32),
            pltpu.VMEM((STEPS + 1, NB, 128, NP), BF16),
            pltpu.VMEM((32, NB, NP), F32),
            pltpu.VMEM((MAX_CH, COLS, 8, 128), F32),
            pltpu.VMEM((MAX_CH, COLS, 8, 128), F32),
            pltpu.VMEM((2, MAX_CH, 8, width), F32),
            pltpu.VMEM((STEPS + 1, 2, 8, width), F32),
            pltpu.VMEM((STEPS + 1, 8, width), F32),
            pltpu.VMEM((2, 2, 8, width), F32),
            pltpu.VMEM((2 * 72 * 8, 128), F32),
            pltpu.VMEM((STEPS + 1, 18, NB, NP), F32),
            pltpu.VMEM((2, 12, NB, NP), F32),
            pltpu.VMEM((2, 8, width), F32),
            pltpu.VMEM((2, 2, BR, width), F32),
            pltpu.VMEM((EXCHANGES, 2, MAX_CH, 8, width // 2), F32),
            pltpu.VMEM((EXCHANGES, 2, MAX_CH, 8, width // 2), F32),
            pltpu.SemaphoreType.DMA((7,)),
            pltpu.SemaphoreType.DMA((EXCHANGES, 2)),
            pltpu.SemaphoreType.DMA((EXCHANGES, 2)),
            pltpu.SemaphoreType.DMA((7,)),
            pltpu.SemaphoreType.DMA((7,)),
        ],
        compiler_params=pltpu.CompilerParams(collective_id=0, has_side_effects=True),
    )(
        flat(offsets),
        flat(velocity),
        flat(affine),
        flat(strain),
        tile_fill,
        force_field,
        flat(cotangent),
    )
    return state_grad.reshape(12, 1, NB, NP), force_grad


def solution(mesh):
    n = mesh.shape["slab"]
    tiles = P(None, "slab", None, None)
    return jax.shard_map(
        functools.partial(per_device, n),
        mesh=mesh,
        in_specs=(tiles, tiles, tiles, tiles, P("slab", None), P(None, "slab", None), tiles),
        out_specs=(tiles, P(None, "slab", None)),
        check_vma=False,
    )
```

```python
import functools

import jax
import jax.numpy as jnp
from jax import lax
from jax.experimental import pallas as pl
from jax.experimental.pallas import tpu as pltpu
from jax.sharding import PartitionSpec as P

BR = 4
BC = 64
NB = 16
NP = 128
STEPS = 4
COLS = 8
DT = 0.1
F32 = jnp.float32
BF16 = jnp.bfloat16
MESH = pl.DeviceIdType.MESH
SHIFTS = (-1, 0, 1)

EXCHANGES = 8
MAX_CH = 5
CHUNKS = 2
SCATTER_BLOCKS = ((15, 0, 1, 2, 3, 4, 5, 6, 7), (8, 9, 10, 11, 12, 13, 14))
GATHER_BLOCKS = ((0, 1, 2, 3, 4, 5, 6), (7, 8, 9, 10, 11, 12, 13, 14, 15))
CHUNK_COLS = ((0, 1, 2, 3), (4, 5, 6, 7))
OWN = STEPS
RAW, STRAIN, COT, FORCE, RATES, ADJ, FGRAD = range(7)
CHIPS = {64: (4, 4, 4), 8: (2, 2, 2), 4: (1, 2, 2)}


def host_of(band, n):
    _, nx, ny = CHIPS[n // 2]
    core, chip = lax.rem(band, 2), lax.div(band, 2)
    y, x, z = lax.rem(chip, ny), lax.rem(lax.div(chip, ny), nx), lax.div(chip, nx * ny)
    y = y + lax.rem(x, 2) * (ny - 1 - 2 * y)
    x = x + lax.rem(z, 2) * (nx - 1 - 2 * x)
    return ((z * nx + x) * ny + y) * 2 + core


def band_of(device, n):
    _, nx, ny = CHIPS[n // 2]
    core, chip = lax.rem(device, 2), lax.div(device, 2)
    y, x, z = lax.rem(chip, ny), lax.rem(lax.div(chip, ny), nx), lax.div(chip, nx * ny)
    x = x + lax.rem(z, 2) * (nx - 1 - 2 * x)
    y = y + lax.rem(x, 2) * (ny - 1 - 2 * y)
    return ((z * nx + x) * ny + y) * 2 + core


def row_spline(d):
    m = jnp.abs(d)
    t = jnp.maximum(1.5 - m, 0.0)
    near = m < 0.5
    value = jnp.where(near, 0.75 - m * m, 0.5 * t * t)
    return value, t, near


def row_slope(d, t, near):
    return jnp.where(near, -2.0 * d, jnp.where(d > 0.0, -t, t))


def col_center(p1):
    return jnp.floor(p1 + 0.5)


def col_parts(p1):
    c = col_center(p1)
    d0 = c - p1
    lo, hi = 0.5 + d0, 0.5 - d0
    values = (0.5 * lo * lo, 0.75 - d0 * d0, 0.5 * hi * hi)
    slopes = (lo, -2.0 * d0, -hi)
    w, wp, dc = [], [], []
    for s, value, slope in zip(SHIFTS, values, slopes):
        inside = jnp.logical_and(c >= float(-s), c <= float(2 * BC - 1 - s))
        w.append(jnp.where(inside, value, 0.0))
        wp.append(jnp.where(inside, slope, 0.0))
        dc.append(jnp.where(inside, d0 + float(s), 0.0))
    return c, w, wp, dc


def split_rows(x):
    top = x.astype(BF16).astype(F32)
    return jnp.concatenate([top, x - top], axis=0)


def roll(x, by):
    return pltpu.roll(x, by % x.shape[-1], axis=x.ndim - 1)


def kernel(
    n,
    off_hbm,
    vel_hbm,
    aff_hbm,
    strn_hbm,
    fill_hbm,
    force_hbm,
    cot_hbm,
    sg,
    fg,
    fill,
    raw,
    aff,
    strn,
    first,
    rates,
    rest,
    force,
    cot,
    st,
    amat,
    hot,
    qm,
    ev,
    od,
    parts,
    vg,
    inv,
    frc,
    gat,
    tsave,
    adjs,
    fgacc,
    fgmove,
    send,
    recv,
    load_sem,
    send_sem,
    recv_sem,
    move_send,
    move_recv,
):
    me = lax.axis_index("slab")
    band = band_of(me, n)
    home = host_of(me, n)
    moved = home != me
    stays = home == me

    def after(i):
        return lax.rem(i + 1, n)

    def before(i):
        return lax.rem(i + n - 1, n)

    ring = (host_of(after(band), n), host_of(before(band), n))
    to_hosts = (host_of(after(me), n), host_of(before(me), n))
    to_owners = (after(band), before(band))
    owners = (after(me), before(me))

    loads = [
        pltpu.make_async_copy(src, dst, load_sem.at[i])
        for i, (src, dst) in enumerate(
            (
                (off_hbm, raw.at[pl.ds(0, 2)]),
                (vel_hbm, raw.at[pl.ds(2, 2)]),
                (aff_hbm, aff),
                (strn_hbm, strn.at[1]),
                (fill_hbm, fill),
                (force_hbm, force.at[1]),
                (cot_hbm, cot.at[1]),
            )
        )
    ]
    for load in loads:
        load.start()

    barrier = pltpu.get_barrier_semaphore()
    for other in ring + to_hosts + to_owners + owners:
        pl.semaphore_signal(barrier, inc=1, device_id=(other,), device_id_type=MESH)

    @pl.when(moved)
    def _():
        pl.semaphore_signal(barrier, inc=1, device_id=(home,), device_id_type=MESH)
        pl.semaphore_signal(barrier, inc=1, device_id=(band,), device_id_type=MESH)

    def barrier_wait():
        @pl.when(moved)
        def _():
            pl.semaphore_wait(barrier, 10)

        @pl.when(stays)
        def _():
            pl.semaphore_wait(barrier, 8)

    def move(which, src, dst, device):
        return pltpu.make_async_remote_copy(
            src_ref=src,
            dst_ref=dst,
            send_sem=move_send.at[which],
            recv_sem=move_recv.at[which],
            device_id=(device,),
            device_id_type=MESH,
        )

    moves = [
        move(RAW, first.at[1], first.at[0], home),
        move(STRAIN, strn.at[1], strn.at[0], home),
        move(COT, cot.at[1], cot.at[0], home),
        move(FORCE, force.at[1], force.at[0], home),
        move(RATES, rates.at[0], rates.at[1], band),
        move(ADJ, rest.at[0], rest.at[1], band),
        move(FGRAD, fgmove.at[0], fgmove.at[1], band),
    ]

    def start_move(which):
        @pl.when(moved)
        def _():
            moves[which].start()

    def end_move(which, ref, src, dst):
        @pl.when(moved)
        def _():
            moves[which].wait_recv()

        @pl.when(stays)
        def _():
            ref[dst] = ref[src]

    lane16 = lax.broadcasted_iota(jnp.int32, (16, 128), 1)
    sub8 = lax.broadcasted_iota(jnp.int32, (8, 128), 0)
    lane8 = lax.broadcasted_iota(jnp.int32, (8, 128), 1)
    rows8 = sub8.astype(F32)
    top_half = sub8 < 4
    left_half = lane8 < 64

    def load_state():
        for i, value in enumerate(
            (BR // 2 + BR * raw[0], BC // 2 + BC * raw[1], raw[2], raw[3])
        ):
            st[OWN, i] = value
            first[1, i] = value
        for i in range(4):
            st[OWN, 4 + i] = aff[i]
            st[OWN, 8 + i] = strn[1, i] + (1.0 if i in (0, 3) else 0.0)

    def host_state():
        for i in range(4):
            st[0, i] = first[0, i]
            amat[0, i] = first[0, 5 + i]

    def place_force(role):
        for a in range(2):
            rows = DT * force[role, a]
            zero = jnp.zeros((2, COLS * 128), F32)
            frc[role, a] = roll(jnp.concatenate([zero, rows, zero], axis=0), BC // 2)

    for i in (4, 0, 1, 2, 3):
        loads[i].wait()
    eye = lax.broadcasted_iota(jnp.int32, (16, 16), 0) == lax.broadcasted_iota(jnp.int32, (16, 16), 1)
    fills = jnp.where(eye, jnp.broadcast_to(fill[...].astype(F32), (16, 16)), 0.0)
    count = jnp.sum(fills, axis=1, keepdims=True)
    first[1, 4] = jnp.where(lane16.astype(F32) < count, 1.0, 0.0)

    def stress_matrix(k, role):
        alive = first[role, 4]
        f00, f01, f10, f11 = (st[k, 8 + i] for i in range(4))
        jac = f00 * f11 - f01 * f10
        pressure = 2.0 * (jac - 1.0) * jac
        sxx = 2.0 * (f00 * f00 + f01 * f01 - 1.0) + pressure
        sxy = 2.0 * (f00 * f10 + f01 * f11)
        syy = 2.0 * (f10 * f10 + f11 * f11 - 1.0) + pressure
        tau = (sxx, sxy, sxy, syy)
        for i in range(4):
            value = alive * (-0.4 * tau[i] + st[k, 4 + i])
            amat[k, i] = value
            if k is OWN:
                first[1, 5 + i] = value

    def prepare_forward(k, role):
        alive = first[role, 4]
        p1 = st[k, 1]
        a_mat = [amat[k, i] for i in range(4)]
        c, w, _, dc = col_parts(p1)
        moved = (alive * st[k, 2], alive * st[k, 3])
        for j in range(3):
            wd = w[j] * dc[j]
            qm[j] = w[j] * alive
            for a in range(2):
                qm[3 + 3 * a + j] = w[j] * moved[a] + wd * a_mat[2 * a + 1]
                qm[9 + 3 * a + j] = w[j] * a_mat[2 * a]
        qm[30] = st[k, 0]
        qm[31] = jnp.where(c < 0.0, c + 128.0, jnp.where(c > 127.0, c - 128.0, c))

    def build_hot(k):
        nodes = lax.broadcasted_iota(jnp.int32, (128, 128), 0).astype(F32)
        for b in range(NB):
            row = qm[31, pl.ds(b, 1), :]
            hot[k, b] = jnp.where(nodes == jnp.broadcast_to(row, (128, 128)), 1.0, 0.0).astype(BF16)

    def adjoint_rows(k, base, adj):
        f00, f01, f10, f11 = (st[k, 8 + i] for i in range(4))
        gf = [adj[8 + i] for i in range(4)]
        v = [adj[2 + a] + DT * adj[a] for a in range(2)]
        x = []
        for a in range(2):
            g0, g1 = gf[2 * a], gf[2 * a + 1]
            x.append(4.0 * (adj[4 + 2 * a] + DT * (g0 * f00 + g1 * f01)))
            x.append(4.0 * (adj[5 + 2 * a] + DT * (g0 * f10 + g1 * f11)))
        _, w, _, dc = col_parts(st[k, 1])
        for j in range(3):
            wd = w[j] * dc[j]
            for a in range(2):
                qm[base + 3 * a + j] = w[j] * v[a] + wd * x[2 * a + 1]
                qm[base + 6 + 3 * a + j] = w[j] * x[2 * a]
        qm[30] = st[k, 0]
        return v, x

    def rate_rows(k):
        v = [rates[1, a] for a in range(2)]
        x = [rates[1, 2 + i] for i in range(4)]
        _, w, _, dc = col_parts(st[k, 1])
        for j in range(3):
            wd = w[j] * dc[j]
            for a in range(2):
                qm[15 + 3 * a + j] = w[j] * v[a] + wd * x[2 * a + 1]
                qm[21 + 3 * a + j] = w[j] * x[2 * a]
        qm[30] = st[k, 0]

    def scatter(k, rows, blocks=range(NB)):
        for b in blocks:
            d = rows8 - jnp.broadcast_to(qm[30, pl.ds(b, 1), :], (8, 128))
            nr, _, _ = row_spline(d)
            nd = nr * d
            pieces = []
            for channel in rows:
                for q, m in channel:
                    x = nr * jnp.broadcast_to(qm[q, pl.ds(b, 1), :], (8, 128))
                    if m is not None:
                        x = x + nd * jnp.broadcast_to(qm[m, pl.ds(b, 1), :], (8, 128))
                    pieces.append(split_rows(x))
            lhs = jnp.concatenate(pieces, axis=0).astype(BF16)
            out = lax.dot_general(
                lhs, hot[k, b], (((1,), (1,)), ((), ())), preferred_element_type=F32
            )
            target = ev if b % 2 == 0 else od
            for ch in range(len(rows)):
                total = None
                for j, s in enumerate(SHIFTS):
                    at = (3 * ch + j) * 16
                    value = out[at : at + 8] + out[at + 8 : at + 16]
                    if s:
                        value = roll(value, s)
                    total = value if total is None else total + value
                if b % 2:
                    total = roll(total, 64)
                target[ch, b // 2] = total

    def forward_channels():
        return [[(j, None) for j in range(3)]] + [
            [(3 + 3 * a + j, 9 + 3 * a + j) for j in range(3)] for a in range(2)
        ]

    def adjoint_channels(base):
        return [[(base + 3 * a + j, base + 6 + 3 * a + j) for j in range(3)] for a in range(2)]

    def combine(count, part, force_role, cols=range(COLS)):
        for ch in range(count):
            for i in cols:
                value = ev[ch, i] + jnp.where(left_half, od[ch, (i - 1) % COLS], od[ch, i])
                if force_role is not None and ch in (1, 2):
                    value = value + frc[force_role, ch - 1, :, pl.ds(i * 128, 128)]
                part[ch, :, pl.ds(i * 128, 128)] = value

    def pack(e, c, count, part):
        for ch in range(count):
            for i in range(2):
                at = CHUNK_COLS[c][2 * i] * 128
                a = part[ch, :, pl.ds(at, 128)]
                b = part[ch, :, pl.ds(at + 128, 128)]
                down = jnp.where(top_half, pltpu.roll(a, 4, axis=0), b)
                up = jnp.where(top_half, a, pltpu.roll(b, 4, axis=0))
                send[e, c, 0, ch, :, pl.ds(i * 128, 128)] = down
                send[e, c, 1, ch, :, pl.ds(i * 128, 128)] = up

    def copies(e, c, count, targets, source=None):
        return [
            pltpu.make_async_remote_copy(
                src_ref=send.at[e if source is None else source, c, side, pl.ds(0, count)],
                dst_ref=recv.at[e, c, side, pl.ds(0, count)],
                send_sem=send_sem.at[e, c, side],
                recv_sem=recv_sem.at[e, c, side],
                device_id=(other,),
                device_id_type=MESH,
            )
            for side, other in enumerate(targets)
        ]

    def start_halo(e, c, count, targets, source=None):
        for copy in copies(e, c, count, targets, source):
            copy.start()

    def wait_halo(e, c, count, targets, source=None):
        for copy in copies(e, c, count, targets, source):
            copy.wait_recv()

    def scatter_and_send(e, k, rows, part, force_role, targets, before_first=None):
        for c in range(CHUNKS):
            scatter(k, rows, SCATTER_BLOCKS[c])
            combine(len(rows), part, force_role, CHUNK_COLS[c])
            pack(e, c, len(rows), part)
            if before_first is not None and c == 0:
                before_first()
            start_halo(e, c, len(rows), targets)

    def summed(e, c, part, ch, i):
        above = recv[e, c, 0, ch, :, pl.ds(i * 128, 128)]
        below = recv[e, c, 1, ch, :, pl.ds(i * 128, 128)]
        first = jnp.where(top_half, above, pltpu.roll(below, 4, axis=0))
        second = jnp.where(top_half, pltpu.roll(above, 4, axis=0), below)
        at = CHUNK_COLS[c][2 * i] * 128
        return (
            part[ch, :, pl.ds(at, 128)] + first,
            part[ch, :, pl.ds(at + 128, 128)] + second,
        )

    def grid_velocity(k, e, c, part):
        for i in range(2):
            mass = summed(e, c, part, 0, i)
            mom = [summed(e, c, part, 1 + a, i) for a in range(2)]
            for h in range(2):
                at = pl.ds(CHUNK_COLS[c][2 * i + h] * 128, 128)
                inverse = 1.0 / (mass[h] + 0.25)
                inv[k, :, at] = inverse
                for a in range(2):
                    vg[k, a, :, at] = mom[a][h] * inverse

    def grid_adjoint(k, e, c, base, part, initial):
        for i in range(2):
            u = [summed(e, c, part, base + a, i) for a in range(2)]
            for h in range(2):
                at = pl.ds(CHUNK_COLS[c][2 * i + h] * 128, 128)
                inverse = inv[k, :, at]
                total = u[0][h] * vg[k, 0, :, at] + u[1][h] * vg[k, 1, :, at]
                part[0, :, at] = -total * inverse
                for a in range(2):
                    value = u[a][h] * inverse
                    part[1 + a, :, at] = value
                    fgacc[a, :, at] = DT * value if initial else fgacc[a, :, at] + DT * value

    def gather(k, column, channels, blocks):
        stride = 3 * channels * 64
        for b in blocks:
            i = b // 2
            pieces = []
            for ch in range(channels):
                window = column(ch, i)
                if b % 2:
                    window = roll(jnp.where(left_half, column(ch, (i + 1) % COLS), window), 64)
                for s in SHIFTS:
                    pieces.append(split_rows(roll(window, -s) if s else window))
            lhs = jnp.concatenate(pieces, axis=0).astype(BF16)
            out = jnp.dot(lhs, hot[k, b], preferred_element_type=F32)
            for q in range(3 * channels):
                value = out[16 * q : 16 * q + 8] + out[16 * q + 8 : 16 * q + 16]
                gat[pl.ds((b // 8) * stride + q * 64 + b % 8, 8, stride=8), :] = value

    def gathered(half, channels, q, r):
        return gat[pl.ds(half * 3 * channels * 64 + q * 64 + r * 8, 8), :]

    def row_sums(half, channels, q, weights):
        totals = [None] * len(weights)
        for r in range(2 * BR):
            g = gathered(half, channels, q, r)
            for t, weight in enumerate(weights):
                value = weight[r] * g
                totals[t] = value if totals[t] is None else totals[t] + value
        return totals

    def dot3(a, b):
        return a[0] * b[0] + a[1] * b[1] + a[2] * b[2]

    def row_weights(p0, slopes):
        plain, slant, slope, slope_d = [], [], [], []
        for r in range(2 * BR):
            d = float(r) - p0
            value, t, near = row_spline(d)
            plain.append(value)
            slant.append(value * d)
            if slopes:
                der = row_slope(d, t, near)
                slope.append(der)
                slope_d.append(der * d)
        return (plain, slant, slope, slope_d) if slopes else (plain, slant)

    def advance(k, store_state, channels=2):
        for half in range(2):
            at = pl.ds(8 * half, 8)
            p0, p1 = st[k, 0, at], st[k, 1, at]
            weights = row_weights(p0, False)
            _, w, _, dc = col_parts(p1)
            wd = [w[j] * dc[j] for j in range(3)]
            new_v, new_c = [], []
            for a in range(2):
                sums = [row_sums(half, channels, 3 * a + j, weights) for j in range(3)]
                r0 = [x[0] for x in sums]
                r1 = [x[1] for x in sums]
                new_v.append(dot3(w, r0))
                new_c.append(4.0 * dot3(w, r1))
                new_c.append(4.0 * dot3(wd, r0))
            for a in range(2):
                tsave[k, a, at] = new_v[a]
            for i in range(4):
                tsave[k, 2 + i, at] = new_c[i]
            if store_state:
                f = [st[k, 8 + i, at] for i in range(4)]
                st[k + 1, 0, at] = p0 + DT * new_v[0]
                st[k + 1, 1, at] = p1 + DT * new_v[1]
                for a in range(2):
                    st[k + 1, 2 + a, at] = new_v[a]
                for i in range(4):
                    st[k + 1, 4 + i, at] = new_c[i]
                for a in range(2):
                    c0, c1 = DT * new_c[2 * a], DT * new_c[2 * a + 1]
                    for j in range(2):
                        st[k + 1, 8 + 2 * a + j, at] = f[2 * a + j] + (c0 * f[j] + c1 * f[2 + j])

    def slopes_of(half, channels, first, p0, p1, count, plain_only):
        weights = row_weights(p0, True)
        _, w, wp, dc = col_parts(p1)
        wd = [w[j] * dc[j] for j in range(3)]
        wpd = [wp[j] * dc[j] for j in range(3)]
        results = []
        for ch in range(first, first + count):
            if ch < first + plain_only:
                sums = [row_sums(half, channels, 3 * ch + j, (weights[0], weights[2])) for j in range(3)]
                r0, r2 = ([x[t] for x in sums] for t in range(2))
                results.append((dot3(w, r2), dot3(wp, r0)))
                continue
            sums = [row_sums(half, channels, 3 * ch + j, weights) for j in range(3)]
            r0, r1, r2, r3 = ([x[t] for x in sums] for t in range(4))
            results.append(
                dict(
                    nw=dot3(w, r0),
                    dw=dot3(w, r1),
                    nwd=dot3(wd, r0),
                    pw=dot3(w, r2),
                    pdw=dot3(w, r3),
                    pwd=dot3(wd, r2),
                    nwp=dot3(wp, r0),
                    dwp=dot3(wp, r1),
                    nwpd=dot3(wpd, r0),
                )
            )
        return results

    def save_slopes(k, channels=2):
        for half in range(2):
            at = pl.ds(8 * half, 8)
            found = slopes_of(half, channels, 0, st[k, 0, at], st[k, 1, at], 2, 0)
            for a, t in enumerate(found):
                for i, name in enumerate(("pw", "pdw", "pwd", "nwp", "dwp", "nwpd")):
                    value = t[name]
                    if name in ("pdw", "nwpd"):
                        value = value + t["nw"]
                    tsave[k, 6 + 6 * a + i, at] = value

    def pull_gather(k, v, x, adj):
        gf = [adj[8 + i] for i in range(4)]
        p0, p1 = adj[0], adj[1]
        for a in range(2):
            pw, pdw, pwd, nwp, dwp, nwpd = (tsave[k, 6 + 6 * a + i] for i in range(6))
            p0 = p0 - (v[a] * pw + x[2 * a] * pdw + x[2 * a + 1] * pwd)
            p1 = p1 - (v[a] * nwp + x[2 * a] * dwp + x[2 * a + 1] * nwpd)
        adj[0] = p0
        adj[1] = p1
        c = [tsave[k, 2 + i] for i in range(4)]
        for b in range(2):
            for j in range(2):
                adj[8 + 2 * b + j] = gf[2 * b + j] + DT * (c[b] * gf[j] + c[2 + b] * gf[2 + j])

    def pull_scatter(k, role, adj, channels=3):
        for half in range(2):
            at = pl.ds(8 * half, 8)
            alive = first[role, 4, at]
            p0, p1 = st[k, 0, at], st[k, 1, at]
            mass, px, py = slopes_of(half, channels, channels - 3, p0, p1, 3, 1)
            a_mat = [amat[k, i, at] for i in range(4)]
            g0 = adj[0, at] - alive * mass[0]
            g1 = adj[1, at] - alive * mass[1]
            back = []
            for a, t in enumerate((px, py)):
                moved = alive * st[k, 2 + a, at]
                a0, a1 = a_mat[2 * a], a_mat[2 * a + 1]
                g0 = g0 - (moved * t["pw"] + a0 * (t["pdw"] + t["nw"]) + a1 * t["pwd"])
                g1 = g1 - (moved * t["nwp"] + a0 * t["dwp"] + a1 * (t["nwpd"] + t["nw"]))
                adj[2 + a, at] = alive * t["nw"]
                back += [alive * t["dw"], alive * t["nwd"]]
            adj[0, at] = g0
            adj[1, at] = g1
            for i in range(4):
                adj[4 + i, at] = back[i]
            f00, f01, f10, f11 = (st[k, 8 + i, at] for i in range(4))
            sxx, syy = -0.4 * back[0], -0.4 * back[3]
            sxy = -0.4 * (back[1] + back[2])
            jac = f00 * f11 - f01 * f10
            gj = (sxx + syy) * (2.0 * (2.0 * jac - 1.0))
            adj[8, at] = adj[8, at] + (4.0 * f00 * sxx + 2.0 * f10 * sxy + gj * f11)
            adj[9, at] = adj[9, at] + (4.0 * f01 * sxx + 2.0 * f11 * sxy - gj * f10)
            adj[10, at] = adj[10, at] + (4.0 * f10 * syy + 2.0 * f00 * sxy - gj * f01)
            adj[11, at] = adj[11, at] + (4.0 * f11 * syy + 2.0 * f01 * sxy + gj * f00)

    def grid_column(k):
        return lambda ch, i: vg[k, ch, :, pl.ds(i * 128, 128)]

    def part_column(part):
        return lambda ch, i: part[ch, :, pl.ds(i * 128, 128)]

    def forward_front(k, role):
        if k or role:
            stress_matrix(k, role)
        prepare_forward(k, role)
        build_hot(k)

    def forward_back(k, e, part, targets):
        for c in range(CHUNKS):
            wait_halo(e, c, 3, targets)
            grid_velocity(k, e, c, part)
            gather(k, grid_column(k), 2, GATHER_BLOCKS[c])
        advance(k, True)

    def backward_back(k, e, part, initial, targets):
        for c in range(CHUNKS):
            wait_halo(e, c, 2, targets)
            grid_adjoint(k, e, c, 0, part, initial)
            gather(k, part_column(part), 3, GATHER_BLOCKS[c])

    part, part_own = parts.at[0], parts.at[1]
    adj, adj_own = adjs.at[0], adjs.at[1]
    last = STEPS - 1

    load_state()
    forward_front(OWN, 1)
    loads[5].wait()
    loads[6].wait()
    place_force(1)

    def enter():
        barrier_wait()
        start_move(RAW)

    scatter_and_send(0, OWN, forward_channels(), part_own, 1, to_hosts, enter)
    start_move(FORCE)
    start_move(STRAIN)
    start_move(COT)
    for c in range(CHUNKS):
        start_halo(7, c, 3, owners, 0)

    end_move(RAW, first, 1, 0)
    host_state()
    forward_front(0, 0)
    scatter(0, forward_channels())
    end_move(FORCE, force, 1, 0)
    place_force(0)
    combine(3, part, 0)
    end_move(STRAIN, strn, 1, 0)
    for i in range(4):
        st[0, 8 + i] = strn[0, i] + (1.0 if i in (0, 3) else 0.0)
    forward_back(0, 0, part, to_hosts)

    for k in range(1, last):
        forward_front(k, 0)
        scatter_and_send(k, k, forward_channels(), part, 0, ring)
        save_slopes(k - 1)
        if k == 1:
            for c in range(CHUNKS):
                wait_halo(7, c, 3, owners, 0)
                grid_velocity(OWN, 7, c, part_own)
        forward_back(k, k, part, ring)

    end_move(COT, cot, 1, 0)
    for i in range(12):
        adj[i] = cot[0, i] * first[0, 4]
    adjoint_rows(last, 15, adj)
    stress_matrix(last, 0)
    prepare_forward(last, 0)
    build_hot(last)
    scatter_and_send(last, last, forward_channels() + adjoint_channels(15), part, 0, ring)
    save_slopes(last - 1)

    def last_column(ch, i):
        return grid_column(last)(ch, i) if ch < 2 else part_column(part)(ch - 2, i)

    for c in range(CHUNKS):
        wait_halo(last, c, 5, ring)
        grid_velocity(last, last, c, part)
        grid_adjoint(last, last, c, 3, part, True)
        gather(last, last_column, 5, GATHER_BLOCKS[c])
    advance(last, False, 5)
    save_slopes(last, 5)
    v, x = adjoint_rows(last, 15, adj)
    pull_gather(last, v, x, adj)
    pull_scatter(last, 0, adj, 5)

    def backward_body(t, carry):
        k = last - 1 - t
        e = last + 1 + t
        v, x = adjoint_rows(k, 15, adj)
        scatter_and_send(e, k, adjoint_channels(15), part, None, ring)
        pull_gather(k, v, x, adj)
        backward_back(k, e, part, False, ring)
        pull_scatter(k, 0, adj)
        return carry

    lax.fori_loop(0, STEPS - 2, backward_body, 0)

    v, x = adjoint_rows(0, 15, adj)
    for i, value in enumerate(v + x):
        rates[0, i] = value
    scatter_and_send(6, 0, adjoint_channels(15), part, None, to_owners, lambda: start_move(RATES))
    pull_gather(0, v, x, adj)
    for i in range(6):
        rest[0, i] = adj[i if i < 2 else 6 + i]
    for a in range(2):
        fgmove[0, a] = roll(fgacc[a], -(BC // 2))[2:6]
    start_move(ADJ)
    start_move(FGRAD)

    end_move(RATES, rates, 0, 1)
    rate_rows(OWN)
    scatter(OWN, adjoint_channels(15))
    combine(2, part_own, None)
    backward_back(OWN, 6, part_own, True, to_owners)
    end_move(ADJ, rest, 0, 1)
    for i in range(6):
        adj_own[i if i < 2 else 6 + i] = rest[1, i]
    pull_scatter(OWN, 1, adj_own)

    sg[0] = adj_own[0] * float(BR)
    sg[1] = adj_own[1] * float(BC)
    for i in range(2, 12):
        sg[i] = adj_own[i]
    end_move(FGRAD, fgmove, 0, 1)
    for a in range(2):
        fg[a] = fgmove[1, a] + roll(fgacc[a], -(BC // 2))[2:6]

    for e in range(EXCHANGES):
        targets = {0: to_hosts, 6: to_owners, 7: owners}.get(e, ring)
        count = 5 if e == last else (2 if e in (4, 5, 6) else 3)
        for c in range(CHUNKS):
            for copy in copies(e, c, count, targets, 0 if e == 7 else None):
                copy.wait_send()

    @pl.when(moved)
    def _():
        for copy in moves:
            copy.wait_send()


def per_device(n, offsets, velocity, affine, strain, tile_fill, force_field, cotangent):
    def flat(x):
        return x.reshape(x.shape[0], NB, NP)

    vmem = pl.BlockSpec(memory_space=pltpu.VMEM)
    width = COLS * 128
    state_grad, force_grad = pl.pallas_call(
        functools.partial(kernel, n),
        out_shape=(
            jax.ShapeDtypeStruct((12, NB, NP), F32),
            jax.ShapeDtypeStruct((2, BR, width), F32),
        ),
        in_specs=[pl.BlockSpec(memory_space=pltpu.HBM)] * 7,
        out_specs=(vmem, vmem),
        scratch_shapes=[
            pltpu.VMEM((1, NB), jnp.int32),
            pltpu.VMEM((4, NB, NP), F32),
            pltpu.VMEM((4, NB, NP), F32),
            pltpu.VMEM((2, 4, NB, NP), F32),
            pltpu.VMEM((2, 9, NB, NP), F32),
            pltpu.VMEM((2, 6, NB, NP), F32),
            pltpu.VMEM((2, 6, NB, NP), F32),
            pltpu.VMEM((2, 2, BR, width), F32),
            pltpu.VMEM((2, 12, NB, NP), F32),
            pltpu.VMEM((STEPS + 1, 12, NB, NP), F32),
            pltpu.VMEM((STEPS + 1, 4, NB, NP), F32),
            pltpu.VMEM((STEPS + 1, NB, 128, NP), BF16),
            pltpu.VMEM((32, NB, NP), F32),
            pltpu.VMEM((MAX_CH, COLS, 8, 128), F32),
            pltpu.VMEM((MAX_CH, COLS, 8, 128), F32),
            pltpu.VMEM((2, MAX_CH, 8, width), F32),
            pltpu.VMEM((STEPS + 1, 2, 8, width), F32),
            pltpu.VMEM((STEPS + 1, 8, width), F32),
            pltpu.VMEM((2, 2, 8, width), F32),
            pltpu.VMEM((2 * 120 * 8, 128), F32),
            pltpu.VMEM((STEPS + 1, 18, NB, NP), F32),
            pltpu.VMEM((2, 12, NB, NP), F32),
            pltpu.VMEM((2, 8, width), F32),
            pltpu.VMEM((2, 2, BR, width), F32),
            pltpu.VMEM((EXCHANGES, CHUNKS, 2, MAX_CH, 8, width // 4), F32),
            pltpu.VMEM((EXCHANGES, CHUNKS, 2, MAX_CH, 8, width // 4), F32),
            pltpu.SemaphoreType.DMA((7,)),
            pltpu.SemaphoreType.DMA((EXCHANGES, CHUNKS, 2)),
            pltpu.SemaphoreType.DMA((EXCHANGES, CHUNKS, 2)),
            pltpu.SemaphoreType.DMA((7,)),
            pltpu.SemaphoreType.DMA((7,)),
        ],
        compiler_params=pltpu.CompilerParams(collective_id=0, has_side_effects=True),
    )(
        flat(offsets),
        flat(velocity),
        flat(affine),
        flat(strain),
        tile_fill,
        force_field,
        flat(cotangent),
    )
    return state_grad.reshape(12, 1, NB, NP), force_grad


def solution(mesh):
    n = mesh.shape["slab"]
    tiles = P(None, "slab", None, None)
    return jax.shard_map(
        functools.partial(per_device, n),
        mesh=mesh,
        in_specs=(tiles, tiles, tiles, tiles, P("slab", None), P(None, "slab", None), tiles),
        out_specs=(tiles, P(None, "slab", None)),
        check_vma=False,
    )
```

```python
import functools

import jax
import jax.numpy as jnp
from jax import lax
from jax.experimental import pallas as pl
from jax.experimental.pallas import tpu as pltpu
from jax.sharding import PartitionSpec as P

BR = 4
BC = 64
NB = 16
NP = 128
STEPS = 4
COLS = 8
DT = 0.1
F32 = jnp.float32
BF16 = jnp.bfloat16
MESH = pl.DeviceIdType.MESH
SHIFTS = (-1, 0, 1)

EXCHANGES = 8
MAX_CH = 5
CHUNKS = 1
SCATTER_BLOCKS = (tuple(range(NB)),)
GATHER_BLOCKS = (tuple(range(NB)),)
CHUNK_COLS = (tuple(range(COLS)),)
OWN = STEPS
RAW, STRAIN, COT, FORCE, RATES, ADJ, FGRAD = range(7)
CHIPS = {64: (4, 4, 4), 8: (2, 2, 2), 4: (1, 2, 2)}


def host_of(band, n):
    _, nx, ny = CHIPS[n // 2]
    core, chip = lax.rem(band, 2), lax.div(band, 2)
    y, x, z = lax.rem(chip, ny), lax.rem(lax.div(chip, ny), nx), lax.div(chip, nx * ny)
    y = y + lax.rem(x, 2) * (ny - 1 - 2 * y)
    x = x + lax.rem(z, 2) * (nx - 1 - 2 * x)
    return ((z * nx + x) * ny + y) * 2 + core


def band_of(device, n):
    _, nx, ny = CHIPS[n // 2]
    core, chip = lax.rem(device, 2), lax.div(device, 2)
    y, x, z = lax.rem(chip, ny), lax.rem(lax.div(chip, ny), nx), lax.div(chip, nx * ny)
    x = x + lax.rem(z, 2) * (nx - 1 - 2 * x)
    y = y + lax.rem(x, 2) * (ny - 1 - 2 * y)
    return ((z * nx + x) * ny + y) * 2 + core


def row_spline(d):
    m = jnp.abs(d)
    t = jnp.maximum(1.5 - m, 0.0)
    near = m < 0.5
    value = jnp.where(near, 0.75 - m * m, 0.5 * t * t)
    return value, t, near


def row_slope(d, t, near):
    return jnp.where(near, -2.0 * d, jnp.where(d > 0.0, -t, t))


def col_center(p1):
    return jnp.floor(p1 + 0.5)


def col_parts(p1):
    c = col_center(p1)
    d0 = c - p1
    lo, hi = 0.5 + d0, 0.5 - d0
    values = (0.5 * lo * lo, 0.75 - d0 * d0, 0.5 * hi * hi)
    slopes = (lo, -2.0 * d0, -hi)
    w, wp, dc = [], [], []
    for s, value, slope in zip(SHIFTS, values, slopes):
        inside = jnp.logical_and(c >= float(-s), c <= float(2 * BC - 1 - s))
        w.append(jnp.where(inside, value, 0.0))
        wp.append(jnp.where(inside, slope, 0.0))
        dc.append(jnp.where(inside, d0 + float(s), 0.0))
    return c, w, wp, dc


def split_rows(x):
    top = x.astype(BF16).astype(F32)
    return jnp.concatenate([top, x - top], axis=0)


def roll(x, by):
    return pltpu.roll(x, by % x.shape[-1], axis=x.ndim - 1)


def kernel(
    n,
    off_hbm,
    vel_hbm,
    aff_hbm,
    strn_hbm,
    fill_hbm,
    force_hbm,
    cot_hbm,
    sg,
    fg,
    fill,
    raw,
    aff,
    strn,
    first,
    rates,
    rest,
    force,
    cot,
    st,
    amat,
    hot,
    qm,
    ev,
    od,
    parts,
    vg,
    inv,
    frc,
    gat,
    tsave,
    adjs,
    fgacc,
    fgmove,
    send,
    recv,
    load_sem,
    send_sem,
    recv_sem,
    move_send,
    move_recv,
):
    me = lax.axis_index("slab")
    band = band_of(me, n)
    home = host_of(me, n)
    moved = home != me
    stays = home == me

    def after(i):
        return lax.rem(i + 1, n)

    def before(i):
        return lax.rem(i + n - 1, n)

    ring = (host_of(after(band), n), host_of(before(band), n))
    to_hosts = (host_of(after(me), n), host_of(before(me), n))
    to_owners = (after(band), before(band))
    owners = (after(me), before(me))

    loads = [
        pltpu.make_async_copy(src, dst, load_sem.at[i])
        for i, (src, dst) in enumerate(
            (
                (off_hbm, raw.at[pl.ds(0, 2)]),
                (vel_hbm, raw.at[pl.ds(2, 2)]),
                (aff_hbm, aff),
                (strn_hbm, strn.at[1]),
                (fill_hbm, fill),
                (force_hbm, force.at[1]),
                (cot_hbm, cot.at[1]),
            )
        )
    ]
    for load in loads:
        load.start()

    barrier = pltpu.get_barrier_semaphore()
    for other in ring + to_hosts + to_owners + owners:
        pl.semaphore_signal(barrier, inc=1, device_id=(other,), device_id_type=MESH)

    @pl.when(moved)
    def _():
        pl.semaphore_signal(barrier, inc=1, device_id=(home,), device_id_type=MESH)
        pl.semaphore_signal(barrier, inc=1, device_id=(band,), device_id_type=MESH)

    def barrier_wait():
        @pl.when(moved)
        def _():
            pl.semaphore_wait(barrier, 10)

        @pl.when(stays)
        def _():
            pl.semaphore_wait(barrier, 8)

    def move(which, src, dst, device):
        return pltpu.make_async_remote_copy(
            src_ref=src,
            dst_ref=dst,
            send_sem=move_send.at[which],
            recv_sem=move_recv.at[which],
            device_id=(device,),
            device_id_type=MESH,
        )

    moves = [
        move(RAW, first.at[1], first.at[0], home),
        move(STRAIN, strn.at[1], strn.at[0], home),
        move(COT, cot.at[1], cot.at[0], home),
        move(FORCE, force.at[1], force.at[0], home),
        move(RATES, rates.at[0], rates.at[1], band),
        move(ADJ, rest.at[0], rest.at[1], band),
        move(FGRAD, fgmove.at[0], fgmove.at[1], band),
    ]

    def start_move(which):
        @pl.when(moved)
        def _():
            moves[which].start()

    def end_move(which, ref, src, dst):
        @pl.when(moved)
        def _():
            moves[which].wait_recv()

        @pl.when(stays)
        def _():
            ref[dst] = ref[src]

    lane16 = lax.broadcasted_iota(jnp.int32, (16, 128), 1)
    sub8 = lax.broadcasted_iota(jnp.int32, (8, 128), 0)
    lane8 = lax.broadcasted_iota(jnp.int32, (8, 128), 1)
    rows8 = sub8.astype(F32)
    top_half = sub8 < 4
    left_half = lane8 < 64

    def load_state():
        for i, value in enumerate(
            (BR // 2 + BR * raw[0], BC // 2 + BC * raw[1], raw[2], raw[3])
        ):
            st[OWN, i] = value
            first[1, i] = value
        for i in range(4):
            st[OWN, 4 + i] = aff[i]
            st[OWN, 8 + i] = strn[1, i] + (1.0 if i in (0, 3) else 0.0)

    def host_state():
        for i in range(4):
            st[0, i] = first[0, i]
            amat[0, i] = first[0, 5 + i]

    def place_force(role):
        for a in range(2):
            rows = DT * force[role, a]
            zero = jnp.zeros((2, COLS * 128), F32)
            frc[role, a] = roll(jnp.concatenate([zero, rows, zero], axis=0), BC // 2)

    for i in (4, 0, 1, 2, 3):
        loads[i].wait()
    eye = lax.broadcasted_iota(jnp.int32, (16, 16), 0) == lax.broadcasted_iota(jnp.int32, (16, 16), 1)
    fills = jnp.where(eye, jnp.broadcast_to(fill[...].astype(F32), (16, 16)), 0.0)
    count = jnp.sum(fills, axis=1, keepdims=True)
    first[1, 4] = jnp.where(lane16.astype(F32) < count, 1.0, 0.0)

    def stress_matrix(k, role):
        alive = first[role, 4]
        f00, f01, f10, f11 = (st[k, 8 + i] for i in range(4))
        jac = f00 * f11 - f01 * f10
        pressure = 2.0 * (jac - 1.0) * jac
        sxx = 2.0 * (f00 * f00 + f01 * f01 - 1.0) + pressure
        sxy = 2.0 * (f00 * f10 + f01 * f11)
        syy = 2.0 * (f10 * f10 + f11 * f11 - 1.0) + pressure
        tau = (sxx, sxy, sxy, syy)
        for i in range(4):
            value = alive * (-0.4 * tau[i] + st[k, 4 + i])
            amat[k, i] = value
            if k is OWN:
                first[1, 5 + i] = value

    def prepare_forward(k, role):
        alive = first[role, 4]
        p1 = st[k, 1]
        a_mat = [amat[k, i] for i in range(4)]
        c, w, _, dc = col_parts(p1)
        moved = (alive * st[k, 2], alive * st[k, 3])
        for j in range(3):
            wd = w[j] * dc[j]
            qm[j] = w[j] * alive
            for a in range(2):
                qm[3 + 3 * a + j] = w[j] * moved[a] + wd * a_mat[2 * a + 1]
                qm[9 + 3 * a + j] = w[j] * a_mat[2 * a]
        qm[30] = st[k, 0]
        qm[31] = jnp.where(c < 0.0, c + 128.0, jnp.where(c > 127.0, c - 128.0, c))

    def build_hot(k):
        nodes = lax.broadcasted_iota(jnp.int32, (128, 128), 0).astype(F32)
        for b in range(NB):
            row = qm[31, pl.ds(b, 1), :]
            hot[k, b] = jnp.where(nodes == jnp.broadcast_to(row, (128, 128)), 1.0, 0.0).astype(BF16)

    def adjoint_rows(k, base, adj):
        f00, f01, f10, f11 = (st[k, 8 + i] for i in range(4))
        gf = [adj[8 + i] for i in range(4)]
        v = [adj[2 + a] + DT * adj[a] for a in range(2)]
        x = []
        for a in range(2):
            g0, g1 = gf[2 * a], gf[2 * a + 1]
            x.append(4.0 * (adj[4 + 2 * a] + DT * (g0 * f00 + g1 * f01)))
            x.append(4.0 * (adj[5 + 2 * a] + DT * (g0 * f10 + g1 * f11)))
        _, w, _, dc = col_parts(st[k, 1])
        for j in range(3):
            wd = w[j] * dc[j]
            for a in range(2):
                qm[base + 3 * a + j] = w[j] * v[a] + wd * x[2 * a + 1]
                qm[base + 6 + 3 * a + j] = w[j] * x[2 * a]
        qm[30] = st[k, 0]
        return v, x

    def rate_rows(k):
        v = [rates[1, a] for a in range(2)]
        x = [rates[1, 2 + i] for i in range(4)]
        _, w, _, dc = col_parts(st[k, 1])
        for j in range(3):
            wd = w[j] * dc[j]
            for a in range(2):
                qm[15 + 3 * a + j] = w[j] * v[a] + wd * x[2 * a + 1]
                qm[21 + 3 * a + j] = w[j] * x[2 * a]
        qm[30] = st[k, 0]

    def scatter(k, rows, blocks=range(NB)):
        for b in blocks:
            d = rows8 - jnp.broadcast_to(qm[30, pl.ds(b, 1), :], (8, 128))
            nr, _, _ = row_spline(d)
            nd = nr * d
            pieces = []
            for channel in rows:
                for q, m in channel:
                    x = nr * jnp.broadcast_to(qm[q, pl.ds(b, 1), :], (8, 128))
                    if m is not None:
                        x = x + nd * jnp.broadcast_to(qm[m, pl.ds(b, 1), :], (8, 128))
                    pieces.append(split_rows(x))
            lhs = jnp.concatenate(pieces, axis=0).astype(BF16)
            out = lax.dot_general(
                lhs, hot[k, b], (((1,), (1,)), ((), ())), preferred_element_type=F32
            )
            target = ev if b % 2 == 0 else od
            for ch in range(len(rows)):
                total = None
                for j, s in enumerate(SHIFTS):
                    at = (3 * ch + j) * 16
                    value = out[at : at + 8] + out[at + 8 : at + 16]
                    if s:
                        value = roll(value, s)
                    total = value if total is None else total + value
                if b % 2:
                    total = roll(total, 64)
                target[ch, b // 2] = total

    def forward_channels():
        return [[(j, None) for j in range(3)]] + [
            [(3 + 3 * a + j, 9 + 3 * a + j) for j in range(3)] for a in range(2)
        ]

    def adjoint_channels(base):
        return [[(base + 3 * a + j, base + 6 + 3 * a + j) for j in range(3)] for a in range(2)]

    def combine(count, part, force_role, cols=range(COLS)):
        for ch in range(count):
            for i in cols:
                value = ev[ch, i] + jnp.where(left_half, od[ch, (i - 1) % COLS], od[ch, i])
                if force_role is not None and ch in (1, 2):
                    value = value + frc[force_role, ch - 1, :, pl.ds(i * 128, 128)]
                part[ch, :, pl.ds(i * 128, 128)] = value

    def pack(e, c, count, part):
        for ch in range(count):
            for i in range(len(CHUNK_COLS[c]) // 2):
                at = CHUNK_COLS[c][2 * i] * 128
                a = part[ch, :, pl.ds(at, 128)]
                b = part[ch, :, pl.ds(at + 128, 128)]
                down = jnp.where(top_half, pltpu.roll(a, 4, axis=0), b)
                up = jnp.where(top_half, a, pltpu.roll(b, 4, axis=0))
                send[e, c, 0, ch, :, pl.ds(i * 128, 128)] = down
                send[e, c, 1, ch, :, pl.ds(i * 128, 128)] = up

    def copies(e, c, count, targets, source=None):
        return [
            pltpu.make_async_remote_copy(
                src_ref=send.at[e if source is None else source, c, side, pl.ds(0, count)],
                dst_ref=recv.at[e, c, side, pl.ds(0, count)],
                send_sem=send_sem.at[e, c, side],
                recv_sem=recv_sem.at[e, c, side],
                device_id=(other,),
                device_id_type=MESH,
            )
            for side, other in enumerate(targets)
        ]

    def start_halo(e, c, count, targets, source=None):
        for copy in copies(e, c, count, targets, source):
            copy.start()

    def wait_halo(e, c, count, targets, source=None):
        for copy in copies(e, c, count, targets, source):
            copy.wait_recv()

    def scatter_and_send(e, k, rows, part, force_role, targets, before_first=None):
        for c in range(CHUNKS):
            scatter(k, rows, SCATTER_BLOCKS[c])
            combine(len(rows), part, force_role, CHUNK_COLS[c])
            pack(e, c, len(rows), part)
            if before_first is not None and c == 0:
                before_first()
            start_halo(e, c, len(rows), targets)

    def summed(e, c, part, ch, i):
        above = recv[e, c, 0, ch, :, pl.ds(i * 128, 128)]
        below = recv[e, c, 1, ch, :, pl.ds(i * 128, 128)]
        first = jnp.where(top_half, above, pltpu.roll(below, 4, axis=0))
        second = jnp.where(top_half, pltpu.roll(above, 4, axis=0), below)
        at = CHUNK_COLS[c][2 * i] * 128
        return (
            part[ch, :, pl.ds(at, 128)] + first,
            part[ch, :, pl.ds(at + 128, 128)] + second,
        )

    def grid_velocity(k, e, c, part):
        for i in range(len(CHUNK_COLS[c]) // 2):
            mass = summed(e, c, part, 0, i)
            mom = [summed(e, c, part, 1 + a, i) for a in range(2)]
            for h in range(2):
                at = pl.ds(CHUNK_COLS[c][2 * i + h] * 128, 128)
                inverse = 1.0 / (mass[h] + 0.25)
                inv[k, :, at] = inverse
                for a in range(2):
                    vg[k, a, :, at] = mom[a][h] * inverse

    def grid_adjoint(k, e, c, base, part, initial):
        for i in range(len(CHUNK_COLS[c]) // 2):
            u = [summed(e, c, part, base + a, i) for a in range(2)]
            for h in range(2):
                at = pl.ds(CHUNK_COLS[c][2 * i + h] * 128, 128)
                inverse = inv[k, :, at]
                total = u[0][h] * vg[k, 0, :, at] + u[1][h] * vg[k, 1, :, at]
                part[0, :, at] = -total * inverse
                for a in range(2):
                    value = u[a][h] * inverse
                    part[1 + a, :, at] = value
                    fgacc[a, :, at] = DT * value if initial else fgacc[a, :, at] + DT * value

    def gather(k, column, channels, blocks):
        stride = 3 * channels * 64
        for b in blocks:
            i = b // 2
            pieces = []
            for ch in range(channels):
                window = column(ch, i)
                if b % 2:
                    window = roll(jnp.where(left_half, column(ch, (i + 1) % COLS), window), 64)
                for s in SHIFTS:
                    pieces.append(split_rows(roll(window, -s) if s else window))
            lhs = jnp.concatenate(pieces, axis=0).astype(BF16)
            out = jnp.dot(lhs, hot[k, b], preferred_element_type=F32)
            for q in range(3 * channels):
                value = out[16 * q : 16 * q + 8] + out[16 * q + 8 : 16 * q + 16]
                gat[pl.ds((b // 8) * stride + q * 64 + b % 8, 8, stride=8), :] = value

    def gathered(half, channels, q, r):
        return gat[pl.ds(half * 3 * channels * 64 + q * 64 + r * 8, 8), :]

    def row_sums(half, channels, q, weights):
        totals = [None] * len(weights)
        for r in range(2 * BR):
            g = gathered(half, channels, q, r)
            for t, weight in enumerate(weights):
                value = weight[r] * g
                totals[t] = value if totals[t] is None else totals[t] + value
        return totals

    def dot3(a, b):
        return a[0] * b[0] + a[1] * b[1] + a[2] * b[2]

    def row_weights(p0, slopes):
        plain, slant, slope, slope_d = [], [], [], []
        for r in range(2 * BR):
            d = float(r) - p0
            value, t, near = row_spline(d)
            plain.append(value)
            slant.append(value * d)
            if slopes:
                der = row_slope(d, t, near)
                slope.append(der)
                slope_d.append(der * d)
        return (plain, slant, slope, slope_d) if slopes else (plain, slant)

    def advance(k, store_state, channels=2):
        for half in range(2):
            at = pl.ds(8 * half, 8)
            p0, p1 = st[k, 0, at], st[k, 1, at]
            weights = row_weights(p0, False)
            _, w, _, dc = col_parts(p1)
            wd = [w[j] * dc[j] for j in range(3)]
            new_v, new_c = [], []
            for a in range(2):
                sums = [row_sums(half, channels, 3 * a + j, weights) for j in range(3)]
                r0 = [x[0] for x in sums]
                r1 = [x[1] for x in sums]
                new_v.append(dot3(w, r0))
                new_c.append(4.0 * dot3(w, r1))
                new_c.append(4.0 * dot3(wd, r0))
            for a in range(2):
                tsave[k, a, at] = new_v[a]
            for i in range(4):
                tsave[k, 2 + i, at] = new_c[i]
            if store_state:
                f = [st[k, 8 + i, at] for i in range(4)]
                st[k + 1, 0, at] = p0 + DT * new_v[0]
                st[k + 1, 1, at] = p1 + DT * new_v[1]
                for a in range(2):
                    st[k + 1, 2 + a, at] = new_v[a]
                for i in range(4):
                    st[k + 1, 4 + i, at] = new_c[i]
                for a in range(2):
                    c0, c1 = DT * new_c[2 * a], DT * new_c[2 * a + 1]
                    for j in range(2):
                        st[k + 1, 8 + 2 * a + j, at] = f[2 * a + j] + (c0 * f[j] + c1 * f[2 + j])

    def slopes_of(half, channels, first, p0, p1, count, plain_only):
        weights = row_weights(p0, True)
        _, w, wp, dc = col_parts(p1)
        wd = [w[j] * dc[j] for j in range(3)]
        wpd = [wp[j] * dc[j] for j in range(3)]
        results = []
        for ch in range(first, first + count):
            if ch < first + plain_only:
                sums = [row_sums(half, channels, 3 * ch + j, (weights[0], weights[2])) for j in range(3)]
                r0, r2 = ([x[t] for x in sums] for t in range(2))
                results.append((dot3(w, r2), dot3(wp, r0)))
                continue
            sums = [row_sums(half, channels, 3 * ch + j, weights) for j in range(3)]
            r0, r1, r2, r3 = ([x[t] for x in sums] for t in range(4))
            results.append(
                dict(
                    nw=dot3(w, r0),
                    dw=dot3(w, r1),
                    nwd=dot3(wd, r0),
                    pw=dot3(w, r2),
                    pdw=dot3(w, r3),
                    pwd=dot3(wd, r2),
                    nwp=dot3(wp, r0),
                    dwp=dot3(wp, r1),
                    nwpd=dot3(wpd, r0),
                )
            )
        return results

    def save_slopes(k, channels=2):
        for half in range(2):
            at = pl.ds(8 * half, 8)
            found = slopes_of(half, channels, 0, st[k, 0, at], st[k, 1, at], 2, 0)
            for a, t in enumerate(found):
                for i, name in enumerate(("pw", "pdw", "pwd", "nwp", "dwp", "nwpd")):
                    value = t[name]
                    if name in ("pdw", "nwpd"):
                        value = value + t["nw"]
                    tsave[k, 6 + 6 * a + i, at] = value

    def pull_gather(k, v, x, adj):
        gf = [adj[8 + i] for i in range(4)]
        p0, p1 = adj[0], adj[1]
        for a in range(2):
            pw, pdw, pwd, nwp, dwp, nwpd = (tsave[k, 6 + 6 * a + i] for i in range(6))
            p0 = p0 - (v[a] * pw + x[2 * a] * pdw + x[2 * a + 1] * pwd)
            p1 = p1 - (v[a] * nwp + x[2 * a] * dwp + x[2 * a + 1] * nwpd)
        adj[0] = p0
        adj[1] = p1
        c = [tsave[k, 2 + i] for i in range(4)]
        for b in range(2):
            for j in range(2):
                adj[8 + 2 * b + j] = gf[2 * b + j] + DT * (c[b] * gf[j] + c[2 + b] * gf[2 + j])

    def pull_scatter(k, role, adj, channels=3):
        for half in range(2):
            at = pl.ds(8 * half, 8)
            alive = first[role, 4, at]
            p0, p1 = st[k, 0, at], st[k, 1, at]
            mass, px, py = slopes_of(half, channels, channels - 3, p0, p1, 3, 1)
            a_mat = [amat[k, i, at] for i in range(4)]
            g0 = adj[0, at] - alive * mass[0]
            g1 = adj[1, at] - alive * mass[1]
            back = []
            for a, t in enumerate((px, py)):
                moved = alive * st[k, 2 + a, at]
                a0, a1 = a_mat[2 * a], a_mat[2 * a + 1]
                g0 = g0 - (moved * t["pw"] + a0 * (t["pdw"] + t["nw"]) + a1 * t["pwd"])
                g1 = g1 - (moved * t["nwp"] + a0 * t["dwp"] + a1 * (t["nwpd"] + t["nw"]))
                adj[2 + a, at] = alive * t["nw"]
                back += [alive * t["dw"], alive * t["nwd"]]
            adj[0, at] = g0
            adj[1, at] = g1
            for i in range(4):
                adj[4 + i, at] = back[i]
            f00, f01, f10, f11 = (st[k, 8 + i, at] for i in range(4))
            sxx, syy = -0.4 * back[0], -0.4 * back[3]
            sxy = -0.4 * (back[1] + back[2])
            jac = f00 * f11 - f01 * f10
            gj = (sxx + syy) * (2.0 * (2.0 * jac - 1.0))
            adj[8, at] = adj[8, at] + (4.0 * f00 * sxx + 2.0 * f10 * sxy + gj * f11)
            adj[9, at] = adj[9, at] + (4.0 * f01 * sxx + 2.0 * f11 * sxy - gj * f10)
            adj[10, at] = adj[10, at] + (4.0 * f10 * syy + 2.0 * f00 * sxy - gj * f01)
            adj[11, at] = adj[11, at] + (4.0 * f11 * syy + 2.0 * f01 * sxy + gj * f00)

    def grid_column(k):
        return lambda ch, i: vg[k, ch, :, pl.ds(i * 128, 128)]

    def part_column(part):
        return lambda ch, i: part[ch, :, pl.ds(i * 128, 128)]

    def forward_front(k, role):
        if k or role:
            stress_matrix(k, role)
        prepare_forward(k, role)
        build_hot(k)

    def forward_back(k, e, part, targets):
        for c in range(CHUNKS):
            wait_halo(e, c, 3, targets)
            grid_velocity(k, e, c, part)
            gather(k, grid_column(k), 2, GATHER_BLOCKS[c])
        advance(k, True)

    def backward_back(k, e, part, initial, targets):
        for c in range(CHUNKS):
            wait_halo(e, c, 2, targets)
            grid_adjoint(k, e, c, 0, part, initial)
            gather(k, part_column(part), 3, GATHER_BLOCKS[c])

    part, part_own = parts.at[0], parts.at[1]
    adj, adj_own = adjs.at[0], adjs.at[1]
    last = STEPS - 1

    load_state()
    forward_front(OWN, 1)
    loads[5].wait()
    loads[6].wait()
    place_force(1)

    def enter():
        barrier_wait()
        start_move(RAW)

    scatter_and_send(0, OWN, forward_channels(), part_own, 1, to_hosts, enter)
    start_move(FORCE)
    start_move(STRAIN)
    start_move(COT)
    for c in range(CHUNKS):
        start_halo(7, c, 3, owners, 0)

    end_move(RAW, first, 1, 0)
    host_state()
    forward_front(0, 0)
    scatter(0, forward_channels())
    end_move(FORCE, force, 1, 0)
    place_force(0)
    combine(3, part, 0)
    end_move(STRAIN, strn, 1, 0)
    for i in range(4):
        st[0, 8 + i] = strn[0, i] + (1.0 if i in (0, 3) else 0.0)
    forward_back(0, 0, part, to_hosts)

    for k in range(1, last):
        forward_front(k, 0)
        scatter_and_send(k, k, forward_channels(), part, 0, ring)
        save_slopes(k - 1)
        if k == 1:
            for c in range(CHUNKS):
                wait_halo(7, c, 3, owners, 0)
                grid_velocity(OWN, 7, c, part_own)
        forward_back(k, k, part, ring)

    end_move(COT, cot, 1, 0)
    for i in range(12):
        adj[i] = cot[0, i] * first[0, 4]
    adjoint_rows(last, 15, adj)
    stress_matrix(last, 0)
    prepare_forward(last, 0)
    build_hot(last)
    scatter_and_send(last, last, forward_channels() + adjoint_channels(15), part, 0, ring)
    save_slopes(last - 1)

    def last_column(ch, i):
        return grid_column(last)(ch, i) if ch < 2 else part_column(part)(ch - 2, i)

    for c in range(CHUNKS):
        wait_halo(last, c, 5, ring)
        grid_velocity(last, last, c, part)
        grid_adjoint(last, last, c, 3, part, True)
        gather(last, last_column, 5, GATHER_BLOCKS[c])
    advance(last, False, 5)
    save_slopes(last, 5)
    v, x = adjoint_rows(last, 15, adj)
    pull_gather(last, v, x, adj)
    pull_scatter(last, 0, adj, 5)

    def backward_body(t, carry):
        k = last - 1 - t
        e = last + 1 + t
        v, x = adjoint_rows(k, 15, adj)
        scatter_and_send(e, k, adjoint_channels(15), part, None, ring)
        pull_gather(k, v, x, adj)
        backward_back(k, e, part, False, ring)
        pull_scatter(k, 0, adj)
        return carry

    lax.fori_loop(0, STEPS - 2, backward_body, 0)

    v, x = adjoint_rows(0, 15, adj)
    for i, value in enumerate(v + x):
        rates[0, i] = value
    scatter_and_send(6, 0, adjoint_channels(15), part, None, to_owners, lambda: start_move(RATES))
    pull_gather(0, v, x, adj)
    for i in range(6):
        rest[0, i] = adj[i if i < 2 else 6 + i]
    for a in range(2):
        fgmove[0, a] = roll(fgacc[a], -(BC // 2))[2:6]
    start_move(ADJ)
    start_move(FGRAD)

    end_move(RATES, rates, 0, 1)
    rate_rows(OWN)
    scatter(OWN, adjoint_channels(15))
    combine(2, part_own, None)
    backward_back(OWN, 6, part_own, True, to_owners)
    end_move(ADJ, rest, 0, 1)
    for i in range(6):
        adj_own[i if i < 2 else 6 + i] = rest[1, i]
    pull_scatter(OWN, 1, adj_own)

    sg[0] = adj_own[0] * float(BR)
    sg[1] = adj_own[1] * float(BC)
    for i in range(2, 12):
        sg[i] = adj_own[i]
    end_move(FGRAD, fgmove, 0, 1)
    for a in range(2):
        fg[a] = fgmove[1, a] + roll(fgacc[a], -(BC // 2))[2:6]

    for e in range(EXCHANGES):
        targets = {0: to_hosts, 6: to_owners, 7: owners}.get(e, ring)
        count = 5 if e == last else (2 if e in (4, 5, 6) else 3)
        for c in range(CHUNKS):
            for copy in copies(e, c, count, targets, 0 if e == 7 else None):
                copy.wait_send()

    @pl.when(moved)
    def _():
        for copy in moves:
            copy.wait_send()


def per_device(n, offsets, velocity, affine, strain, tile_fill, force_field, cotangent):
    def flat(x):
        return x.reshape(x.shape[0], NB, NP)

    vmem = pl.BlockSpec(memory_space=pltpu.VMEM)
    width = COLS * 128
    state_grad, force_grad = pl.pallas_call(
        functools.partial(kernel, n),
        out_shape=(
            jax.ShapeDtypeStruct((12, NB, NP), F32),
            jax.ShapeDtypeStruct((2, BR, width), F32),
        ),
        in_specs=[pl.BlockSpec(memory_space=pltpu.HBM)] * 7,
        out_specs=(vmem, vmem),
        scratch_shapes=[
            pltpu.VMEM((1, NB), jnp.int32),
            pltpu.VMEM((4, NB, NP), F32),
            pltpu.VMEM((4, NB, NP), F32),
            pltpu.VMEM((2, 4, NB, NP), F32),
            pltpu.VMEM((2, 9, NB, NP), F32),
            pltpu.VMEM((2, 6, NB, NP), F32),
            pltpu.VMEM((2, 6, NB, NP), F32),
            pltpu.VMEM((2, 2, BR, width), F32),
            pltpu.VMEM((2, 12, NB, NP), F32),
            pltpu.VMEM((STEPS + 1, 12, NB, NP), F32),
            pltpu.VMEM((STEPS + 1, 4, NB, NP), F32),
            pltpu.VMEM((STEPS + 1, NB, 128, NP), BF16),
            pltpu.VMEM((32, NB, NP), F32),
            pltpu.VMEM((MAX_CH, COLS, 8, 128), F32),
            pltpu.VMEM((MAX_CH, COLS, 8, 128), F32),
            pltpu.VMEM((2, MAX_CH, 8, width), F32),
            pltpu.VMEM((STEPS + 1, 2, 8, width), F32),
            pltpu.VMEM((STEPS + 1, 8, width), F32),
            pltpu.VMEM((2, 2, 8, width), F32),
            pltpu.VMEM((2 * 120 * 8, 128), F32),
            pltpu.VMEM((STEPS + 1, 18, NB, NP), F32),
            pltpu.VMEM((2, 12, NB, NP), F32),
            pltpu.VMEM((2, 8, width), F32),
            pltpu.VMEM((2, 2, BR, width), F32),
            pltpu.VMEM((EXCHANGES, CHUNKS, 2, MAX_CH, 8, width // 2 // CHUNKS), F32),
            pltpu.VMEM((EXCHANGES, CHUNKS, 2, MAX_CH, 8, width // 2 // CHUNKS), F32),
            pltpu.SemaphoreType.DMA((7,)),
            pltpu.SemaphoreType.DMA((EXCHANGES, CHUNKS, 2)),
            pltpu.SemaphoreType.DMA((EXCHANGES, CHUNKS, 2)),
            pltpu.SemaphoreType.DMA((7,)),
            pltpu.SemaphoreType.DMA((7,)),
        ],
        compiler_params=pltpu.CompilerParams(collective_id=0, has_side_effects=True, vmem_limit_bytes=24 << 20),
    )(
        pltpu.with_memory_space_constraint(flat(offsets), pltpu.HBM),
        pltpu.with_memory_space_constraint(flat(velocity), pltpu.HBM),
        pltpu.with_memory_space_constraint(flat(affine), pltpu.HBM),
        pltpu.with_memory_space_constraint(flat(strain), pltpu.HBM),
        pltpu.with_memory_space_constraint(tile_fill, pltpu.HBM),
        pltpu.with_memory_space_constraint(force_field, pltpu.HBM),
        pltpu.with_memory_space_constraint(flat(cotangent), pltpu.HBM),
    )
    return state_grad.reshape(12, 1, NB, NP), force_grad


def solution(mesh):
    n = mesh.shape["slab"]
    tiles = P(None, "slab", None, None)
    return jax.shard_map(
        functools.partial(per_device, n),
        mesh=mesh,
        in_specs=(tiles, tiles, tiles, tiles, P("slab", None), P(None, "slab", None), tiles),
        out_specs=(tiles, P(None, "slab", None)),
        check_vma=False,
    )
```

```python
import functools

import jax
import jax.numpy as jnp
from jax import lax
from jax.experimental import pallas as pl
from jax.experimental.pallas import tpu as pltpu
from jax.sharding import PartitionSpec as P

BR = 4
BC = 64
NB = 16
NP = 128
STEPS = 4
COLS = 8
DT = 0.1
F32 = jnp.float32
BF16 = jnp.bfloat16
MESH = pl.DeviceIdType.MESH
SHIFTS = (-1, 0, 1)

EXCHANGES = 8
MAX_CH = 5
CHUNKS = 1
CHUNK_COLS = (tuple(range(COLS)),)
OWN = STEPS
RAW, STRAIN, COT, FORCE, RATES, ADJ, FGRAD = range(7)
CHIPS = {64: (4, 4, 4), 8: (2, 2, 2), 4: (1, 2, 2)}


def host_of(band, n):
    _, nx, ny = CHIPS[n // 2]
    core, chip = lax.rem(band, 2), lax.div(band, 2)
    y, x, z = lax.rem(chip, ny), lax.rem(lax.div(chip, ny), nx), lax.div(chip, nx * ny)
    y = y + lax.rem(x, 2) * (ny - 1 - 2 * y)
    x = x + lax.rem(z, 2) * (nx - 1 - 2 * x)
    return ((z * nx + x) * ny + y) * 2 + core


def band_of(device, n):
    _, nx, ny = CHIPS[n // 2]
    core, chip = lax.rem(device, 2), lax.div(device, 2)
    y, x, z = lax.rem(chip, ny), lax.rem(lax.div(chip, ny), nx), lax.div(chip, nx * ny)
    x = x + lax.rem(z, 2) * (nx - 1 - 2 * x)
    y = y + lax.rem(x, 2) * (ny - 1 - 2 * y)
    return ((z * nx + x) * ny + y) * 2 + core


def row_spline(d):
    m = jnp.abs(d)
    t = jnp.maximum(1.5 - m, 0.0)
    near = m < 0.5
    value = jnp.where(near, 0.75 - m * m, 0.5 * t * t)
    return value, t, near


def row_slope(d, t, near):
    return jnp.where(near, -2.0 * d, jnp.where(d > 0.0, -t, t))


def col_center(p1):
    return jnp.floor(p1 + 0.5)


def col_parts(p1):
    c = col_center(p1)
    d0 = c - p1
    lo, hi = 0.5 + d0, 0.5 - d0
    values = (0.5 * lo * lo, 0.75 - d0 * d0, 0.5 * hi * hi)
    slopes = (lo, -2.0 * d0, -hi)
    w, wp, dc = [], [], []
    for s, value, slope in zip(SHIFTS, values, slopes):
        inside = jnp.logical_and(c >= float(-s), c <= float(2 * BC - 1 - s))
        w.append(jnp.where(inside, value, 0.0))
        wp.append(jnp.where(inside, slope, 0.0))
        dc.append(jnp.where(inside, d0 + float(s), 0.0))
    return c, w, wp, dc


def split_rows(x):
    top = x.astype(BF16).astype(F32)
    return jnp.concatenate([top, x - top], axis=0)


def roll(x, by):
    return pltpu.roll(x, by % x.shape[-1], axis=x.ndim - 1)


def kernel(
    n,
    off_hbm,
    vel_hbm,
    aff_hbm,
    strn_hbm,
    fill_hbm,
    force_hbm,
    cot_hbm,
    sg,
    fg,
    fill,
    raw,
    aff,
    strn,
    first,
    rates,
    rest,
    force,
    cot,
    st,
    amat,
    hot,
    toh,
    qm,
    ev,
    od,
    parts,
    vg,
    inv,
    frc,
    gat,
    tsave,
    adjs,
    fgacc,
    fgmove,
    send,
    recv,
    load_sem,
    send_sem,
    recv_sem,
    move_send,
    move_recv,
):
    me = lax.axis_index("slab")
    band = band_of(me, n)
    home = host_of(me, n)
    moved = home != me
    stays = home == me

    def after(i):
        return lax.rem(i + 1, n)

    def before(i):
        return lax.rem(i + n - 1, n)

    ring = (host_of(after(band), n), host_of(before(band), n))
    to_hosts = (host_of(after(me), n), host_of(before(me), n))
    to_owners = (after(band), before(band))
    owners = (after(me), before(me))

    loads = [
        pltpu.make_async_copy(src, dst, load_sem.at[i])
        for i, (src, dst) in enumerate(
            (
                (off_hbm, raw.at[pl.ds(0, 2)]),
                (vel_hbm, raw.at[pl.ds(2, 2)]),
                (aff_hbm, aff),
                (strn_hbm, strn.at[1]),
                (fill_hbm, fill),
                (force_hbm, force.at[1]),
                (cot_hbm, cot.at[1]),
            )
        )
    ]
    for load in loads:
        load.start()

    barrier = pltpu.get_barrier_semaphore()
    for other in ring + to_hosts + to_owners + owners:
        pl.semaphore_signal(barrier, inc=1, device_id=(other,), device_id_type=MESH)

    @pl.when(moved)
    def _():
        pl.semaphore_signal(barrier, inc=1, device_id=(home,), device_id_type=MESH)
        pl.semaphore_signal(barrier, inc=1, device_id=(band,), device_id_type=MESH)

    def barrier_wait():
        @pl.when(moved)
        def _():
            pl.semaphore_wait(barrier, 10)

        @pl.when(stays)
        def _():
            pl.semaphore_wait(barrier, 8)

    def move(which, src, dst, device):
        return pltpu.make_async_remote_copy(
            src_ref=src,
            dst_ref=dst,
            send_sem=move_send.at[which],
            recv_sem=move_recv.at[which],
            device_id=(device,),
            device_id_type=MESH,
        )

    moves = [
        move(RAW, first.at[1], first.at[0], home),
        move(STRAIN, strn.at[1], strn.at[0], home),
        move(COT, cot.at[1], cot.at[0], home),
        move(FORCE, force.at[1], force.at[0], home),
        move(RATES, rates.at[0], rates.at[1], band),
        move(ADJ, rest.at[0], rest.at[1], band),
        move(FGRAD, fgmove.at[0], fgmove.at[1], band),
    ]

    def start_move(which):
        @pl.when(moved)
        def _():
            moves[which].start()

    def end_move(which, ref, src, dst):
        @pl.when(moved)
        def _():
            moves[which].wait_recv()

        @pl.when(stays)
        def _():
            ref[dst] = ref[src]

    lane16 = lax.broadcasted_iota(jnp.int32, (16, 128), 1)
    sub8 = lax.broadcasted_iota(jnp.int32, (8, 128), 0)
    lane8 = lax.broadcasted_iota(jnp.int32, (8, 128), 1)
    rows8 = sub8.astype(F32)
    top_half = sub8 < 4
    left_half = lane8 < 64

    def load_state():
        for i, value in enumerate(
            (BR // 2 + BR * raw[0], BC // 2 + BC * raw[1], raw[2], raw[3])
        ):
            st[OWN, i] = value
            first[1, i] = value
        for i in range(4):
            st[OWN, 4 + i] = aff[i]
            st[OWN, 8 + i] = strn[1, i] + (1.0 if i in (0, 3) else 0.0)

    def host_state():
        for i in range(4):
            st[0, i] = first[0, i]
            amat[0, i] = first[0, 5 + i]

    def place_force(role):
        for a in range(2):
            rows = DT * force[role, a]
            zero = jnp.zeros((2, COLS * 128), F32)
            frc[role, a] = roll(jnp.concatenate([zero, rows, zero], axis=0), BC // 2)

    for i in (4, 0, 1, 2, 3):
        loads[i].wait()
    eye = lax.broadcasted_iota(jnp.int32, (16, 16), 0) == lax.broadcasted_iota(jnp.int32, (16, 16), 1)
    fills = jnp.where(eye, jnp.broadcast_to(fill[...].astype(F32), (16, 16)), 0.0)
    count = jnp.sum(fills, axis=1, keepdims=True)
    first[1, 4] = jnp.where(lane16.astype(F32) < count, 1.0, 0.0)

    def stress_matrix(k, role):
        alive = first[role, 4]
        f00, f01, f10, f11 = (st[k, 8 + i] for i in range(4))
        jac = f00 * f11 - f01 * f10
        pressure = 2.0 * (jac - 1.0) * jac
        sxx = 2.0 * (f00 * f00 + f01 * f01 - 1.0) + pressure
        sxy = 2.0 * (f00 * f10 + f01 * f11)
        syy = 2.0 * (f10 * f10 + f11 * f11 - 1.0) + pressure
        tau = (sxx, sxy, sxy, syy)
        for i in range(4):
            value = alive * (-0.4 * tau[i] + st[k, 4 + i])
            amat[k, i] = value
            if k is OWN:
                first[1, 5 + i] = value

    def prepare_forward(k, role):
        alive = first[role, 4]
        p1 = st[k, 1]
        a_mat = [amat[k, i] for i in range(4)]
        c, w, _, dc = col_parts(p1)
        moved = (alive * st[k, 2], alive * st[k, 3])
        for j in range(3):
            wd = w[j] * dc[j]
            qm[j] = w[j] * alive
            for a in range(2):
                qm[3 + 3 * a + j] = w[j] * moved[a] + wd * a_mat[2 * a + 1]
                qm[9 + 3 * a + j] = w[j] * a_mat[2 * a]
        qm[30] = st[k, 0]
        qm[31] = jnp.where(c < 0.0, c + 128.0, jnp.where(c > 127.0, c - 128.0, c))

    def build_hot(k):
        nodes = lax.broadcasted_iota(jnp.int32, (128, 128), 0).astype(F32)
        for b in range(NB):
            row = qm[31, pl.ds(b, 1), :]
            hot[k, b] = jnp.where(nodes == jnp.broadcast_to(row, (128, 128)), 1.0, 0.0).astype(BF16)

    def adjoint_rows(k, base, adj):
        f00, f01, f10, f11 = (st[k, 8 + i] for i in range(4))
        gf = [adj[8 + i] for i in range(4)]
        v = [adj[2 + a] + DT * adj[a] for a in range(2)]
        x = []
        for a in range(2):
            g0, g1 = gf[2 * a], gf[2 * a + 1]
            x.append(4.0 * (adj[4 + 2 * a] + DT * (g0 * f00 + g1 * f01)))
            x.append(4.0 * (adj[5 + 2 * a] + DT * (g0 * f10 + g1 * f11)))
        _, w, _, dc = col_parts(st[k, 1])
        for j in range(3):
            wd = w[j] * dc[j]
            for a in range(2):
                qm[base + 3 * a + j] = w[j] * v[a] + wd * x[2 * a + 1]
                qm[base + 6 + 3 * a + j] = w[j] * x[2 * a]
        qm[30] = st[k, 0]
        return v, x

    def rate_rows(k):
        v = [rates[1, a] for a in range(2)]
        x = [rates[1, 2 + i] for i in range(4)]
        _, w, _, dc = col_parts(st[k, 1])
        for j in range(3):
            wd = w[j] * dc[j]
            for a in range(2):
                qm[15 + 3 * a + j] = w[j] * v[a] + wd * x[2 * a + 1]
                qm[21 + 3 * a + j] = w[j] * x[2 * a]
        qm[30] = st[k, 0]

    def turn_hot(k):
        for b in range(NB):
            toh[k, b] = hot[k, b].T

    def pair_hot(ref, k, i, zero):
        return jnp.concatenate(
            [
                jnp.concatenate([ref[k, 2 * i], zero], axis=1),
                jnp.concatenate([zero, ref[k, 2 * i + 1]], axis=1),
            ],
            axis=0,
        )

    def scatter(k, rows, turned=False):
        zero = jnp.zeros((128, NP), BF16)
        for i in range(NB // 2):
            sides = []
            for b in (2 * i, 2 * i + 1):
                d = rows8 - jnp.broadcast_to(qm[30, pl.ds(b, 1), :], (8, 128))
                nr, _, _ = row_spline(d)
                nd = nr * d
                pieces = []
                for channel in rows:
                    for q, m in channel:
                        x = nr * jnp.broadcast_to(qm[q, pl.ds(b, 1), :], (8, 128))
                        if m is not None:
                            x = x + nd * jnp.broadcast_to(qm[m, pl.ds(b, 1), :], (8, 128))
                        pieces.append(split_rows(x))
                sides.append(jnp.concatenate(pieces, axis=0).astype(BF16))
            out = lax.dot_general(
                jnp.concatenate(sides, axis=1),
                pair_hot(toh if turned else hot, k, i, zero),
                (((1,), (0 if turned else 1,)), ((), ())),
                preferred_element_type=F32,
            )
            for side, target in enumerate((ev, od)):
                for ch in range(len(rows)):
                    total = None
                    for j, s in enumerate(SHIFTS):
                        at = (3 * ch + j) * 16
                        value = out[at : at + 16, 128 * side : 128 * side + 128]
                        value = value[:8] + value[8:]
                        if s:
                            value = roll(value, s)
                        total = value if total is None else total + value
                    if side:
                        total = roll(total, 64)
                    target[ch, i] = total

    def forward_channels():
        return [[(j, None) for j in range(3)]] + [
            [(3 + 3 * a + j, 9 + 3 * a + j) for j in range(3)] for a in range(2)
        ]

    def adjoint_channels(base):
        return [[(base + 3 * a + j, base + 6 + 3 * a + j) for j in range(3)] for a in range(2)]

    def combine(count, part, force_role, cols=range(COLS)):
        for ch in range(count):
            for i in cols:
                value = ev[ch, i] + jnp.where(left_half, od[ch, (i - 1) % COLS], od[ch, i])
                if force_role is not None and ch in (1, 2):
                    value = value + frc[force_role, ch - 1, :, pl.ds(i * 128, 128)]
                part[ch, :, pl.ds(i * 128, 128)] = value

    def pack(e, c, count, part):
        for ch in range(count):
            for i in range(len(CHUNK_COLS[c]) // 2):
                at = CHUNK_COLS[c][2 * i] * 128
                a = part[ch, :, pl.ds(at, 128)]
                b = part[ch, :, pl.ds(at + 128, 128)]
                down = jnp.where(top_half, pltpu.roll(a, 4, axis=0), b)
                up = jnp.where(top_half, a, pltpu.roll(b, 4, axis=0))
                send[e, c, 0, ch, :, pl.ds(i * 128, 128)] = down
                send[e, c, 1, ch, :, pl.ds(i * 128, 128)] = up

    def copies(e, c, count, targets, source=None):
        return [
            pltpu.make_async_remote_copy(
                src_ref=send.at[e if source is None else source, c, side, pl.ds(0, count)],
                dst_ref=recv.at[e, c, side, pl.ds(0, count)],
                send_sem=send_sem.at[e, c, side],
                recv_sem=recv_sem.at[e, c, side],
                device_id=(other,),
                device_id_type=MESH,
            )
            for side, other in enumerate(targets)
        ]

    def start_halo(e, c, count, targets, source=None):
        for copy in copies(e, c, count, targets, source):
            copy.start()

    def wait_halo(e, c, count, targets, source=None):
        for copy in copies(e, c, count, targets, source):
            copy.wait_recv()

    def scatter_and_send(e, k, rows, part, force_role, targets, before_first=None):
        for c in range(CHUNKS):
            scatter(k, rows, len(rows) == 2)
            combine(len(rows), part, force_role, CHUNK_COLS[c])
            pack(e, c, len(rows), part)
            if before_first is not None and c == 0:
                before_first()
            start_halo(e, c, len(rows), targets)

    def summed(e, c, part, ch, i):
        above = recv[e, c, 0, ch, :, pl.ds(i * 128, 128)]
        below = recv[e, c, 1, ch, :, pl.ds(i * 128, 128)]
        first = jnp.where(top_half, above, pltpu.roll(below, 4, axis=0))
        second = jnp.where(top_half, pltpu.roll(above, 4, axis=0), below)
        at = CHUNK_COLS[c][2 * i] * 128
        return (
            part[ch, :, pl.ds(at, 128)] + first,
            part[ch, :, pl.ds(at + 128, 128)] + second,
        )

    def grid_velocity(k, e, c, part):
        for i in range(len(CHUNK_COLS[c]) // 2):
            mass = summed(e, c, part, 0, i)
            mom = [summed(e, c, part, 1 + a, i) for a in range(2)]
            for h in range(2):
                at = pl.ds(CHUNK_COLS[c][2 * i + h] * 128, 128)
                inverse = 1.0 / (mass[h] + 0.25)
                inv[k, :, at] = inverse
                for a in range(2):
                    vg[k, a, :, at] = mom[a][h] * inverse

    def grid_adjoint(k, e, c, base, part, initial):
        for i in range(len(CHUNK_COLS[c]) // 2):
            u = [summed(e, c, part, base + a, i) for a in range(2)]
            for h in range(2):
                at = pl.ds(CHUNK_COLS[c][2 * i + h] * 128, 128)
                inverse = inv[k, :, at]
                total = u[0][h] * vg[k, 0, :, at] + u[1][h] * vg[k, 1, :, at]
                part[0, :, at] = -total * inverse
                for a in range(2):
                    value = u[a][h] * inverse
                    part[1 + a, :, at] = value
                    fgacc[a, :, at] = DT * value if initial else fgacc[a, :, at] + DT * value

    def gather(k, column, channels):
        stride = 3 * channels * 64
        zero = jnp.zeros((128, NP), BF16)
        for i in range(NB // 2):
            pieces = ([], [])
            for ch in range(channels):
                window = column(ch, i)
                shifted = roll(jnp.where(left_half, column(ch, (i + 1) % COLS), window), 64)
                for s in SHIFTS:
                    pieces[0].append(split_rows(roll(window, -s) if s else window))
                    pieces[1].append(split_rows(roll(shifted, -s) if s else shifted))
            lhs = jnp.concatenate(
                [jnp.concatenate(side, axis=0).astype(BF16) for side in pieces], axis=1
            )
            out = jnp.dot(lhs, pair_hot(hot, k, i, zero), preferred_element_type=F32)
            for side in range(2):
                b = 2 * i + side
                for q in range(3 * channels):
                    rows = out[16 * q : 16 * q + 16, 128 * side : 128 * side + 128]
                    gat[pl.ds((b // 8) * stride + q * 64 + b % 8, 8, stride=8), :] = rows[:8] + rows[8:]

    def gathered(half, channels, q, r):
        return gat[pl.ds(half * 3 * channels * 64 + q * 64 + r * 8, 8), :]

    def row_sums(half, channels, q, weights):
        totals = [None] * len(weights)
        for r in range(2 * BR):
            g = gathered(half, channels, q, r)
            for t, weight in enumerate(weights):
                value = weight[r] * g
                totals[t] = value if totals[t] is None else totals[t] + value
        return totals

    def dot3(a, b):
        return a[0] * b[0] + a[1] * b[1] + a[2] * b[2]

    def row_weights(p0, slopes):
        plain, slant, slope, slope_d = [], [], [], []
        for r in range(2 * BR):
            d = float(r) - p0
            value, t, near = row_spline(d)
            plain.append(value)
            slant.append(value * d)
            if slopes:
                der = row_slope(d, t, near)
                slope.append(der)
                slope_d.append(der * d)
        return (plain, slant, slope, slope_d) if slopes else (plain, slant)

    def advance(k, store_state, channels=2):
        for half in range(2):
            at = pl.ds(8 * half, 8)
            p0, p1 = st[k, 0, at], st[k, 1, at]
            weights = row_weights(p0, False)
            _, w, _, dc = col_parts(p1)
            wd = [w[j] * dc[j] for j in range(3)]
            new_v, new_c = [], []
            for a in range(2):
                sums = [row_sums(half, channels, 3 * a + j, weights) for j in range(3)]
                r0 = [x[0] for x in sums]
                r1 = [x[1] for x in sums]
                new_v.append(dot3(w, r0))
                new_c.append(4.0 * dot3(w, r1))
                new_c.append(4.0 * dot3(wd, r0))
            for a in range(2):
                tsave[k, a, at] = new_v[a]
            for i in range(4):
                tsave[k, 2 + i, at] = new_c[i]
            if store_state:
                f = [st[k, 8 + i, at] for i in range(4)]
                st[k + 1, 0, at] = p0 + DT * new_v[0]
                st[k + 1, 1, at] = p1 + DT * new_v[1]
                for a in range(2):
                    st[k + 1, 2 + a, at] = new_v[a]
                for i in range(4):
                    st[k + 1, 4 + i, at] = new_c[i]
                for a in range(2):
                    c0, c1 = DT * new_c[2 * a], DT * new_c[2 * a + 1]
                    for j in range(2):
                        st[k + 1, 8 + 2 * a + j, at] = f[2 * a + j] + (c0 * f[j] + c1 * f[2 + j])

    def slopes_of(half, channels, first, p0, p1, count, plain_only):
        weights = row_weights(p0, True)
        _, w, wp, dc = col_parts(p1)
        wd = [w[j] * dc[j] for j in range(3)]
        wpd = [wp[j] * dc[j] for j in range(3)]
        results = []
        for ch in range(first, first + count):
            if ch < first + plain_only:
                sums = [row_sums(half, channels, 3 * ch + j, (weights[0], weights[2])) for j in range(3)]
                r0, r2 = ([x[t] for x in sums] for t in range(2))
                results.append((dot3(w, r2), dot3(wp, r0)))
                continue
            sums = [row_sums(half, channels, 3 * ch + j, weights) for j in range(3)]
            r0, r1, r2, r3 = ([x[t] for x in sums] for t in range(4))
            results.append(
                dict(
                    nw=dot3(w, r0),
                    dw=dot3(w, r1),
                    nwd=dot3(wd, r0),
                    pw=dot3(w, r2),
                    pdw=dot3(w, r3),
                    pwd=dot3(wd, r2),
                    nwp=dot3(wp, r0),
                    dwp=dot3(wp, r1),
                    nwpd=dot3(wpd, r0),
                )
            )
        return results

    def save_slopes(k, channels=2):
        for half in range(2):
            at = pl.ds(8 * half, 8)
            found = slopes_of(half, channels, 0, st[k, 0, at], st[k, 1, at], 2, 0)
            for a, t in enumerate(found):
                for i, name in enumerate(("pw", "pdw", "pwd", "nwp", "dwp", "nwpd")):
                    value = t[name]
                    if name in ("pdw", "nwpd"):
                        value = value + t["nw"]
                    tsave[k, 6 + 6 * a + i, at] = value

    def pull_gather(k, v, x, adj):
        gf = [adj[8 + i] for i in range(4)]
        p0, p1 = adj[0], adj[1]
        for a in range(2):
            pw, pdw, pwd, nwp, dwp, nwpd = (tsave[k, 6 + 6 * a + i] for i in range(6))
            p0 = p0 - (v[a] * pw + x[2 * a] * pdw + x[2 * a + 1] * pwd)
            p1 = p1 - (v[a] * nwp + x[2 * a] * dwp + x[2 * a + 1] * nwpd)
        adj[0] = p0
        adj[1] = p1
        c = [tsave[k, 2 + i] for i in range(4)]
        for b in range(2):
            for j in range(2):
                adj[8 + 2 * b + j] = gf[2 * b + j] + DT * (c[b] * gf[j] + c[2 + b] * gf[2 + j])

    def pull_scatter(k, role, adj, channels=3):
        for half in range(2):
            at = pl.ds(8 * half, 8)
            alive = first[role, 4, at]
            p0, p1 = st[k, 0, at], st[k, 1, at]
            mass, px, py = slopes_of(half, channels, channels - 3, p0, p1, 3, 1)
            a_mat = [amat[k, i, at] for i in range(4)]
            g0 = adj[0, at] - alive * mass[0]
            g1 = adj[1, at] - alive * mass[1]
            back = []
            for a, t in enumerate((px, py)):
                moved = alive * st[k, 2 + a, at]
                a0, a1 = a_mat[2 * a], a_mat[2 * a + 1]
                g0 = g0 - (moved * t["pw"] + a0 * (t["pdw"] + t["nw"]) + a1 * t["pwd"])
                g1 = g1 - (moved * t["nwp"] + a0 * t["dwp"] + a1 * (t["nwpd"] + t["nw"]))
                adj[2 + a, at] = alive * t["nw"]
                back += [alive * t["dw"], alive * t["nwd"]]
            adj[0, at] = g0
            adj[1, at] = g1
            for i in range(4):
                adj[4 + i, at] = back[i]
            f00, f01, f10, f11 = (st[k, 8 + i, at] for i in range(4))
            sxx, syy = -0.4 * back[0], -0.4 * back[3]
            sxy = -0.4 * (back[1] + back[2])
            jac = f00 * f11 - f01 * f10
            gj = (sxx + syy) * (2.0 * (2.0 * jac - 1.0))
            adj[8, at] = adj[8, at] + (4.0 * f00 * sxx + 2.0 * f10 * sxy + gj * f11)
            adj[9, at] = adj[9, at] + (4.0 * f01 * sxx + 2.0 * f11 * sxy - gj * f10)
            adj[10, at] = adj[10, at] + (4.0 * f10 * syy + 2.0 * f00 * sxy - gj * f01)
            adj[11, at] = adj[11, at] + (4.0 * f11 * syy + 2.0 * f01 * sxy + gj * f00)

    def grid_column(k):
        return lambda ch, i: vg[k, ch, :, pl.ds(i * 128, 128)]

    def part_column(part):
        return lambda ch, i: part[ch, :, pl.ds(i * 128, 128)]

    def forward_front(k, role):
        if k or role:
            stress_matrix(k, role)
        prepare_forward(k, role)
        build_hot(k)

    def forward_back(k, e, part, targets):
        for c in range(CHUNKS):
            wait_halo(e, c, 3, targets)
            grid_velocity(k, e, c, part)
            gather(k, grid_column(k), 2)
        advance(k, True)

    def backward_back(k, e, part, initial, targets):
        for c in range(CHUNKS):
            wait_halo(e, c, 2, targets)
            grid_adjoint(k, e, c, 0, part, initial)
            gather(k, part_column(part), 3)

    part, part_own = parts.at[0], parts.at[1]
    adj, adj_own = adjs.at[0], adjs.at[1]
    last = STEPS - 1

    load_state()
    forward_front(OWN, 1)
    loads[5].wait()
    loads[6].wait()
    place_force(1)

    def enter():
        barrier_wait()
        start_move(RAW)

    enter()
    scatter_and_send(0, OWN, forward_channels(), part_own, 1, to_hosts)
    start_move(FORCE)
    start_move(STRAIN)
    start_move(COT)
    for c in range(CHUNKS):
        start_halo(7, c, 3, owners, 0)

    end_move(RAW, first, 1, 0)
    host_state()
    forward_front(0, 0)
    scatter(0, forward_channels())
    end_move(FORCE, force, 1, 0)
    place_force(0)
    combine(3, part, 0)
    end_move(STRAIN, strn, 1, 0)
    for i in range(4):
        st[0, 8 + i] = strn[0, i] + (1.0 if i in (0, 3) else 0.0)
    forward_back(0, 0, part, to_hosts)

    for k in range(1, last):
        forward_front(k, 0)
        scatter_and_send(k, k, forward_channels(), part, 0, ring)
        save_slopes(k - 1)
        turn_hot(k - 1)
        if k == 1:
            turn_hot(OWN)
            for c in range(CHUNKS):
                wait_halo(7, c, 3, owners, 0)
                grid_velocity(OWN, 7, c, part_own)
        forward_back(k, k, part, ring)

    end_move(COT, cot, 1, 0)
    for i in range(12):
        adj[i] = cot[0, i] * first[0, 4]
    adjoint_rows(last, 15, adj)
    stress_matrix(last, 0)
    prepare_forward(last, 0)
    build_hot(last)
    scatter_and_send(last, last, forward_channels() + adjoint_channels(15), part, 0, ring)
    save_slopes(last - 1)
    turn_hot(last - 1)

    def last_column(ch, i):
        return grid_column(last)(ch, i) if ch < 2 else part_column(part)(ch - 2, i)

    for c in range(CHUNKS):
        wait_halo(last, c, 5, ring)
        grid_velocity(last, last, c, part)
        grid_adjoint(last, last, c, 3, part, True)
        gather(last, last_column, 5)
    advance(last, False, 5)
    save_slopes(last, 5)
    v, x = adjoint_rows(last, 15, adj)
    pull_gather(last, v, x, adj)
    pull_scatter(last, 0, adj, 5)

    def backward_body(t, carry):
        k = last - 1 - t
        e = last + 1 + t
        v, x = adjoint_rows(k, 15, adj)
        scatter_and_send(e, k, adjoint_channels(15), part, None, ring)
        pull_gather(k, v, x, adj)
        backward_back(k, e, part, False, ring)
        pull_scatter(k, 0, adj)
        return carry

    lax.fori_loop(0, STEPS - 2, backward_body, 0)

    v, x = adjoint_rows(0, 15, adj)
    for i, value in enumerate(v + x):
        rates[0, i] = value
    start_move(RATES)
    scatter_and_send(6, 0, adjoint_channels(15), part, None, to_owners)
    pull_gather(0, v, x, adj)
    for i in range(6):
        rest[0, i] = adj[i if i < 2 else 6 + i]
    for a in range(2):
        fgmove[0, a] = roll(fgacc[a], -(BC // 2))[2:6]
    start_move(ADJ)
    start_move(FGRAD)

    end_move(RATES, rates, 0, 1)
    rate_rows(OWN)
    scatter(OWN, adjoint_channels(15), True)
    combine(2, part_own, None)
    backward_back(OWN, 6, part_own, True, to_owners)
    end_move(ADJ, rest, 0, 1)
    for i in range(6):
        adj_own[i if i < 2 else 6 + i] = rest[1, i]
    pull_scatter(OWN, 1, adj_own)

    sg[0] = adj_own[0] * float(BR)
    sg[1] = adj_own[1] * float(BC)
    for i in range(2, 12):
        sg[i] = adj_own[i]
    end_move(FGRAD, fgmove, 0, 1)
    for a in range(2):
        fg[a] = fgmove[1, a] + roll(fgacc[a], -(BC // 2))[2:6]

    for e in range(EXCHANGES):
        targets = {0: to_hosts, 6: to_owners, 7: owners}.get(e, ring)
        count = 5 if e == last else (2 if e in (4, 5, 6) else 3)
        for c in range(CHUNKS):
            for copy in copies(e, c, count, targets, 0 if e == 7 else None):
                copy.wait_send()

    @pl.when(moved)
    def _():
        for copy in moves:
            copy.wait_send()


def per_device(n, offsets, velocity, affine, strain, tile_fill, force_field, cotangent):
    def flat(x):
        return x.reshape(x.shape[0], NB, NP)

    vmem = pl.BlockSpec(memory_space=pltpu.VMEM)
    width = COLS * 128
    state_grad, force_grad = pl.pallas_call(
        functools.partial(kernel, n),
        out_shape=(
            jax.ShapeDtypeStruct((12, NB, NP), F32),
            jax.ShapeDtypeStruct((2, BR, width), F32),
        ),
        in_specs=[pl.BlockSpec(memory_space=pltpu.HBM)] * 7,
        out_specs=(vmem, vmem),
        scratch_shapes=[
            pltpu.VMEM((1, NB), jnp.int32),
            pltpu.VMEM((4, NB, NP), F32),
            pltpu.VMEM((4, NB, NP), F32),
            pltpu.VMEM((2, 4, NB, NP), F32),
            pltpu.VMEM((2, 9, NB, NP), F32),
            pltpu.VMEM((2, 6, NB, NP), F32),
            pltpu.VMEM((2, 6, NB, NP), F32),
            pltpu.VMEM((2, 2, BR, width), F32),
            pltpu.VMEM((2, 12, NB, NP), F32),
            pltpu.VMEM((STEPS + 1, 12, NB, NP), F32),
            pltpu.VMEM((STEPS + 1, 4, NB, NP), F32),
            pltpu.VMEM((STEPS + 1, NB, 128, NP), BF16),
            pltpu.VMEM((STEPS + 1, NB, NP, 128), BF16),
            pltpu.VMEM((32, NB, NP), F32),
            pltpu.VMEM((MAX_CH, COLS, 8, 128), F32),
            pltpu.VMEM((MAX_CH, COLS, 8, 128), F32),
            pltpu.VMEM((2, MAX_CH, 8, width), F32),
            pltpu.VMEM((STEPS + 1, 2, 8, width), F32),
            pltpu.VMEM((STEPS + 1, 8, width), F32),
            pltpu.VMEM((2, 2, 8, width), F32),
            pltpu.VMEM((2 * 120 * 8, 128), F32),
            pltpu.VMEM((STEPS + 1, 18, NB, NP), F32),
            pltpu.VMEM((2, 12, NB, NP), F32),
            pltpu.VMEM((2, 8, width), F32),
            pltpu.VMEM((2, 2, BR, width), F32),
            pltpu.VMEM((EXCHANGES, CHUNKS, 2, MAX_CH, 8, width // 2 // CHUNKS), F32),
            pltpu.VMEM((EXCHANGES, CHUNKS, 2, MAX_CH, 8, width // 2 // CHUNKS), F32),
            pltpu.SemaphoreType.DMA((7,)),
            pltpu.SemaphoreType.DMA((EXCHANGES, CHUNKS, 2)),
            pltpu.SemaphoreType.DMA((EXCHANGES, CHUNKS, 2)),
            pltpu.SemaphoreType.DMA((7,)),
            pltpu.SemaphoreType.DMA((7,)),
        ],
        compiler_params=pltpu.CompilerParams(collective_id=0, has_side_effects=True, vmem_limit_bytes=24 << 20),
    )(
        pltpu.with_memory_space_constraint(flat(offsets), pltpu.HBM),
        pltpu.with_memory_space_constraint(flat(velocity), pltpu.HBM),
        pltpu.with_memory_space_constraint(flat(affine), pltpu.HBM),
        pltpu.with_memory_space_constraint(flat(strain), pltpu.HBM),
        pltpu.with_memory_space_constraint(tile_fill, pltpu.HBM),
        pltpu.with_memory_space_constraint(force_field, pltpu.HBM),
        pltpu.with_memory_space_constraint(flat(cotangent), pltpu.HBM),
    )
    return state_grad.reshape(12, 1, NB, NP), force_grad


def solution(mesh):
    n = mesh.shape["slab"]
    tiles = P(None, "slab", None, None)
    return jax.shard_map(
        functools.partial(per_device, n),
        mesh=mesh,
        in_specs=(tiles, tiles, tiles, tiles, P("slab", None), P(None, "slab", None), tiles),
        out_specs=(tiles, P(None, "slab", None)),
        check_vma=False,
    )
```

```python
import functools

import jax
import jax.numpy as jnp
from jax import lax
from jax.experimental import pallas as pl
from jax.experimental.pallas import tpu as pltpu
from jax.sharding import PartitionSpec as P

BR = 4
BC = 64
NB = 16
NP = 128
STEPS = 4
COLS = 8
DT = 0.1
F32 = jnp.float32
BF16 = jnp.bfloat16
MESH = pl.DeviceIdType.MESH
SHIFTS = (-1, 0, 1)

EXCHANGES = 8
MAX_CH = 5
CHUNKS = 1
CHUNK_COLS = (tuple(range(COLS)),)
OWN = STEPS
RAW, STRAIN, COT, FORCE, RATES, ADJ, FGRAD = range(7)
CHIPS = {64: (4, 4, 4), 8: (2, 2, 2), 4: (1, 2, 2)}


def host_of(band, n):
    _, nx, ny = CHIPS[n // 2]
    core, chip = lax.rem(band, 2), lax.div(band, 2)
    y, x, z = lax.rem(chip, ny), lax.rem(lax.div(chip, ny), nx), lax.div(chip, nx * ny)
    y = y + lax.rem(x, 2) * (ny - 1 - 2 * y)
    x = x + lax.rem(z, 2) * (nx - 1 - 2 * x)
    return ((z * nx + x) * ny + y) * 2 + core


def band_of(device, n):
    _, nx, ny = CHIPS[n // 2]
    core, chip = lax.rem(device, 2), lax.div(device, 2)
    y, x, z = lax.rem(chip, ny), lax.rem(lax.div(chip, ny), nx), lax.div(chip, nx * ny)
    x = x + lax.rem(z, 2) * (nx - 1 - 2 * x)
    y = y + lax.rem(x, 2) * (ny - 1 - 2 * y)
    return ((z * nx + x) * ny + y) * 2 + core


def row_spline(d):
    m = jnp.abs(d)
    t = jnp.maximum(1.5 - m, 0.0)
    near = m < 0.5
    value = jnp.where(near, 0.75 - m * m, 0.5 * t * t)
    return value, t, near


def row_slope(d, t, near):
    return jnp.where(near, -2.0 * d, jnp.where(d > 0.0, -t, t))


def col_center(p1):
    return jnp.floor(p1 + 0.5)


def col_parts(p1):
    c = col_center(p1)
    d0 = c - p1
    lo, hi = 0.5 + d0, 0.5 - d0
    values = (0.5 * lo * lo, 0.75 - d0 * d0, 0.5 * hi * hi)
    slopes = (lo, -2.0 * d0, -hi)
    w, wp, dc = [], [], []
    for s, value, slope in zip(SHIFTS, values, slopes):
        inside = jnp.logical_and(c >= float(-s), c <= float(2 * BC - 1 - s))
        w.append(jnp.where(inside, value, 0.0))
        wp.append(jnp.where(inside, slope, 0.0))
        dc.append(jnp.where(inside, d0 + float(s), 0.0))
    return c, w, wp, dc


def split_rows(x):
    top = x.astype(BF16).astype(F32)
    return jnp.concatenate([top, x - top], axis=0)


def roll(x, by):
    return pltpu.roll(x, by % x.shape[-1], axis=x.ndim - 1)


def kernel(
    n,
    off_hbm,
    vel_hbm,
    aff_hbm,
    strn_hbm,
    fill_hbm,
    force_hbm,
    cot_hbm,
    sg,
    fg,
    fill,
    raw,
    aff,
    strn,
    first,
    rates,
    rest,
    force,
    cot,
    st,
    amat,
    hot,
    toh,
    qm,
    ev,
    od,
    parts,
    vg,
    inv,
    frc,
    gat,
    tsave,
    adjs,
    fgacc,
    fgmove,
    send,
    recv,
    load_sem,
    send_sem,
    recv_sem,
    move_send,
    move_recv,
):
    me = lax.axis_index("slab")
    band = band_of(me, n)
    home = host_of(me, n)
    moved = home != me
    stays = home == me

    def after(i):
        return lax.rem(i + 1, n)

    def before(i):
        return lax.rem(i + n - 1, n)

    ring = (host_of(after(band), n), host_of(before(band), n))
    to_hosts = (host_of(after(me), n), host_of(before(me), n))
    to_owners = (after(band), before(band))
    owners = (after(me), before(me))

    loads = [
        pltpu.make_async_copy(src, dst, load_sem.at[i])
        for i, (src, dst) in enumerate(
            (
                (off_hbm, raw.at[pl.ds(0, 2)]),
                (vel_hbm, raw.at[pl.ds(2, 2)]),
                (aff_hbm, aff),
                (strn_hbm, strn.at[1]),
                (fill_hbm, fill),
                (force_hbm, force.at[1]),
                (cot_hbm, cot.at[1]),
            )
        )
    ]
    for load in loads:
        load.start()

    barrier = pltpu.get_barrier_semaphore()
    for other in ring + to_hosts + to_owners + owners:
        pl.semaphore_signal(barrier, inc=1, device_id=(other,), device_id_type=MESH)

    @pl.when(moved)
    def _():
        pl.semaphore_signal(barrier, inc=1, device_id=(home,), device_id_type=MESH)
        pl.semaphore_signal(barrier, inc=1, device_id=(band,), device_id_type=MESH)

    def barrier_wait():
        @pl.when(moved)
        def _():
            pl.semaphore_wait(barrier, 10)

        @pl.when(stays)
        def _():
            pl.semaphore_wait(barrier, 8)

    def move(which, src, dst, device):
        return pltpu.make_async_remote_copy(
            src_ref=src,
            dst_ref=dst,
            send_sem=move_send.at[which],
            recv_sem=move_recv.at[which],
            device_id=(device,),
            device_id_type=MESH,
        )

    moves = [
        move(RAW, first.at[1], first.at[0], home),
        move(STRAIN, strn.at[1], strn.at[0], home),
        move(COT, cot.at[1], cot.at[0], home),
        move(FORCE, force.at[1], force.at[0], home),
        move(RATES, rates.at[0], rates.at[1], band),
        move(ADJ, rest.at[0], rest.at[1], band),
        move(FGRAD, fgmove.at[0], fgmove.at[1], band),
    ]

    def start_move(which):
        @pl.when(moved)
        def _():
            moves[which].start()

    def end_move(which, ref, src, dst):
        @pl.when(moved)
        def _():
            moves[which].wait_recv()

        @pl.when(stays)
        def _():
            ref[dst] = ref[src]

    lane16 = lax.broadcasted_iota(jnp.int32, (16, 128), 1)
    sub8 = lax.broadcasted_iota(jnp.int32, (8, 128), 0)
    lane8 = lax.broadcasted_iota(jnp.int32, (8, 128), 1)
    rows8 = sub8.astype(F32)
    top_half = sub8 < 4
    left_half = lane8 < 64

    def load_state():
        for i, value in enumerate(
            (BR // 2 + BR * raw[0], BC // 2 + BC * raw[1], raw[2], raw[3])
        ):
            st[OWN, i] = value
            first[1, i] = value
        for i in range(4):
            st[OWN, 4 + i] = aff[i]
            st[OWN, 8 + i] = strn[1, i] + (1.0 if i in (0, 3) else 0.0)

    def host_state():
        for i in range(4):
            st[0, i] = first[0, i]
            amat[0, i] = first[0, 5 + i]

    def place_force(role):
        for a in range(2):
            rows = DT * force[role, a]
            zero = jnp.zeros((2, COLS * 128), F32)
            frc[role, a] = roll(jnp.concatenate([zero, rows, zero], axis=0), BC // 2)

    for i in (4, 0, 1, 2, 3):
        loads[i].wait()
    eye = lax.broadcasted_iota(jnp.int32, (16, 16), 0) == lax.broadcasted_iota(jnp.int32, (16, 16), 1)
    fills = jnp.where(eye, jnp.broadcast_to(fill[...].astype(F32), (16, 16)), 0.0)
    count = jnp.sum(fills, axis=1, keepdims=True)
    first[1, 4] = jnp.where(lane16.astype(F32) < count, 1.0, 0.0)

    def stress_matrix(k, role):
        alive = first[role, 4]
        f00, f01, f10, f11 = (st[k, 8 + i] for i in range(4))
        jac = f00 * f11 - f01 * f10
        pressure = 2.0 * (jac - 1.0) * jac
        sxx = 2.0 * (f00 * f00 + f01 * f01 - 1.0) + pressure
        sxy = 2.0 * (f00 * f10 + f01 * f11)
        syy = 2.0 * (f10 * f10 + f11 * f11 - 1.0) + pressure
        tau = (sxx, sxy, sxy, syy)
        for i in range(4):
            value = alive * (-0.4 * tau[i] + st[k, 4 + i])
            amat[k, i] = value
            if k is OWN:
                first[1, 5 + i] = value

    def prepare_forward(k, role):
        alive = first[role, 4]
        p1 = st[k, 1]
        a_mat = [amat[k, i] for i in range(4)]
        c, w, _, dc = col_parts(p1)
        moved = (alive * st[k, 2], alive * st[k, 3])
        for j in range(3):
            wd = w[j] * dc[j]
            qm[j] = w[j] * alive
            for a in range(2):
                qm[3 + 3 * a + j] = w[j] * moved[a] + wd * a_mat[2 * a + 1]
                qm[9 + 3 * a + j] = w[j] * a_mat[2 * a]
        qm[30] = st[k, 0]
        qm[31] = jnp.where(c < 0.0, c + 128.0, jnp.where(c > 127.0, c - 128.0, c))

    def build_hot(k):
        nodes = lax.broadcasted_iota(jnp.int32, (128, 128), 0).astype(F32)
        for b in range(NB):
            row = qm[31, pl.ds(b, 1), :]
            hot[k, b] = jnp.where(nodes == jnp.broadcast_to(row, (128, 128)), 1.0, 0.0).astype(BF16)

    def adjoint_rows(k, base, adj):
        f00, f01, f10, f11 = (st[k, 8 + i] for i in range(4))
        gf = [adj[8 + i] for i in range(4)]
        v = [adj[2 + a] + DT * adj[a] for a in range(2)]
        x = []
        for a in range(2):
            g0, g1 = gf[2 * a], gf[2 * a + 1]
            x.append(4.0 * (adj[4 + 2 * a] + DT * (g0 * f00 + g1 * f01)))
            x.append(4.0 * (adj[5 + 2 * a] + DT * (g0 * f10 + g1 * f11)))
        _, w, _, dc = col_parts(st[k, 1])
        for j in range(3):
            wd = w[j] * dc[j]
            for a in range(2):
                qm[base + 3 * a + j] = w[j] * v[a] + wd * x[2 * a + 1]
                qm[base + 6 + 3 * a + j] = w[j] * x[2 * a]
        qm[30] = st[k, 0]
        return v, x

    def rate_rows(k):
        v = [rates[1, a] for a in range(2)]
        x = [rates[1, 2 + i] for i in range(4)]
        _, w, _, dc = col_parts(st[k, 1])
        for j in range(3):
            wd = w[j] * dc[j]
            for a in range(2):
                qm[15 + 3 * a + j] = w[j] * v[a] + wd * x[2 * a + 1]
                qm[21 + 3 * a + j] = w[j] * x[2 * a]
        qm[30] = st[k, 0]

    def turn_hot(k):
        for b in range(NB):
            toh[k, b] = hot[k, b].T

    def pair_hot(ref, k, i, zero):
        return jnp.concatenate(
            [
                jnp.concatenate([ref[k, 2 * i], zero], axis=1),
                jnp.concatenate([zero, ref[k, 2 * i + 1]], axis=1),
            ],
            axis=0,
        )

    def scatter(k, rows, turned=False):
        zero = jnp.zeros((128, NP), BF16)
        for i in range(NB // 2):
            sides = []
            for b in (2 * i, 2 * i + 1):
                d = rows8 - jnp.broadcast_to(qm[30, pl.ds(b, 1), :], (8, 128))
                nr, _, _ = row_spline(d)
                nd = nr * d
                pieces = []
                for channel in rows:
                    for q, m in channel:
                        x = nr * jnp.broadcast_to(qm[q, pl.ds(b, 1), :], (8, 128))
                        if m is not None:
                            x = x + nd * jnp.broadcast_to(qm[m, pl.ds(b, 1), :], (8, 128))
                        pieces.append(split_rows(x))
                sides.append(jnp.concatenate(pieces, axis=0).astype(BF16))
            out = lax.dot_general(
                jnp.concatenate(sides, axis=1),
                pair_hot(toh if turned else hot, k, i, zero),
                (((1,), (0 if turned else 1,)), ((), ())),
                preferred_element_type=F32,
            )
            for side, target in enumerate((ev, od)):
                for ch in range(len(rows)):
                    total = None
                    for j, s in enumerate(SHIFTS):
                        at = (3 * ch + j) * 16
                        value = out[at : at + 16, 128 * side : 128 * side + 128]
                        value = value[:8] + value[8:]
                        if s:
                            value = roll(value, s)
                        total = value if total is None else total + value
                    if side:
                        total = roll(total, 64)
                    target[ch, i] = total

    def forward_channels():
        return [[(j, None) for j in range(3)]] + [
            [(3 + 3 * a + j, 9 + 3 * a + j) for j in range(3)] for a in range(2)
        ]

    def adjoint_channels(base):
        return [[(base + 3 * a + j, base + 6 + 3 * a + j) for j in range(3)] for a in range(2)]

    def combine(count, part, force_role, cols=range(COLS)):
        for ch in range(count):
            for i in cols:
                value = ev[ch, i] + jnp.where(left_half, od[ch, (i - 1) % COLS], od[ch, i])
                if force_role is not None and ch in (1, 2):
                    value = value + frc[force_role, ch - 1, :, pl.ds(i * 128, 128)]
                part[ch, :, pl.ds(i * 128, 128)] = value

    def pack(e, c, count, part):
        for ch in range(count):
            for i in range(len(CHUNK_COLS[c]) // 2):
                at = CHUNK_COLS[c][2 * i] * 128
                a = part[ch, :, pl.ds(at, 128)]
                b = part[ch, :, pl.ds(at + 128, 128)]
                down = jnp.where(top_half, pltpu.roll(a, 4, axis=0), b)
                up = jnp.where(top_half, a, pltpu.roll(b, 4, axis=0))
                send[e, c, 0, ch, :, pl.ds(i * 128, 128)] = down
                send[e, c, 1, ch, :, pl.ds(i * 128, 128)] = up

    def copies(e, c, count, targets, source=None):
        return [
            pltpu.make_async_remote_copy(
                src_ref=send.at[e if source is None else source, c, side, pl.ds(0, count)],
                dst_ref=recv.at[e, c, side, pl.ds(0, count)],
                send_sem=send_sem.at[e, c, side],
                recv_sem=recv_sem.at[e, c, side],
                device_id=(other,),
                device_id_type=MESH,
            )
            for side, other in enumerate(targets)
        ]

    def start_halo(e, c, count, targets, source=None):
        for copy in copies(e, c, count, targets, source):
            copy.start()

    def wait_halo(e, c, count, targets, source=None):
        for copy in copies(e, c, count, targets, source):
            copy.wait_recv()

    def scatter_and_send(e, k, rows, part, force_role, targets, before_first=None):
        for c in range(CHUNKS):
            scatter(k, rows, len(rows) == 2)
            combine(len(rows), part, force_role, CHUNK_COLS[c])
            pack(e, c, len(rows), part)
            if before_first is not None and c == 0:
                before_first()
            start_halo(e, c, len(rows), targets)

    def summed(e, c, part, ch, i):
        above = recv[e, c, 0, ch, :, pl.ds(i * 128, 128)]
        below = recv[e, c, 1, ch, :, pl.ds(i * 128, 128)]
        first = jnp.where(top_half, above, pltpu.roll(below, 4, axis=0))
        second = jnp.where(top_half, pltpu.roll(above, 4, axis=0), below)
        at = CHUNK_COLS[c][2 * i] * 128
        return (
            part[ch, :, pl.ds(at, 128)] + first,
            part[ch, :, pl.ds(at + 128, 128)] + second,
        )

    def grid_velocity(k, e, c, part):
        for i in range(len(CHUNK_COLS[c]) // 2):
            mass = summed(e, c, part, 0, i)
            mom = [summed(e, c, part, 1 + a, i) for a in range(2)]
            for h in range(2):
                at = pl.ds(CHUNK_COLS[c][2 * i + h] * 128, 128)
                inverse = 1.0 / (mass[h] + 0.25)
                inv[k, :, at] = inverse
                for a in range(2):
                    vg[k, a, :, at] = mom[a][h] * inverse

    def grid_adjoint(k, e, c, base, part, initial):
        for i in range(len(CHUNK_COLS[c]) // 2):
            u = [summed(e, c, part, base + a, i) for a in range(2)]
            for h in range(2):
                at = pl.ds(CHUNK_COLS[c][2 * i + h] * 128, 128)
                inverse = inv[k, :, at]
                total = u[0][h] * vg[k, 0, :, at] + u[1][h] * vg[k, 1, :, at]
                part[0, :, at] = -total * inverse
                for a in range(2):
                    value = u[a][h] * inverse
                    part[1 + a, :, at] = value
                    fgacc[a, :, at] = DT * value if initial else fgacc[a, :, at] + DT * value

    def gather(k, column, channels):
        stride = 3 * channels * 64
        zero = jnp.zeros((128, NP), BF16)
        for i in range(NB // 2):
            pieces = ([], [])
            for ch in range(channels):
                window = column(ch, i)
                shifted = roll(jnp.where(left_half, column(ch, (i + 1) % COLS), window), 64)
                for s in SHIFTS:
                    pieces[0].append(split_rows(roll(window, -s) if s else window))
                    pieces[1].append(split_rows(roll(shifted, -s) if s else shifted))
            lhs = jnp.concatenate(
                [jnp.concatenate(side, axis=0).astype(BF16) for side in pieces], axis=1
            )
            out = jnp.dot(lhs, pair_hot(hot, k, i, zero), preferred_element_type=F32)
            for side in range(2):
                b = 2 * i + side
                for q in range(3 * channels):
                    rows = out[16 * q : 16 * q + 16, 128 * side : 128 * side + 128]
                    gat[pl.ds((b // 8) * stride + q * 64 + b % 8, 8, stride=8), :] = rows[:8] + rows[8:]

    def gathered(half, channels, q, r):
        return gat[pl.ds(half * 3 * channels * 64 + q * 64 + r * 8, 8), :]

    def row_sums(half, channels, q, weights):
        totals = [None] * len(weights)
        for r in range(2 * BR):
            g = gathered(half, channels, q, r)
            for t, weight in enumerate(weights):
                value = weight[r] * g
                totals[t] = value if totals[t] is None else totals[t] + value
        return totals

    def dot3(a, b):
        return a[0] * b[0] + a[1] * b[1] + a[2] * b[2]

    def row_weights(p0, slopes):
        plain, slant, slope, slope_d = [], [], [], []
        for r in range(2 * BR):
            d = float(r) - p0
            value, t, near = row_spline(d)
            plain.append(value)
            slant.append(value * d)
            if slopes:
                der = row_slope(d, t, near)
                slope.append(der)
                slope_d.append(der * d)
        return (plain, slant, slope, slope_d) if slopes else (plain, slant)

    def advance(k, store_state, channels=2):
        for half in range(2):
            at = pl.ds(8 * half, 8)
            p0, p1 = st[k, 0, at], st[k, 1, at]
            weights = row_weights(p0, False)
            _, w, _, dc = col_parts(p1)
            wd = [w[j] * dc[j] for j in range(3)]
            new_v, new_c = [], []
            for a in range(2):
                sums = [row_sums(half, channels, 3 * a + j, weights) for j in range(3)]
                r0 = [x[0] for x in sums]
                r1 = [x[1] for x in sums]
                new_v.append(dot3(w, r0))
                new_c.append(4.0 * dot3(w, r1))
                new_c.append(4.0 * dot3(wd, r0))
            for a in range(2):
                tsave[k, a, at] = new_v[a]
            for i in range(4):
                tsave[k, 2 + i, at] = new_c[i]
            if store_state:
                f = [st[k, 8 + i, at] for i in range(4)]
                st[k + 1, 0, at] = p0 + DT * new_v[0]
                st[k + 1, 1, at] = p1 + DT * new_v[1]
                for a in range(2):
                    st[k + 1, 2 + a, at] = new_v[a]
                for i in range(4):
                    st[k + 1, 4 + i, at] = new_c[i]
                for a in range(2):
                    c0, c1 = DT * new_c[2 * a], DT * new_c[2 * a + 1]
                    for j in range(2):
                        st[k + 1, 8 + 2 * a + j, at] = f[2 * a + j] + (c0 * f[j] + c1 * f[2 + j])

    def slopes_of(half, channels, first, p0, p1, count, plain_only):
        weights = row_weights(p0, True)
        _, w, wp, dc = col_parts(p1)
        wd = [w[j] * dc[j] for j in range(3)]
        wpd = [wp[j] * dc[j] for j in range(3)]
        results = []
        for ch in range(first, first + count):
            if ch < first + plain_only:
                sums = [row_sums(half, channels, 3 * ch + j, (weights[0], weights[2])) for j in range(3)]
                r0, r2 = ([x[t] for x in sums] for t in range(2))
                results.append((dot3(w, r2), dot3(wp, r0)))
                continue
            sums = [row_sums(half, channels, 3 * ch + j, weights) for j in range(3)]
            r0, r1, r2, r3 = ([x[t] for x in sums] for t in range(4))
            results.append(
                dict(
                    nw=dot3(w, r0),
                    dw=dot3(w, r1),
                    nwd=dot3(wd, r0),
                    pw=dot3(w, r2),
                    pdw=dot3(w, r3),
                    pwd=dot3(wd, r2),
                    nwp=dot3(wp, r0),
                    dwp=dot3(wp, r1),
                    nwpd=dot3(wpd, r0),
                )
            )
        return results

    def save_slopes(k, channels=2):
        for half in range(2):
            at = pl.ds(8 * half, 8)
            found = slopes_of(half, channels, 0, st[k, 0, at], st[k, 1, at], 2, 0)
            for a, t in enumerate(found):
                for i, name in enumerate(("pw", "pdw", "pwd", "nwp", "dwp", "nwpd")):
                    value = t[name]
                    if name in ("pdw", "nwpd"):
                        value = value + t["nw"]
                    tsave[k, 6 + 6 * a + i, at] = value

    def pull_gather(k, v, x, adj):
        gf = [adj[8 + i] for i in range(4)]
        p0, p1 = adj[0], adj[1]
        for a in range(2):
            pw, pdw, pwd, nwp, dwp, nwpd = (tsave[k, 6 + 6 * a + i] for i in range(6))
            p0 = p0 - (v[a] * pw + x[2 * a] * pdw + x[2 * a + 1] * pwd)
            p1 = p1 - (v[a] * nwp + x[2 * a] * dwp + x[2 * a + 1] * nwpd)
        adj[0] = p0
        adj[1] = p1
        c = [tsave[k, 2 + i] for i in range(4)]
        for b in range(2):
            for j in range(2):
                adj[8 + 2 * b + j] = gf[2 * b + j] + DT * (c[b] * gf[j] + c[2 + b] * gf[2 + j])

    def pull_scatter(k, role, adj, channels=3):
        for half in range(2):
            at = pl.ds(8 * half, 8)
            alive = first[role, 4, at]
            p0, p1 = st[k, 0, at], st[k, 1, at]
            mass, px, py = slopes_of(half, channels, channels - 3, p0, p1, 3, 1)
            a_mat = [amat[k, i, at] for i in range(4)]
            g0 = adj[0, at] - alive * mass[0]
            g1 = adj[1, at] - alive * mass[1]
            back = []
            for a, t in enumerate((px, py)):
                moved = alive * st[k, 2 + a, at]
                a0, a1 = a_mat[2 * a], a_mat[2 * a + 1]
                g0 = g0 - (moved * t["pw"] + a0 * (t["pdw"] + t["nw"]) + a1 * t["pwd"])
                g1 = g1 - (moved * t["nwp"] + a0 * t["dwp"] + a1 * (t["nwpd"] + t["nw"]))
                adj[2 + a, at] = alive * t["nw"]
                back += [alive * t["dw"], alive * t["nwd"]]
            adj[0, at] = g0
            adj[1, at] = g1
            for i in range(4):
                adj[4 + i, at] = back[i]
            f00, f01, f10, f11 = (st[k, 8 + i, at] for i in range(4))
            sxx, syy = -0.4 * back[0], -0.4 * back[3]
            sxy = -0.4 * (back[1] + back[2])
            jac = f00 * f11 - f01 * f10
            gj = (sxx + syy) * (2.0 * (2.0 * jac - 1.0))
            adj[8, at] = adj[8, at] + (4.0 * f00 * sxx + 2.0 * f10 * sxy + gj * f11)
            adj[9, at] = adj[9, at] + (4.0 * f01 * sxx + 2.0 * f11 * sxy - gj * f10)
            adj[10, at] = adj[10, at] + (4.0 * f10 * syy + 2.0 * f00 * sxy - gj * f01)
            adj[11, at] = adj[11, at] + (4.0 * f11 * syy + 2.0 * f01 * sxy + gj * f00)

    def grid_column(k):
        return lambda ch, i: vg[k, ch, :, pl.ds(i * 128, 128)]

    def part_column(part):
        return lambda ch, i: part[ch, :, pl.ds(i * 128, 128)]

    def forward_front(k, role):
        if k or role:
            stress_matrix(k, role)
        prepare_forward(k, role)
        build_hot(k)

    def forward_back(k, e, part, targets):
        for c in range(CHUNKS):
            wait_halo(e, c, 3, targets)
            grid_velocity(k, e, c, part)
            gather(k, grid_column(k), 2)
        advance(k, True)

    def backward_back(k, e, part, initial, targets):
        for c in range(CHUNKS):
            wait_halo(e, c, 2, targets)
            grid_adjoint(k, e, c, 0, part, initial)
            gather(k, part_column(part), 3)

    part, part_own = parts.at[0], parts.at[1]
    adj, adj_own = adjs.at[0], adjs.at[1]
    last = STEPS - 1

    load_state()
    forward_front(OWN, 1)
    loads[5].wait()
    loads[6].wait()
    place_force(1)

    def enter():
        barrier_wait()
        start_move(RAW)

    enter()
    scatter_and_send(0, OWN, forward_channels(), part_own, 1, to_hosts)
    start_move(FORCE)
    start_move(STRAIN)

    end_move(RAW, first, 1, 0)
    host_state()
    forward_front(0, 0)
    scatter(0, forward_channels())
    combine(3, part, None)
    for c in range(CHUNKS):
        wait_halo(0, c, 3, to_hosts)
    end_move(FORCE, force, 1, 0)
    place_force(0)
    for a in range(2):
        part[1 + a] = part[1 + a] + frc[0, a]
    for c in range(CHUNKS):
        grid_velocity(0, 0, c, part)
        gather(0, grid_column(0), 2)
    end_move(STRAIN, strn, 1, 0)
    for i in range(4):
        st[0, 8 + i] = strn[0, i] + (1.0 if i in (0, 3) else 0.0)
    advance(0, True)
    start_move(COT)
    for c in range(CHUNKS):
        start_halo(7, c, 3, owners, 0)

    for k in range(1, last):
        forward_front(k, 0)
        scatter_and_send(k, k, forward_channels(), part, 0, ring)
        save_slopes(k - 1)
        turn_hot(k - 1)
        if k == 2:
            turn_hot(OWN)
            for c in range(CHUNKS):
                wait_halo(7, c, 3, owners, 0)
                grid_velocity(OWN, 7, c, part_own)
        forward_back(k, k, part, ring)

    end_move(COT, cot, 1, 0)
    for i in range(12):
        adj[i] = cot[0, i] * first[0, 4]
    adjoint_rows(last, 15, adj)
    stress_matrix(last, 0)
    prepare_forward(last, 0)
    build_hot(last)
    scatter_and_send(last, last, forward_channels() + adjoint_channels(15), part, 0, ring)
    save_slopes(last - 1)
    turn_hot(last - 1)

    def last_column(ch, i):
        return grid_column(last)(ch, i) if ch < 2 else part_column(part)(ch - 2, i)

    for c in range(CHUNKS):
        wait_halo(last, c, 5, ring)
        grid_velocity(last, last, c, part)
        grid_adjoint(last, last, c, 3, part, True)
        gather(last, last_column, 5)
    advance(last, False, 5)
    save_slopes(last, 5)
    v, x = adjoint_rows(last, 15, adj)
    pull_gather(last, v, x, adj)
    pull_scatter(last, 0, adj, 5)

    def backward_body(t, carry):
        k = last - 1 - t
        e = last + 1 + t
        v, x = adjoint_rows(k, 15, adj)
        scatter_and_send(e, k, adjoint_channels(15), part, None, ring)
        pull_gather(k, v, x, adj)
        backward_back(k, e, part, False, ring)
        pull_scatter(k, 0, adj)
        return carry

    lax.fori_loop(0, STEPS - 2, backward_body, 0)

    v, x = adjoint_rows(0, 15, adj)
    for i, value in enumerate(v + x):
        rates[0, i] = value
    start_move(RATES)
    scatter_and_send(6, 0, adjoint_channels(15), part, None, to_owners)
    pull_gather(0, v, x, adj)
    for i in range(6):
        rest[0, i] = adj[i if i < 2 else 6 + i]
    for a in range(2):
        fgmove[0, a] = roll(fgacc[a], -(BC // 2))[2:6]
    start_move(ADJ)
    start_move(FGRAD)

    end_move(RATES, rates, 0, 1)
    rate_rows(OWN)
    scatter(OWN, adjoint_channels(15), True)
    combine(2, part_own, None)
    backward_back(OWN, 6, part_own, True, to_owners)
    end_move(ADJ, rest, 0, 1)
    for i in range(6):
        adj_own[i if i < 2 else 6 + i] = rest[1, i]
    pull_scatter(OWN, 1, adj_own)

    sg[0] = adj_own[0] * float(BR)
    sg[1] = adj_own[1] * float(BC)
    for i in range(2, 12):
        sg[i] = adj_own[i]
    end_move(FGRAD, fgmove, 0, 1)
    for a in range(2):
        fg[a] = fgmove[1, a] + roll(fgacc[a], -(BC // 2))[2:6]

    for e in range(EXCHANGES):
        targets = {0: to_hosts, 6: to_owners, 7: owners}.get(e, ring)
        count = 5 if e == last else (2 if e in (4, 5, 6) else 3)
        for c in range(CHUNKS):
            for copy in copies(e, c, count, targets, 0 if e == 7 else None):
                copy.wait_send()

    @pl.when(moved)
    def _():
        for copy in moves:
            copy.wait_send()


def per_device(n, offsets, velocity, affine, strain, tile_fill, force_field, cotangent):
    def flat(x):
        return x.reshape(x.shape[0], NB, NP)

    vmem = pl.BlockSpec(memory_space=pltpu.VMEM)
    width = COLS * 128
    state_grad, force_grad = pl.pallas_call(
        functools.partial(kernel, n),
        out_shape=(
            jax.ShapeDtypeStruct((12, NB, NP), F32),
            jax.ShapeDtypeStruct((2, BR, width), F32),
        ),
        in_specs=[pl.BlockSpec(memory_space=pltpu.HBM)] * 7,
        out_specs=(vmem, vmem),
        scratch_shapes=[
            pltpu.VMEM((1, NB), jnp.int32),
            pltpu.VMEM((4, NB, NP), F32),
            pltpu.VMEM((4, NB, NP), F32),
            pltpu.VMEM((2, 4, NB, NP), F32),
            pltpu.VMEM((2, 9, NB, NP), F32),
            pltpu.VMEM((2, 6, NB, NP), F32),
            pltpu.VMEM((2, 6, NB, NP), F32),
            pltpu.VMEM((2, 2, BR, width), F32),
            pltpu.VMEM((2, 12, NB, NP), F32),
            pltpu.VMEM((STEPS + 1, 12, NB, NP), F32),
            pltpu.VMEM((STEPS + 1, 4, NB, NP), F32),
            pltpu.VMEM((STEPS + 1, NB, 128, NP), BF16),
            pltpu.VMEM((STEPS + 1, NB, NP, 128), BF16),
            pltpu.VMEM((32, NB, NP), F32),
            pltpu.VMEM((MAX_CH, COLS, 8, 128), F32),
            pltpu.VMEM((MAX_CH, COLS, 8, 128), F32),
            pltpu.VMEM((2, MAX_CH, 8, width), F32),
            pltpu.VMEM((STEPS + 1, 2, 8, width), F32),
            pltpu.VMEM((STEPS + 1, 8, width), F32),
            pltpu.VMEM((2, 2, 8, width), F32),
            pltpu.VMEM((2 * 120 * 8, 128), F32),
            pltpu.VMEM((STEPS + 1, 18, NB, NP), F32),
            pltpu.VMEM((2, 12, NB, NP), F32),
            pltpu.VMEM((2, 8, width), F32),
            pltpu.VMEM((2, 2, BR, width), F32),
            pltpu.VMEM((EXCHANGES, CHUNKS, 2, MAX_CH, 8, width // 2 // CHUNKS), F32),
            pltpu.VMEM((EXCHANGES, CHUNKS, 2, MAX_CH, 8, width // 2 // CHUNKS), F32),
            pltpu.SemaphoreType.DMA((7,)),
            pltpu.SemaphoreType.DMA((EXCHANGES, CHUNKS, 2)),
            pltpu.SemaphoreType.DMA((EXCHANGES, CHUNKS, 2)),
            pltpu.SemaphoreType.DMA((7,)),
            pltpu.SemaphoreType.DMA((7,)),
        ],
        compiler_params=pltpu.CompilerParams(collective_id=0, has_side_effects=True, vmem_limit_bytes=24 << 20),
    )(
        pltpu.with_memory_space_constraint(flat(offsets), pltpu.HBM),
        pltpu.with_memory_space_constraint(flat(velocity), pltpu.HBM),
        pltpu.with_memory_space_constraint(flat(affine), pltpu.HBM),
        pltpu.with_memory_space_constraint(flat(strain), pltpu.HBM),
        pltpu.with_memory_space_constraint(tile_fill, pltpu.HBM),
        pltpu.with_memory_space_constraint(force_field, pltpu.HBM),
        pltpu.with_memory_space_constraint(flat(cotangent), pltpu.HBM),
    )
    return state_grad.reshape(12, 1, NB, NP), force_grad


def solution(mesh):
    n = mesh.shape["slab"]
    tiles = P(None, "slab", None, None)
    return jax.shard_map(
        functools.partial(per_device, n),
        mesh=mesh,
        in_specs=(tiles, tiles, tiles, tiles, P("slab", None), P(None, "slab", None), tiles),
        out_specs=(tiles, P(None, "slab", None)),
        check_vma=False,
    )
```
